32 devices in a mesh: dp: 2 (over x), tp: 4 (over z), pp: 4 (over y, core).
Axes of the slice: x: 2, y: 2, z: 4, core: 2. Of those that a mesh axis runs over, the one named last changes fastest.
Arguments:
- x_in: bfloat16 [8, 32, 64, 2048], P(None, 'dp', 'tp'), parts along dimension 1
- ln_params: float32 [4, 4, 2048], P('pp')
- w_q: bfloat16 [4, 2048, 16, 1, 128], P('pp', None, 'tp')
- w_k: bfloat16 [4, 2048, 16, 128], P('pp', None, 'tp')
- w_v: bfloat16 [4, 2048, 16, 128], P('pp', None, 'tp')
- w_o: bfloat16 [4, 16, 1, 128, 2048], P('pp', 'tp')
- w_up: bfloat16 [4, 2048, 8192], P('pp', None, 'tp')
- w_down: bfloat16 [4, 8192, 2048], P('pp', 'tp')
Outputs:
- output: bfloat16 [4, 8, 32, 64, 2048], P('pp', None, 'dp', 'tp'), parts along dimension 2
There are 2 independent parts. The reference program is written for one: setup_inputs(seed, part) draws one part's arguments, and reference() takes and returns one part's arrays. A program takes and returns all parts, laid end to end along the dimension named above; an argument that names none is the same for every part.
All inputs are finite; a program needn't handle non-finite values.
Results may differ from the reference program's by a relative error of at most 0.0189104.
Values are sent between devices in bfloat16 or wider.
A program may use at most 1 GiB of HBM per device.

```python
import jax
import jax.numpy as jnp
from jax import lax

STAGES = 4
MICRO_BATCHES = 8
BATCH_SIZE = 16
SEQ_LEN = 64
D_MODEL = 2048
NUM_HEADS = 16
KV_COUNT = 16
HEAD_DIM = 128
FF_DIM = 8192

GROUP_SIZE = NUM_HEADS // KV_COUNT
LN_EPS = 1e-5
ROPE_BASE = 10000.0


def setup_inputs(seed: int = 0, part: int = 0) -> dict:
    rng_keys = jax.random.split(jax.random.key(seed), 8)
    x_key = jax.random.fold_in(rng_keys[0], part)
    x_in = jax.random.normal(x_key, (MICRO_BATCHES, BATCH_SIZE, SEQ_LEN, D_MODEL), jnp.float32)
    ln_offset = jnp.array([1.0, 0.0, 1.0, 0.0], jnp.float32)[None, :, None]
    ln_params = ln_offset + 0.5 * jax.random.normal(rng_keys[1], (STAGES, 4, D_MODEL), jnp.float32)
    in_scale = D_MODEL ** -0.5
    w_q = (1.25 * in_scale) * jax.random.normal(rng_keys[2], (STAGES, D_MODEL, KV_COUNT, GROUP_SIZE, HEAD_DIM), jnp.float32)
    w_k = (1.25 * in_scale) * jax.random.normal(rng_keys[3], (STAGES, D_MODEL, KV_COUNT, HEAD_DIM), jnp.float32)
    w_v = in_scale * jax.random.normal(rng_keys[4], (STAGES, D_MODEL, KV_COUNT, HEAD_DIM), jnp.float32)
    w_o = (3.0 * (NUM_HEADS * HEAD_DIM) ** -0.5) * jax.random.normal(rng_keys[5], (STAGES, KV_COUNT, GROUP_SIZE, HEAD_DIM, D_MODEL), jnp.float32)
    w_up = in_scale * jax.random.normal(rng_keys[6], (STAGES, D_MODEL, FF_DIM), jnp.float32)
    w_down = (FF_DIM ** -0.5) * jax.random.normal(rng_keys[7], (STAGES, FF_DIM, D_MODEL), jnp.float32)
    return {"x_in": x_in.astype(jnp.bfloat16), "ln_params": ln_params, "w_q": w_q.astype(jnp.bfloat16), "w_k": w_k.astype(jnp.bfloat16), "w_v": w_v.astype(jnp.bfloat16), "w_o": w_o.astype(jnp.bfloat16), "w_up": w_up.astype(jnp.bfloat16), "w_down": w_down.astype(jnp.bfloat16)}


def layer_norm(x_act, ln_gain, ln_bias):
    x_f32 = x_act.astype(jnp.float32)
    row_mean = jnp.mean(x_f32, axis=-1, keepdims=True)
    centred = x_f32 - row_mean
    variance = jnp.mean(centred * centred, axis=-1, keepdims=True)
    return (centred * lax.rsqrt(variance + LN_EPS) * ln_gain + ln_bias).astype(jnp.bfloat16)


def rope_tables():
    positions = jnp.arange(SEQ_LEN, dtype=jnp.float32)
    inv_freq = ROPE_BASE ** (-2.0 * jnp.arange(HEAD_DIM // 2, dtype=jnp.float32) / HEAD_DIM)
    angles = positions[:, None] * inv_freq[None, :]
    return jnp.cos(angles), jnp.sin(angles)


def apply_rope(proj, cos_tab, sin_tab):
    half_dim = HEAD_DIM // 2
    table_shape = (1, SEQ_LEN) + (1,) * (proj.ndim - 3) + (half_dim,)
    cos_bcast = cos_tab.reshape(table_shape)
    sin_bcast = sin_tab.reshape(table_shape)
    first_half = proj[..., :half_dim]
    second_half = proj[..., half_dim:]
    return jnp.concatenate([first_half * cos_bcast - second_half * sin_bcast, second_half * cos_bcast + first_half * sin_bcast], axis=-1)


def parallel_block(x_act, ln_par, w_q, w_k, w_v, w_o, w_up, w_down):
    num_rows = BATCH_SIZE * SEQ_LEN
    h_attn = layer_norm(x_act, ln_par[0], ln_par[1]).reshape(num_rows, D_MODEL)
    h_mlp = layer_norm(x_act, ln_par[2], ln_par[3]).reshape(num_rows, D_MODEL)
    cos_tab, sin_tab = rope_tables()
    q_proj = jnp.dot(h_attn, w_q.reshape(D_MODEL, NUM_HEADS * HEAD_DIM), preferred_element_type=jnp.float32)
    q_proj = apply_rope(q_proj.reshape(BATCH_SIZE, SEQ_LEN, KV_COUNT, GROUP_SIZE, HEAD_DIM), cos_tab, sin_tab).astype(jnp.bfloat16)
    k_proj = jnp.dot(h_attn, w_k.reshape(D_MODEL, KV_COUNT * HEAD_DIM), preferred_element_type=jnp.float32)
    k_proj = apply_rope(k_proj.reshape(BATCH_SIZE, SEQ_LEN, KV_COUNT, HEAD_DIM), cos_tab, sin_tab).astype(jnp.bfloat16)
    v_proj = jnp.dot(h_attn, w_v.reshape(D_MODEL, KV_COUNT * HEAD_DIM), preferred_element_type=jnp.float32).astype(jnp.bfloat16)
    v_proj = v_proj.reshape(BATCH_SIZE, SEQ_LEN, KV_COUNT, HEAD_DIM)
    allowed = jnp.arange(SEQ_LEN)[:, None, None] >= jnp.arange(SEQ_LEN)[None, None, :]

    def group_attention(operands):
        q_grp, k_grp, v_grp = operands
        scores = jnp.einsum("btgh,bsh->btgs", q_grp.astype(jnp.float32), k_grp.astype(jnp.float32)) * (HEAD_DIM ** -0.5)
        probs_bf = jax.nn.softmax(jnp.where(allowed, scores, -1e30), axis=-1).astype(jnp.bfloat16)
        return jnp.einsum("btgs,bsh->btgh", probs_bf.astype(jnp.float32), v_grp.astype(jnp.float32)).astype(jnp.bfloat16)

    context = lax.map(group_attention, (jnp.moveaxis(q_proj, 2, 0), jnp.moveaxis(k_proj, 2, 0), jnp.moveaxis(v_proj, 2, 0)))
    context = jnp.moveaxis(context, 0, 2).reshape(num_rows, NUM_HEADS * HEAD_DIM)
    attn_out = jnp.dot(context, w_o.reshape(NUM_HEADS * HEAD_DIM, D_MODEL), preferred_element_type=jnp.float32)
    hidden = jax.nn.gelu(jnp.dot(h_mlp, w_up, preferred_element_type=jnp.float32), approximate=False).astype(jnp.bfloat16)
    mlp_out = jnp.dot(hidden, w_down, preferred_element_type=jnp.float32)
    summed = x_act.reshape(num_rows, D_MODEL).astype(jnp.float32) + attn_out + mlp_out
    return summed.astype(jnp.bfloat16).reshape(BATCH_SIZE, SEQ_LEN, D_MODEL)


def reference(x_in, ln_params, w_q, w_k, w_v, w_o, w_up, w_down):
    def one_micro(x_act):
        def stage_step(x_cur, weights):
            ln_par, wq_s, wk_s, wv_s, wo_s, wup_s, wdown_s = weights
            y_next = parallel_block(x_cur, ln_par, wq_s, wk_s, wv_s, wo_s, wup_s, wdown_s)
            return y_next, y_next
        _, per_stage = lax.scan(stage_step, x_act, (ln_params, w_q, w_k, w_v, w_o, w_up, w_down))
        return per_stage
    stacked = lax.map(one_micro, x_in)
    return jnp.swapaxes(stacked, 0, 1)
```

```python
import functools

import jax
import jax.numpy as jnp
from jax import lax
from jax.experimental import pallas as pl
from jax.experimental.pallas import tpu as pltpu
from jax.sharding import PartitionSpec as P

LN_EPS = 1e-5
ROPE_BASE = 10000.0
CHUNKS_PER_MICRO = 4
NT = 256
NX, NR, NP, NY, NS = 4, 4, 2, 3, 4
MESH = pl.DeviceIdType.MESH


def rope_tables(seq_len, head_dim):
    positions = jnp.arange(seq_len, dtype=jnp.float32)
    inv_freq = ROPE_BASE ** (-2.0 * jnp.arange(head_dim // 2, dtype=jnp.float32) / head_dim)
    angles = positions[:, None] * inv_freq[None, :]
    return jnp.cos(angles), jnp.sin(angles)


def pipeline_kernel(dims, x_hbm, ln_ref, cos_ref, sin_ref, mask_ref, wqkv_hbm, wo_hbm, wup_hbm, wdn_hbm, out_hbm,
                    wqkv, wup, wod, xin, xfull, rbuf, part, ha, hm, qkv, act, ybuf,
                    w_sem, xin_sem, ag_ss, ag_rs, rs_ss, rs_rs, out_sem, fwd_sem):
    nc, tp, pp, heads, hd = dims
    rb, d_model = xin.shape[1:]
    rows = tp * rb
    ff = wup.shape[1]
    qd = heads * hd
    last = tp - 1
    z = lax.axis_index("tp")
    s = lax.axis_index("pp")
    has_left, has_right = z > 0, z < last
    has_prev, has_next = s > 0, s < pp - 1

    def remote(src, dst, ss, rs, to):
        return pltpu.make_async_remote_copy(src_ref=src, dst_ref=dst, send_sem=ss, recv_sem=rs, device_id=to, device_id_type=MESH)

    def neighbour(way):
        return {"tp": jnp.minimum(z + 1, last) if way == 0 else jnp.maximum(z - 1, 0)}

    def ag_copy(c, h, way):
        b = jnp.clip(z - h if way == 0 else z + h, 0, last)
        src = xin.at[c] if h == 0 else xfull.at[c % NX, b]
        return remote(src, xfull.at[c % NX, b], ag_ss.at[c % NS, way, h], ag_rs.at[c % NS, way, h], neighbour(way))

    def ag_sends(h, way):
        return has_right & (z >= h) if way == 0 else has_left & (z + h <= last)

    def ag_gets(h, way):
        return z - 1 - h >= 0 if way == 0 else z + 1 + h <= last

    def rs_copy(c, h, way):
        d = jnp.clip(z + last - h if way == 0 else z - last + h, 0, last)
        return remote(part.at[c % NP, d], rbuf.at[c % NR, way, h], rs_ss.at[c % NS, way, h], rs_rs.at[c % NS, way, h], neighbour(way))

    def rs_sends(h, way):
        return z <= h if way == 0 else last - z <= h

    def rs_sends_all(h, way):
        return rs_sends(h, way) & (has_right if way == 0 else has_left)

    def rs_gets(h, way):
        return has_left & (z - 1 <= h) if way == 0 else has_right & (last - 1 - z <= h)

    def out_copy(c):
        return pltpu.make_async_copy(ybuf.at[c % NY], out_hbm.at[c], out_sem.at[c % NY])

    def fwd_copy(c):
        return remote(ybuf.at[c % NY], xin.at[c], fwd_sem.at[c % NY], xin_sem.at[c], {"pp": jnp.minimum(s + 1, pp - 1)})

    weight_copies = [
        pltpu.make_async_copy(wqkv_hbm, wqkv, w_sem.at[0]),
        pltpu.make_async_copy(wup_hbm, wup, w_sem.at[1]),
        pltpu.make_async_copy(wo_hbm, wod.at[pl.ds(0, qd)], w_sem.at[2]),
        pltpu.make_async_copy(wdn_hbm, wod.at[pl.ds(qd, ff)], w_sem.at[3]),
    ]

    @pl.when(s == 0)
    def _():
        def load(c, carry):
            pltpu.make_async_copy(x_hbm.at[c], xin.at[c], xin_sem.at[c]).start()
            return carry
        lax.fori_loop(0, nc, load, 0)

    for copy in weight_copies:
        copy.start()

    for way, alone in ((0, z == 0), (1, z == last)):
        @pl.when(alone)
        def _(way=way):
            for k in range(NR):
                rbuf[k, way, last - 1] = jnp.zeros(rbuf.shape[3:], rbuf.dtype)

    barrier = pltpu.get_barrier_semaphore()
    for there, to in ((has_left, neighbour(1)), (has_right, neighbour(0)), (has_prev, {"pp": jnp.maximum(s - 1, 0)}), (has_next, {"pp": jnp.minimum(s + 1, pp - 1)})):
        @pl.when(there)
        def _(to=to):
            pl.semaphore_signal(barrier, inc=1, device_id=to, device_id_type=MESH)
    pl.semaphore_wait(barrier, has_left.astype(jnp.int32) + has_right.astype(jnp.int32) + has_prev.astype(jnp.int32) + has_next.astype(jnp.int32))

    def on(cond, fn):
        pl.when(cond)(fn)

    def ag_start(c):
        pltpu.make_async_copy(x_hbm.at[c], xin.at[c], xin_sem.at[c]).wait()
        for way in (0, 1):
            on(ag_sends(0, way), ag_copy(c, 0, way).start)
        xfull[c % NX, z] = xin[c]

    def ag_hop(c, h):
        for way in (0, 1):
            on(ag_gets(h - 1, way), ag_copy(c, h - 1, way).wait_recv)
            if h < last:
                on(ag_sends(h, way), ag_copy(c, h, way).start)

    def ag_drain(c):
        for h in range(last):
            for way in (0, 1):
                on(ag_sends(h, way), ag_copy(c, h, way).wait_send)

    def rs_hop(c, h):
        for way in (0, 1):
            @pl.when(rs_sends_all(h, way))
            def _(way=way):
                if h > 0:
                    @pl.when(rs_gets(h - 1, way))
                    def _():
                        rs_copy(c, h - 1, way).wait_recv()
                        d = z + last - h if way == 0 else z - last + h
                        mine = part[c % NP, d].astype(jnp.float32)
                        part[c % NP, d] = (mine + rbuf[c % NR, way, h - 1].astype(jnp.float32)).astype(part.dtype)
                rs_copy(c, h, way).start()

    def rs_drain(c):
        for h in range(last):
            for way in (0, 1):
                on(rs_sends_all(h, way), rs_copy(c, h, way).wait_send)

    def finish(c):
        @pl.when(c >= NY)
        def _():
            out_copy(c - NY).wait()
            on(has_next, fwd_copy(c - NY).wait_send)
        for way in (0, 1):
            on(rs_gets(last - 1, way), rs_copy(c, last - 1, way).wait_recv)
        f32 = jnp.float32
        total = xin[c].astype(f32) + part[c % NP, z].astype(f32)
        total = total + rbuf[c % NR, 0, last - 1].astype(f32) + rbuf[c % NR, 1, last - 1].astype(f32)
        ybuf[c % NY] = total.astype(ybuf.dtype)
        on(has_next, fwd_copy(c).start)
        out_copy(c).start()

    lt = min(rb, 32)
    per_block = rb // lt

    def norms(c):
        def tile(t, carry):
            x_f32 = xfull[c % NX, t // per_block, pl.ds((t % per_block) * lt, lt)].astype(jnp.float32)
            row_mean = jnp.mean(x_f32, axis=-1, keepdims=True)
            centred = x_f32 - row_mean
            variance = jnp.mean(centred * centred, axis=-1, keepdims=True)
            unit = centred * lax.rsqrt(variance + LN_EPS)
            at = pl.ds(pl.multiple_of(t * lt, lt), lt)
            ha[at] = (unit * ln_ref[0:1] + ln_ref[1:2]).astype(ha.dtype)
            hm[at] = (unit * ln_ref[2:3] + ln_ref[3:4]).astype(hm.dtype)
            return carry
        lax.fori_loop(0, rows // lt, tile, 0, unroll=2)

    def cols(n):
        return pl.ds(pl.multiple_of(n * NT, NT), NT)

    per_tile = NT // hd

    def projections():
        def rotated(n, carry):
            y = jnp.dot(ha[...], wqkv[:, cols(n)], preferred_element_type=jnp.float32)
            for j in range(per_tile):
                head = y[:, j * hd:(j + 1) * hd]
                turned = head * cos_ref[...] + pltpu.roll(head, hd // 2, 1) * sin_ref[...]
                qkv[n * per_tile + j] = turned.astype(qkv.dtype)
            return carry
        lax.fori_loop(0, 2 * qd // NT, rotated, 0, unroll=2)

        def plain(n, carry):
            y = jnp.dot(ha[...], wqkv[:, cols(n)], preferred_element_type=jnp.float32)
            for j in range(per_tile):
                qkv[n * per_tile + j] = y[:, j * hd:(j + 1) * hd].astype(qkv.dtype)
            return carry
        lax.fori_loop(2 * qd // NT, 3 * qd // NT, plain, 0, unroll=True)

    def attention():
        for h in range(heads):
            scores = lax.dot_general(qkv[h], qkv[heads + h], (((1,), (1,)), ((), ())), preferred_element_type=jnp.float32) * (hd ** -0.5)
            floor = mask_ref[...]
            scores = jnp.where(floor == 0.0, scores, floor)
            raised = jnp.exp(scores - jnp.max(scores, axis=-1, keepdims=True))
            probs = (raised * (1.0 / jnp.sum(raised, axis=-1, keepdims=True))).astype(qkv.dtype)
            act[:, h * hd:(h + 1) * hd] = jnp.dot(probs, qkv[2 * heads + h], preferred_element_type=jnp.float32).astype(act.dtype)

    def mlp_up():
        def tile(n, carry):
            u = jnp.dot(hm[...], wup[:, cols(n)], preferred_element_type=jnp.float32)
            g = 0.5 * u * (1.0 + lax.erf(u * (0.5 ** 0.5)))
            act[:, pl.ds(pl.multiple_of(qd + n * NT, NT), NT)] = g.astype(act.dtype)
            return carry
        lax.fori_loop(0, ff // NT, tile, 0, unroll=2)

    def project_out(c):
        def tile(n, carry):
            o = jnp.dot(act[...], wod[:, cols(n)], preferred_element_type=jnp.float32).astype(part.dtype)
            for b in range(tp):
                part[c % NP, b, :, cols(n)] = o[b * rb:(b + 1) * rb]
            return carry
        lax.fori_loop(0, d_model // NT, tile, 0, unroll=2)

    def holds(c):
        return (c >= 0) & (c < nc)

    def slot(i, carry):
        @pl.when(holds(i))
        def _():
            ag_start(i)

        @pl.when(holds(i - 1))
        def _():
            ag_hop(i - 1, 2)

        @pl.when(holds(i - 4))
        def _():
            rs_drain(i - 4)

        @pl.when(holds(i - 2))
        def _():
            @pl.when(i == 2)
            def _():
                weight_copies[2].wait()
                weight_copies[3].wait()
            project_out(i - 2)
            rs_hop(i - 2, 0)

        @pl.when(holds(i - 3))
        def _():
            rs_hop(i - 3, 2)

        @pl.when(holds(i))
        def _():
            ag_hop(i, 1)

        @pl.when(holds(i - 1))
        def _():
            ag_hop(i - 1, 3)
            @pl.when(i == 1)
            def _():
                weight_copies[0].wait()
            norms(i - 1)
            projections()
            attention()

        @pl.when(holds(i - 2))
        def _():
            rs_hop(i - 2, 1)

        @pl.when(holds(i - 3))
        def _():
            finish(i - 3)

        @pl.when(holds(i - 2))
        def _():
            ag_drain(i - 2)

        @pl.when(holds(i - 1))
        def _():
            @pl.when(i == 1)
            def _():
                weight_copies[1].wait()
            mlp_up()
        return carry

    lax.fori_loop(0, nc + 4, slot, 0)

    for c in range(nc - NY, nc):
        out_copy(c).wait()
        on(has_next, fwd_copy(c).wait_send)


def solution(mesh):
    tp, pp = mesh.shape["tp"], mesh.shape["pp"]

    def stage_body(x_in, ln_params, w_q, w_k, w_v, w_o, w_up, w_down):
        num_micro, batch_dim, tok, d_model = x_in.shape
        heads, hd = w_k.shape[2:]
        ff = w_up.shape[2]
        seqs = batch_dim // CHUNKS_PER_MICRO
        nc = num_micro * CHUNKS_PER_MICRO
        rb = seqs * tok
        rows = tp * rb
        qd = heads * hd
        bf16, f32 = jnp.bfloat16, jnp.float32

        row = jnp.arange(rows)
        pos = row // rb * tok + row % tok
        seq = row % rb // tok
        cos_tab, sin_tab = rope_tables(tp * tok, hd)
        cos_rows = jnp.concatenate([cos_tab, cos_tab], axis=-1)[pos]
        sin_rows = jnp.concatenate([-sin_tab, sin_tab], axis=-1)[pos]
        same = seq[:, None] == seq[None, :]
        allowed = same & (pos[:, None] >= pos[None, :])
        mask = jnp.where(allowed, 0.0, jnp.where(same, -1e30, -3e38)).astype(f32)
        w_qkv = jnp.concatenate([w_q.reshape(d_model, qd), w_k.reshape(d_model, qd), w_v.reshape(d_model, qd)], axis=1)

        any_spec = pl.BlockSpec(memory_space=pl.ANY)
        vmem_spec = pl.BlockSpec(memory_space=pltpu.VMEM)
        dma = pltpu.SemaphoreType.DMA
        flops = 2 * num_micro * tp * batch_dim * tok * (3 * qd * d_model + qd * d_model + 2 * ff * d_model)
        out = pl.pallas_call(
            functools.partial(pipeline_kernel, (nc, tp, pp, heads, hd)),
            out_shape=jax.ShapeDtypeStruct((nc, rb, d_model), bf16),
            in_specs=[any_spec, vmem_spec, vmem_spec, vmem_spec, vmem_spec, any_spec, any_spec, any_spec, any_spec],
            out_specs=any_spec,
            scratch_shapes=[
                pltpu.VMEM((d_model, 3 * qd), bf16),
                pltpu.VMEM((d_model, ff), bf16),
                pltpu.VMEM((qd + ff, d_model), bf16),
                pltpu.VMEM((nc, rb, d_model), bf16),
                pltpu.VMEM((NX, tp, rb, d_model), bf16),
                pltpu.VMEM((NR, 2, tp - 1, rb, d_model), bf16),
                pltpu.VMEM((NP, tp, rb, d_model), bf16),
                pltpu.VMEM((rows, d_model), bf16),
                pltpu.VMEM((rows, d_model), bf16),
                pltpu.VMEM((3 * heads, rows, hd), bf16),
                pltpu.VMEM((rows, qd + ff), bf16),
                pltpu.VMEM((NY, rb, d_model), bf16),
                dma((4,)),
                dma((nc,)),
                dma((NS, 2, tp - 1)),
                dma((NS, 2, tp - 1)),
                dma((NS, 2, tp - 1)),
                dma((NS, 2, tp - 1)),
                dma((NY,)),
                dma((NY,)),
            ],
            compiler_params=pltpu.CompilerParams(collective_id=0, has_side_effects=True, vmem_limit_bytes=67043328),
            cost_estimate=pl.CostEstimate(flops=flops, bytes_accessed=50 * 2 ** 20, transcendentals=0),
            name="pipeline",
        )(x_in.reshape(nc, rb, d_model), ln_params[0], cos_rows, sin_rows, mask, w_qkv, w_o.reshape(qd, d_model), w_up[0], w_down[0])
        return out.reshape(1, num_micro, batch_dim, tok, d_model)

    in_specs = (P(None, "dp", "tp", None), P("pp", None, None), P("pp", None, "tp", None, None), P("pp", None, "tp", None), P("pp", None, "tp", None), P("pp", "tp", None, None, None), P("pp", None, "tp"), P("pp", "tp", None))
    return jax.shard_map(stage_body, mesh=mesh, in_specs=in_specs, out_specs=P("pp", None, "dp", "tp", None), check_vma=False)
```

```python
import functools

import jax
import jax.numpy as jnp
from jax import lax
from jax.experimental import pallas as pl
from jax.experimental.pallas import tpu as pltpu
from jax.sharding import PartitionSpec as P

LN_EPS = 1e-5
ROPE_BASE = 10000.0
CHUNKS_PER_MICRO = 8
NT = 256
NX, NR, NP, NS = 4, 4, 3, 4
TURN = (("gather0", 0), ("scatter1", 3), ("gather2", 1), ("up", 2), ("finish", 4), ("out", 2), ("gather1", 0), ("scatter0", 2), ("scatter2", 3), ("heads", 1))
MESH = pl.DeviceIdType.MESH


def rope_tables(seq_len, head_dim):
    positions = jnp.arange(seq_len, dtype=jnp.float32)
    inv_freq = ROPE_BASE ** (-2.0 * jnp.arange(head_dim // 2, dtype=jnp.float32) / head_dim)
    angles = positions[:, None] * inv_freq[None, :]
    return jnp.cos(angles), jnp.sin(angles)


def pipeline_kernel(dims, x_hbm, ln_ref, cos_ref, sin_ref, wq_hbm, wk_hbm, wv_hbm, wo_hbm, wup_hbm, wdn_hbm, xin,
                    wqkv, wup, wod, xfull, rbuf, part, ha, hm, qkv, act, mask_ref,
                    w_sem, xin_sem, ag_ss, ag_rs, rs_ss, rs_rs, fwd_sem):
    nc, tp, pp, heads, hd, tok = dims
    rb, d_model = xin.shape[1:]
    rows = tp * rb
    ff = wup.shape[1]
    qd = heads * hd
    last = tp - 1
    z = lax.axis_index("tp")
    s = lax.axis_index("pp")
    has_left, has_right = z > 0, z < last
    has_prev, has_next = s > 0, s < pp - 1

    def remote(src, dst, ss, rs, to):
        return pltpu.make_async_remote_copy(src_ref=src, dst_ref=dst, send_sem=ss, recv_sem=rs, device_id=to, device_id_type=MESH)

    def neighbour(way):
        return {"tp": jnp.minimum(z + 1, last) if way == 0 else jnp.maximum(z - 1, 0)}

    def ag_copy(c, h, way):
        b = jnp.clip(z - h if way == 0 else z + h, 0, last)
        src = xin.at[c] if h == 0 else xfull.at[c % NX, b]
        return remote(src, xfull.at[c % NX, b], ag_ss.at[c % NS, way, h], ag_rs.at[c % NS, way, h], neighbour(way))

    def ag_sends(h, way):
        return has_right & (z >= h) if way == 0 else has_left & (z + h <= last)

    def ag_gets(h, way):
        return z - 1 - h >= 0 if way == 0 else z + 1 + h <= last

    def rs_copy(c, h, way):
        d = jnp.clip(z + last - h if way == 0 else z - last + h, 0, last)
        return remote(part.at[c % NP, d], rbuf.at[c % NR, way, h], rs_ss.at[c % NS, way, h], rs_rs.at[c % NS, way, h], neighbour(way))

    def rs_sends(h, way):
        return z <= h if way == 0 else last - z <= h

    def rs_sends_all(h, way):
        return rs_sends(h, way) & (has_right if way == 0 else has_left)

    def rs_gets(h, way):
        return has_left & (z - 1 <= h) if way == 0 else has_right & (last - 1 - z <= h)

    def fwd_copy(c):
        return remote(xin.at[c], xin.at[c], fwd_sem.at[c], xin_sem.at[c], {"pp": jnp.minimum(s + 1, pp - 1)})

    weight_copies = [
        pltpu.make_async_copy(wq_hbm, wqkv.at[:, pl.ds(0, qd)], w_sem.at[0]),
        pltpu.make_async_copy(wk_hbm, wqkv.at[:, pl.ds(qd, qd)], w_sem.at[1]),
        pltpu.make_async_copy(wv_hbm, wqkv.at[:, pl.ds(2 * qd, qd)], w_sem.at[2]),
        pltpu.make_async_copy(wup_hbm, wup, w_sem.at[3]),
        pltpu.make_async_copy(wo_hbm, wod.at[pl.ds(0, qd)], w_sem.at[4]),
        pltpu.make_async_copy(wdn_hbm, wod.at[pl.ds(qd, ff)], w_sem.at[5]),
    ]

    @pl.when(s == 0)
    def _():
        def load(c, carry):
            pltpu.make_async_copy(x_hbm.at[c], xin.at[c], xin_sem.at[c]).start()
            return carry
        lax.fori_loop(0, nc, load, 0)

    for copy in weight_copies:
        copy.start()

    for way, alone in ((0, z == 0), (1, z == last)):
        @pl.when(alone)
        def _(way=way):
            for k in range(NR):
                rbuf[k, way, last - 1] = jnp.zeros(rbuf.shape[3:], rbuf.dtype)

    row = lax.broadcasted_iota(jnp.int32, (rows, rows), 0)
    col = lax.broadcasted_iota(jnp.int32, (rows, rows), 1)
    same = row % rb // tok == col % rb // tok
    later = row // rb * tok + row % tok >= col // rb * tok + col % tok
    mask_ref[...] = jnp.where(same, jnp.where(later, 0.0, -1e30), -3e38)

    barrier = pltpu.get_barrier_semaphore()
    for there, to in ((has_left, neighbour(1)), (has_right, neighbour(0)), (has_prev, {"pp": jnp.maximum(s - 1, 0)}), (has_next, {"pp": jnp.minimum(s + 1, pp - 1)})):
        @pl.when(there)
        def _(to=to):
            pl.semaphore_signal(barrier, inc=1, device_id=to, device_id_type=MESH)
    pl.semaphore_wait(barrier, has_left.astype(jnp.int32) + has_right.astype(jnp.int32) + has_prev.astype(jnp.int32) + has_next.astype(jnp.int32))

    def on(cond, fn):
        pl.when(cond)(fn)

    def ag_start(c):
        pltpu.make_async_copy(x_hbm.at[c], xin.at[c], xin_sem.at[c]).wait()
        for way in (0, 1):
            on(ag_sends(0, way), ag_copy(c, 0, way).start)
        xfull[c % NX, z] = xin[c]

    def ag_hop(c, h):
        for way in (0, 1):
            on(ag_gets(h - 1, way), ag_copy(c, h - 1, way).wait_recv)
            if h < last:
                on(ag_sends(h, way), ag_copy(c, h, way).start)

    def ag_drain(c):
        for h in range(last):
            for way in (0, 1):
                on(ag_sends(h, way), ag_copy(c, h, way).wait_send)

    def rs_hop(c, h):
        for way in (0, 1):
            @pl.when(rs_sends_all(h, way))
            def _(way=way):
                if h > 0:
                    @pl.when(rs_gets(h - 1, way))
                    def _():
                        rs_copy(c, h - 1, way).wait_recv()
                        d = z + last - h if way == 0 else z - last + h
                        mine = part[c % NP, d].astype(jnp.float32)
                        part[c % NP, d] = (mine + rbuf[c % NR, way, h - 1].astype(jnp.float32)).astype(part.dtype)
                rs_copy(c, h, way).start()

    def rs_drain(c):
        for h in range(last):
            for way in (0, 1):
                on(rs_sends_all(h, way), rs_copy(c, h, way).wait_send)

    def finish(c):
        for way in (0, 1):
            on(rs_gets(last - 1, way), rs_copy(c, last - 1, way).wait_recv)
        f32 = jnp.float32
        total = xin[c].astype(f32) + part[c % NP, z].astype(f32)
        total = total + rbuf[c % NR, 0, last - 1].astype(f32) + rbuf[c % NR, 1, last - 1].astype(f32)
        xin[c] = total.astype(xin.dtype)
        on(has_next, fwd_copy(c).start)

    lt = min(rb, 32)
    per_block = rb // lt

    def norms(c):
        def tile(t, carry):
            x_f32 = xfull[c % NX, t // per_block, pl.ds((t % per_block) * lt, lt)].astype(jnp.float32)
            row_mean = jnp.mean(x_f32, axis=-1, keepdims=True)
            centred = x_f32 - row_mean
            variance = jnp.mean(centred * centred, axis=-1, keepdims=True)
            unit = centred * lax.rsqrt(variance + LN_EPS)
            at = pl.ds(pl.multiple_of(t * lt, lt), lt)
            ha[at] = (unit * ln_ref[0:1] + ln_ref[1:2]).astype(ha.dtype)
            hm[at] = (unit * ln_ref[2:3] + ln_ref[3:4]).astype(hm.dtype)
            return carry
        lax.fori_loop(0, rows // lt, tile, 0, unroll=2)

    def cols(n):
        return pl.ds(pl.multiple_of(n * NT, NT), NT)

    per_tile = NT // hd

    def projections():
        def rotated(n, carry):
            y = jnp.dot(ha[...], wqkv[:, cols(n)], preferred_element_type=jnp.float32)
            for j in range(per_tile):
                head = y[:, j * hd:(j + 1) * hd]
                turned = head * cos_ref[...] + pltpu.roll(head, hd // 2, 1) * sin_ref[...]
                qkv[n * per_tile + j] = turned.astype(qkv.dtype)
            return carry
        lax.fori_loop(0, 2 * qd // NT, rotated, 0, unroll=2)

        def plain(n, carry):
            y = jnp.dot(ha[...], wqkv[:, cols(n)], preferred_element_type=jnp.float32)
            for j in range(per_tile):
                qkv[n * per_tile + j] = y[:, j * hd:(j + 1) * hd].astype(qkv.dtype)
            return carry
        lax.fori_loop(2 * qd // NT, 3 * qd // NT, plain, 0, unroll=True)

    def attention():
        for h in range(heads):
            scores = lax.dot_general(qkv[h], qkv[heads + h], (((1,), (1,)), ((), ())), preferred_element_type=jnp.float32) * (hd ** -0.5)
            floor = mask_ref[...]
            scores = jnp.where(floor == 0.0, scores, floor)
            raised = jnp.exp(scores - jnp.max(scores, axis=-1, keepdims=True))
            probs = (raised * (1.0 / jnp.sum(raised, axis=-1, keepdims=True))).astype(qkv.dtype)
            act[:, h * hd:(h + 1) * hd] = jnp.dot(probs, qkv[2 * heads + h], preferred_element_type=jnp.float32).astype(act.dtype)

    def mlp_up():
        def tile(n, carry):
            u = jnp.dot(hm[...], wup[:, cols(n)], preferred_element_type=jnp.float32)
            g = 0.5 * u * (1.0 + lax.erf(u * (0.5 ** 0.5)))
            act[:, pl.ds(pl.multiple_of(qd + n * NT, NT), NT)] = g.astype(act.dtype)
            return carry
        lax.fori_loop(0, ff // NT, tile, 0, unroll=2)

    def project_out(c):
        def tile(n, carry):
            o = jnp.dot(act[...], wod[:, cols(n)], preferred_element_type=jnp.float32).astype(part.dtype)
            for b in range(tp):
                part[c % NP, b, :, cols(n)] = o[b * rb:(b + 1) * rb]
            return carry
        lax.fori_loop(0, d_model // NT, tile, 0, unroll=2)

    def holds(c):
        return (c >= 0) & (c < nc)

    def weights_ready(c, first, count):
        @pl.when(c == 0)
        def _():
            for copy in weight_copies[first:first + count]:
                copy.wait()

    def heads_step(c):
        ag_hop(c, last)
        weights_ready(c, 0, 3)
        norms(c)
        projections()
        attention()

    def up_step(c):
        weights_ready(c, 3, 1)
        mlp_up()

    def out_step(c):
        weights_ready(c, 4, 2)
        ag_drain(c)
        on(c >= NP, lambda: rs_drain(c - NP))
        project_out(c)

    steps = {
        "gather0": ag_start,
        "gather1": lambda c: ag_hop(c, 1),
        "gather2": lambda c: ag_hop(c, 2),
        "heads": heads_step,
        "up": up_step,
        "out": out_step,
        "scatter0": lambda c: rs_hop(c, 0),
        "scatter1": lambda c: rs_hop(c, 1),
        "scatter2": lambda c: rs_hop(c, 2),
        "finish": finish,
    }

    def turn(i, carry):
        for name, behind in TURN:
            c = i - behind
            on((c >= 0) & (c < nc), functools.partial(steps[name], c))
        return carry

    lax.fori_loop(0, nc + max(behind for _, behind in TURN), turn, 0)

    for c in range(nc - NP, nc):
        rs_drain(c)

    @pl.when(has_next)
    def _():
        def sent(c, carry):
            fwd_copy(c).wait_send()
            return carry
        lax.fori_loop(0, nc, sent, 0)


def solution(mesh):
    tp, pp = mesh.shape["tp"], mesh.shape["pp"]

    def stage_body(x_in, ln_params, w_q, w_k, w_v, w_o, w_up, w_down):
        num_micro, batch_dim, tok, d_model = x_in.shape
        heads, hd = w_k.shape[2:]
        ff = w_up.shape[2]
        seqs = batch_dim // CHUNKS_PER_MICRO
        nc = num_micro * CHUNKS_PER_MICRO
        rb = seqs * tok
        rows = tp * rb
        qd = heads * hd
        bf16, f32 = jnp.bfloat16, jnp.float32

        cos_tab, sin_tab = rope_tables(tp * tok, hd)
        per_row = lambda t: jnp.broadcast_to(t.reshape(tp, 1, tok, hd), (tp, seqs, tok, hd)).reshape(rows, hd)
        cos_rows = per_row(jnp.concatenate([cos_tab, cos_tab], axis=-1))
        sin_rows = per_row(jnp.concatenate([-sin_tab, sin_tab], axis=-1))

        any_spec = pl.BlockSpec(memory_space=pl.ANY)
        vmem_spec = pl.BlockSpec(memory_space=pltpu.VMEM)
        dma = pltpu.SemaphoreType.DMA
        flops = 2 * num_micro * tp * batch_dim * tok * (3 * qd * d_model + qd * d_model + 2 * ff * d_model)
        out = pl.pallas_call(
            functools.partial(pipeline_kernel, (nc, tp, pp, heads, hd, tok)),
            out_shape=pltpu.VMEM((nc, rb, d_model), bf16),
            in_specs=[any_spec, vmem_spec, vmem_spec, vmem_spec] + [any_spec] * 6,
            out_specs=vmem_spec,
            scratch_shapes=[
                pltpu.VMEM((d_model, 3 * qd), bf16),
                pltpu.VMEM((d_model, ff), bf16),
                pltpu.VMEM((qd + ff, d_model), bf16),
                pltpu.VMEM((NX, tp, rb, d_model), bf16),
                pltpu.VMEM((NR, 2, tp - 1, rb, d_model), bf16),
                pltpu.VMEM((NP, tp, rb, d_model), bf16),
                pltpu.VMEM((rows, d_model), bf16),
                pltpu.VMEM((rows, d_model), bf16),
                pltpu.VMEM((3 * heads, rows, hd), bf16),
                pltpu.VMEM((rows, qd + ff), bf16),
                pltpu.VMEM((rows, rows), f32),
                dma((6,)),
                dma((nc,)),
                dma((NS, 2, tp - 1)),
                dma((NS, 2, tp - 1)),
                dma((NS, 2, tp - 1)),
                dma((NS, 2, tp - 1)),
                dma((nc,)),
            ],
            compiler_params=pltpu.CompilerParams(collective_id=0, has_side_effects=True, vmem_limit_bytes=52 * 2 ** 20),
            cost_estimate=pl.CostEstimate(flops=flops, bytes_accessed=50 * 2 ** 20, transcendentals=0),
            name="pipeline",
        )(x_in.reshape(nc, rb, d_model), ln_params[0], cos_rows, sin_rows, w_q.reshape(d_model, qd), w_k.reshape(d_model, qd), w_v.reshape(d_model, qd), w_o.reshape(qd, d_model), w_up[0], w_down[0])
        return out.reshape(1, num_micro, batch_dim, tok, d_model)

    in_specs = (P(None, "dp", "tp", None), P("pp", None, None), P("pp", None, "tp", None, None), P("pp", None, "tp", None), P("pp", None, "tp", None), P("pp", "tp", None, None, None), P("pp", None, "tp"), P("pp", "tp", None))
    return jax.shard_map(stage_body, mesh=mesh, in_specs=in_specs, out_specs=P("pp", None, "dp", "tp", None), check_vma=False)
```

```python
import functools

import jax
import jax.numpy as jnp
from jax import lax
from jax.experimental import pallas as pl
from jax.experimental.pallas import tpu as pltpu
from jax.sharding import PartitionSpec as P

LN_EPS = 1e-5
ROPE_BASE = 10000.0
CHUNKS_PER_MICRO = 8
NT = 256
NX, NR, NP, NS = 4, 4, 3, 4
LATE = 3
TURN = (("gather0", 0), ("scatter1", 3), ("gather2", 1), ("up", 2), ("finish", 4), ("out", 2), ("gather1", 0), ("scatter0", 2), ("scatter2", 3), ("heads", 1))
MESH = pl.DeviceIdType.MESH


def rope_tables(seq_len, head_dim):
    positions = jnp.arange(seq_len, dtype=jnp.float32)
    inv_freq = ROPE_BASE ** (-2.0 * jnp.arange(head_dim // 2, dtype=jnp.float32) / head_dim)
    angles = positions[:, None] * inv_freq[None, :]
    return jnp.cos(angles), jnp.sin(angles)


def pipeline_kernel(dims, x_hbm, cos_tab, sin_tab, wq_hbm, wk_hbm, wv_hbm, ln_hbm, wup_hbm, wo_hbm, wdn_hbm,
                    xin, lq_hbm, lk_hbm, lv_hbm, lln_hbm, lup_hbm, lo_hbm, ldn_hbm,
                    wqkv, ln_ref, wup, wod, xlate, xfull, rbuf, part, ha, hm, qkv, act, mask_ref, cos_ref, sin_ref,
                    w_sem, xin_sem, ag_ss, ag_rs, rs_ss, rs_rs, fwd_sem, home_sem, lw_ss, lw_rs):
    nc, nl, tp, pp, heads, hd, tok = dims
    rb, d_model = xin.shape[1:]
    rows = tp * rb
    ff = wup.shape[1]
    qd = heads * hd
    last = tp - 1
    z = lax.axis_index("tp")
    s = lax.axis_index("pp")
    has_left, has_right = z > 0, z < last
    has_prev, has_next = s > 0, s < pp - 1
    half = pp // 2
    front = s < half

    def remote(src, dst, ss, rs, to):
        return pltpu.make_async_remote_copy(src_ref=src, dst_ref=dst, send_sem=ss, recv_sem=rs, device_id=to, device_id_type=MESH)

    def neighbour(way):
        return {"tp": jnp.minimum(z + 1, last) if way == 0 else jnp.maximum(z - 1, 0)}

    def ag_copy(c, h, way, first=None):
        b = jnp.clip(z - h if way == 0 else z + h, 0, last)
        src = (first if first is not None else xin.at[0]) if h == 0 else xfull.at[c % NX, b]
        return remote(src, xfull.at[c % NX, b], ag_ss.at[c % NS, way, h], ag_rs.at[c % NS, way, h], neighbour(way))

    def ag_sends(h, way):
        return has_right & (z >= h) if way == 0 else has_left & (z + h <= last)

    def ag_gets(h, way):
        return z - 1 - h >= 0 if way == 0 else z + 1 + h <= last

    def rs_copy(c, h, way):
        d = jnp.clip(z + last - h if way == 0 else z - last + h, 0, last)
        return remote(part.at[c % NP, d], rbuf.at[c % NR, way, h], rs_ss.at[c % NS, way, h], rs_rs.at[c % NS, way, h], neighbour(way))

    def rs_sends(h, way):
        return z <= h if way == 0 else last - z <= h

    def rs_sends_all(h, way):
        return rs_sends(h, way) & (has_right if way == 0 else has_left)

    def rs_gets(h, way):
        return has_left & (z - 1 <= h) if way == 0 else has_right & (last - 1 - z <= h)

    def fwd_copy(v):
        return remote(xin.at[v], xin.at[v], fwd_sem.at[v], xin_sem.at[v], {"pp": jnp.minimum(s + 1, pp - 1)})

    def turn_copy(v):
        return remote(xin.at[v], xlate.at[v - (nc - nl)], fwd_sem.at[v], xin_sem.at[v + nl], {"pp": 0})

    def next_late_copy(v):
        return remote(xlate.at[v - nc], xlate.at[v - nc], fwd_sem.at[v], xin_sem.at[v], {"pp": jnp.minimum(s + 1, pp - 1)})

    def home_copy(v):
        return remote(xlate.at[v - nc], xin.at[v - nl], home_sem.at[v - nc], xin_sem.at[v - nl], {"pp": jnp.minimum(s + half, pp - 1)})

    own = [wq_hbm, wk_hbm, wv_hbm, ln_hbm, wup_hbm, wo_hbm, wdn_hbm]
    late = [lq_hbm, lk_hbm, lv_hbm, lln_hbm, lup_hbm, lo_hbm, ldn_hbm]
    held = [wqkv.at[:, pl.ds(0, qd)], wqkv.at[:, pl.ds(qd, qd)], wqkv.at[:, pl.ds(2 * qd, qd)], ln_ref, wup, wod.at[pl.ds(0, qd)], wod.at[pl.ds(qd, ff)]]
    weight_copies = [pltpu.make_async_copy(src, dst, w_sem.at[k]) for k, (src, dst) in enumerate(zip(own, held))]
    swap_copies = [pltpu.make_async_copy(src, dst, w_sem.at[k]) for k, (src, dst) in enumerate(zip(late, held))]
    lend_copies = [remote(src, dst, lw_ss.at[k], lw_rs.at[k], {"pp": jnp.maximum(s - half, 0)}) for k, (src, dst) in enumerate(zip(own, late))]

    @pl.when(s == 0)
    def _():
        def load(c, carry):
            pltpu.make_async_copy(x_hbm.at[c], xin.at[c], xin_sem.at[c]).start()
            return carry
        lax.fori_loop(0, nc, load, 0)

    for copy in weight_copies:
        copy.start()

    for way, alone in ((0, z == 0), (1, z == last)):
        @pl.when(alone)
        def _(way=way):
            for k in range(NR):
                rbuf[k, way, last - 1] = jnp.zeros(rbuf.shape[3:], rbuf.dtype)

    row = lax.broadcasted_iota(jnp.int32, (rows, rows), 0)
    col = lax.broadcasted_iota(jnp.int32, (rows, rows), 1)
    same = row % rb // tok == col % rb // tok
    later = row // rb * tok + row % tok >= col // rb * tok + col % tok
    mask_ref[...] = jnp.where(same, jnp.where(later, 0.0, -1e30), -3e38)
    for b in range(tp):
        for q in range(rb // tok):
            to, of = slice(b * rb + q * tok, b * rb + (q + 1) * tok), slice(b * tok, (b + 1) * tok)
            cos_ref[to] = cos_tab[of]
            sin_ref[to] = sin_tab[of]

    barrier = pltpu.get_barrier_semaphore()
    for there, to in ((has_left, neighbour(1)), (has_right, neighbour(0)), (has_prev, {"pp": jnp.maximum(s - 1, 0)}), (has_next, {"pp": jnp.minimum(s + 1, pp - 1)}), (front, {"pp": jnp.minimum(s + half, pp - 1)}), (s >= half, {"pp": jnp.maximum(s - half, 0)})):
        @pl.when(there)
        def _(to=to):
            pl.semaphore_signal(barrier, inc=1, device_id=to, device_id_type=MESH)
    pl.semaphore_wait(barrier, has_left.astype(jnp.int32) + has_right.astype(jnp.int32) + has_prev.astype(jnp.int32) + has_next.astype(jnp.int32) + 1)

    @pl.when(s >= half)
    def _():
        for copy in lend_copies:
            copy.start()

    def on(cond, fn):
        pl.when(cond)(fn)

    def in_its_place(c, fn):
        on(c < nc, lambda: fn(xin.at[c]))
        on(c >= nc, lambda: fn(xlate.at[c - nc]))

    def ag_start(c):
        pltpu.make_async_copy(x_hbm.at[0], xin.at[0], xin_sem.at[c]).wait()

        def send(place):
            for way in (0, 1):
                on(ag_sends(0, way), ag_copy(c, 0, way, place).start)
            xfull[c % NX, z] = place[...]
        in_its_place(c, send)

    def ag_hop(c, h):
        for way in (0, 1):
            on(ag_gets(h - 1, way), ag_copy(c, h - 1, way).wait_recv)
            if h < last:
                on(ag_sends(h, way), ag_copy(c, h, way).start)

    def ag_drain(c):
        for h in range(last):
            for way in (0, 1):
                on(ag_sends(h, way), ag_copy(c, h, way).wait_send)

    def rs_hop(c, h):
        for way in (0, 1):
            @pl.when(rs_sends_all(h, way))
            def _(way=way):
                if h > 0:
                    @pl.when(rs_gets(h - 1, way))
                    def _():
                        rs_copy(c, h - 1, way).wait_recv()
                        d = z + last - h if way == 0 else z - last + h
                        mine = part[c % NP, d].astype(jnp.float32)
                        part[c % NP, d] = (mine + rbuf[c % NR, way, h - 1].astype(jnp.float32)).astype(part.dtype)
                rs_copy(c, h, way).start()

    def rs_drain(c):
        for h in range(last):
            for way in (0, 1):
                on(rs_sends_all(h, way), rs_copy(c, h, way).wait_send)

    def finish(c):
        for way in (0, 1):
            on(rs_gets(last - 1, way), rs_copy(c, last - 1, way).wait_recv)
        f32 = jnp.float32

        def add(place):
            total = place[...].astype(f32) + part[c % NP, z].astype(f32)
            total = total + rbuf[c % NR, 0, last - 1].astype(f32) + rbuf[c % NR, 1, last - 1].astype(f32)
            place[...] = total.astype(xin.dtype)
        in_its_place(c, add)
        turns = (s == half - 1) & (c >= nc - nl)
        on(has_next & (c < nc) & ~turns, lambda: fwd_copy(c).start())
        on(turns & (c < nc), lambda: turn_copy(c).start())
        on((s < half - 1) & (c >= nc), lambda: next_late_copy(c).start())
        on(front & (c >= nc), lambda: home_copy(c).start())

    lt = min(rb, 32)
    per_block = rb // lt

    def norms(c):
        def tile(t, carry):
            x_f32 = xfull[c % NX, t // per_block, pl.ds((t % per_block) * lt, lt)].astype(jnp.float32)
            row_mean = jnp.mean(x_f32, axis=-1, keepdims=True)
            centred = x_f32 - row_mean
            variance = jnp.mean(centred * centred, axis=-1, keepdims=True)
            unit = centred * lax.rsqrt(variance + LN_EPS)
            at = pl.ds(pl.multiple_of(t * lt, lt), lt)
            ha[at] = (unit * ln_ref[0:1] + ln_ref[1:2]).astype(ha.dtype)
            hm[at] = (unit * ln_ref[2:3] + ln_ref[3:4]).astype(hm.dtype)
            return carry
        lax.fori_loop(0, rows // lt, tile, 0, unroll=2)

    def cols(n):
        return pl.ds(pl.multiple_of(n * NT, NT), NT)

    per_tile = NT // hd

    def projections():
        def rotated(n, carry):
            y = jnp.dot(ha[...], wqkv[:, cols(n)], preferred_element_type=jnp.float32)
            for j in range(per_tile):
                head = y[:, j * hd:(j + 1) * hd]
                turned = head * cos_ref[...] + pltpu.roll(head, hd // 2, 1) * sin_ref[...]
                qkv[n * per_tile + j] = turned.astype(qkv.dtype)
            return carry
        lax.fori_loop(0, 2 * qd // NT, rotated, 0, unroll=2)

        def plain(n, carry):
            y = jnp.dot(ha[...], wqkv[:, cols(n)], preferred_element_type=jnp.float32)
            for j in range(per_tile):
                qkv[n * per_tile + j] = y[:, j * hd:(j + 1) * hd].astype(qkv.dtype)
            return carry
        lax.fori_loop(2 * qd // NT, 3 * qd // NT, plain, 0, unroll=True)

    def attention():
        for h in range(heads):
            scores = lax.dot_general(qkv[h], qkv[heads + h], (((1,), (1,)), ((), ())), preferred_element_type=jnp.float32) * (hd ** -0.5)
            floor = mask_ref[...]
            scores = jnp.where(floor == 0.0, scores, floor)
            raised = jnp.exp(scores - jnp.max(scores, axis=-1, keepdims=True))
            probs = (raised * (1.0 / jnp.sum(raised, axis=-1, keepdims=True))).astype(qkv.dtype)
            act[:, h * hd:(h + 1) * hd] = jnp.dot(probs, qkv[2 * heads + h], preferred_element_type=jnp.float32).astype(act.dtype)

    def mlp_up():
        def tile(n, carry):
            u = jnp.dot(hm[...], wup[:, cols(n)], preferred_element_type=jnp.float32)
            g = 0.5 * u * (1.0 + lax.erf(u * (0.5 ** 0.5)))
            act[:, pl.ds(pl.multiple_of(qd + n * NT, NT), NT)] = g.astype(act.dtype)
            return carry
        lax.fori_loop(0, ff // NT, tile, 0, unroll=2)

    def project_out(c):
        def tile(n, carry):
            o = jnp.dot(act[...], wod[:, cols(n)], preferred_element_type=jnp.float32).astype(part.dtype)
            for b in range(tp):
                part[c % NP, b, :, cols(n)] = o[b * rb:(b + 1) * rb]
            return carry
        lax.fori_loop(0, d_model // NT, tile, 0, unroll=2)

    def holds(c):
        return (c >= 0) & (c < nc)

    def weights_ready(c, ks):
        @pl.when((c == 0) | (c == nc))
        def _():
            for k in ks:
                weight_copies[k].wait()

    def swap_weights(c, ks):
        @pl.when(front & (c == nc - 1))
        def _():
            for k in ks:
                lend_copies[k].wait_recv()
                swap_copies[k].start()

    def heads_step(c, lo):
        ag_hop(c, last)
        weights_ready(c, (0, 1, 2, 3))
        norms(c)
        projections()
        swap_weights(c, (0, 1, 2, 3))
        attention()

    def up_step(c, lo):
        weights_ready(c, (4,))
        mlp_up()
        swap_weights(c, (4,))

    def out_step(c, lo):
        weights_ready(c, (5, 6))
        ag_drain(c)
        on(c - NP >= lo, lambda: rs_drain(c - NP))
        project_out(c)
        swap_weights(c, (5, 6))

    steps = {
        "gather0": lambda c, lo: ag_start(c),
        "gather1": lambda c, lo: ag_hop(c, 1),
        "gather2": lambda c, lo: ag_hop(c, 2),
        "heads": heads_step,
        "up": up_step,
        "out": out_step,
        "scatter0": lambda c, lo: rs_hop(c, 0),
        "scatter1": lambda c, lo: rs_hop(c, 1),
        "scatter2": lambda c, lo: rs_hop(c, 2),
        "finish": lambda c, lo: finish(c),
    }
    span = max(behind for _, behind in TURN)

    def segment(k, carry):
        lo = k * nc
        hi = jnp.where(front, jnp.where(k == 0, nc, nc + nl), jnp.where(k == 0, nc - nl, nc))

        def turn(i, carry):
            for name, behind in TURN:
                c = i - behind
                on((c >= lo) & (c < hi), functools.partial(steps[name], c, lo))
            return carry

        lax.fori_loop(lo, jnp.where(hi > lo, hi + span, lo), turn, 0)
        for back in range(1, NP + 1):
            on(hi - back >= lo, lambda: rs_drain(hi - back))
        return carry

    lax.fori_loop(0, 2, segment, 0)

    @pl.when(has_next)
    def _():
        def sent(v, carry):
            fwd_copy(v).wait_send()
            return carry
        lax.fori_loop(0, jnp.where(s < half - 1, nc, nc - nl), sent, 0)

    for k in range(nl):
        on(s == half - 1, turn_copy(nc - nl + k).wait_send)
        on(s < half - 1, next_late_copy(nc + k).wait_send)
        on(front, home_copy(nc + k).wait_send)

    @pl.when(s >= half)
    def _():
        for copy in lend_copies:
            copy.wait_send()
        for k in range(nl):
            c = nc - nl + k
            pltpu.make_async_copy(x_hbm.at[0], xin.at[0], xin_sem.at[c]).wait()


def solution(mesh):
    tp, pp = mesh.shape["tp"], mesh.shape["pp"]

    def stage_body(x_in, ln_params, w_q, w_k, w_v, w_o, w_up, w_down):
        num_micro, batch_dim, tok, d_model = x_in.shape
        heads, hd = w_k.shape[2:]
        ff = w_up.shape[2]
        seqs = batch_dim // CHUNKS_PER_MICRO
        nc = num_micro * CHUNKS_PER_MICRO
        rb = seqs * tok
        rows = tp * rb
        qd = heads * hd
        bf16, f32 = jnp.bfloat16, jnp.float32

        cos_tab, sin_tab = rope_tables(tp * tok, hd)
        cos_full = jnp.concatenate([cos_tab, cos_tab], axis=-1)
        sin_full = jnp.concatenate([-sin_tab, sin_tab], axis=-1)

        any_spec = pl.BlockSpec(memory_space=pl.ANY)
        vmem_spec = pl.BlockSpec(memory_space=pltpu.VMEM)
        dma = pltpu.SemaphoreType.DMA
        flops = 2 * num_micro * tp * batch_dim * tok * (3 * qd * d_model + qd * d_model + 2 * ff * d_model)
        out, *_ = pl.pallas_call(
            functools.partial(pipeline_kernel, (nc, LATE, tp, pp, heads, hd, tok)),
            out_shape=[pltpu.VMEM((nc, rb, d_model), bf16)] + [jax.ShapeDtypeStruct((d_model, qd), bf16)] * 3 + [
                jax.ShapeDtypeStruct((4, d_model), f32), jax.ShapeDtypeStruct((d_model, ff), bf16),
                jax.ShapeDtypeStruct((qd, d_model), bf16), jax.ShapeDtypeStruct((ff, d_model), bf16)],
            in_specs=[any_spec, vmem_spec, vmem_spec] + [any_spec] * 7,
            out_specs=[vmem_spec] + [any_spec] * 7,
            scratch_shapes=[
                pltpu.VMEM((d_model, 3 * qd), bf16),
                pltpu.VMEM((4, d_model), f32),
                pltpu.VMEM((d_model, ff), bf16),
                pltpu.VMEM((qd + ff, d_model), bf16),
                pltpu.VMEM((LATE, rb, d_model), bf16),
                pltpu.VMEM((NX, tp, rb, d_model), bf16),
                pltpu.VMEM((NR, 2, tp - 1, rb, d_model), bf16),
                pltpu.VMEM((NP, tp, rb, d_model), bf16),
                pltpu.VMEM((rows, d_model), bf16),
                pltpu.VMEM((rows, d_model), bf16),
                pltpu.VMEM((3 * heads, rows, hd), bf16),
                pltpu.VMEM((rows, qd + ff), bf16),
                pltpu.VMEM((rows, rows), f32),
                pltpu.VMEM((rows, hd), f32),
                pltpu.VMEM((rows, hd), f32),
                dma((7,)),
                dma((nc + LATE,)),
                dma((NS, 2, tp - 1)),
                dma((NS, 2, tp - 1)),
                dma((NS, 2, tp - 1)),
                dma((NS, 2, tp - 1)),
                dma((nc + LATE,)),
                dma((LATE,)),
                dma((7,)),
                dma((7,)),
            ],
            compiler_params=pltpu.CompilerParams(collective_id=0, has_side_effects=True, vmem_limit_bytes=52 * 2 ** 20),
            cost_estimate=pl.CostEstimate(flops=flops, bytes_accessed=50 * 2 ** 20, transcendentals=0),
            name="pipeline",
        )(x_in.reshape(nc, rb, d_model), cos_full, sin_full, w_q.reshape(d_model, qd), w_k.reshape(d_model, qd), w_v.reshape(d_model, qd), ln_params[0], w_up[0], w_o.reshape(qd, d_model), w_down[0])
        return out.reshape(1, num_micro, batch_dim, tok, d_model)

    in_specs = (P(None, "dp", "tp", None), P("pp", None, None), P("pp", None, "tp", None, None), P("pp", None, "tp", None), P("pp", None, "tp", None), P("pp", "tp", None, None, None), P("pp", None, "tp"), P("pp", "tp", None))
    return jax.shard_map(stage_body, mesh=mesh, in_specs=in_specs, out_specs=P("pp", None, "dp", "tp", None), check_vma=False)
```

```python
import functools

import jax
import jax.numpy as jnp
from jax import lax
from jax.experimental import pallas as pl
from jax.experimental.pallas import tpu as pltpu
from jax.sharding import PartitionSpec as P

LN_EPS = 1e-5
ROPE_BASE = 10000.0
CHUNKS_PER_MICRO = 8
NT = 256
NX, NR, NP, NS = 4, 4, 3, 4
LATE = 3
AHEAD = 4
TURN = (("gather0", 0), ("scatter1", 3), ("gather2", 1), ("up", 2), ("finish", 4), ("out", 2), ("scatter0", 2), ("gather1", 0), ("arrive", 1), ("scatter2", 3), ("heads", 1))
MESH = pl.DeviceIdType.MESH


def rope_tables(seq_len, head_dim):
    positions = jnp.arange(seq_len, dtype=jnp.float32)
    inv_freq = ROPE_BASE ** (-2.0 * jnp.arange(head_dim // 2, dtype=jnp.float32) / head_dim)
    angles = positions[:, None] * inv_freq[None, :]
    return jnp.cos(angles), jnp.sin(angles)


def pipeline_kernel(dims, x_hbm, cos_tab, sin_tab, wq_hbm, wk_hbm, wv_hbm, ln_hbm, wup_hbm, wo_hbm, wdn_hbm,
                    xin, lq_hbm, lk_hbm, lv_hbm, lln_hbm, lup_hbm, lo_hbm, ldn_hbm,
                    wqkv, ln_ref, wup, wod, xlate, xfull, rbuf, part, ha, hm, qkv, act, mask_ref, cos_ref, sin_ref,
                    w_sem, xin_sem, ag_ss, ag_rs, rs_ss, rs_rs, fwd_sem, home_sem, lw_ss, lw_rs):
    nc, nl, tp, pp, heads, hd, tok = dims
    rb, d_model = xin.shape[1:]
    rows = tp * rb
    ff = wup.shape[1]
    qd = heads * hd
    last = tp - 1
    z = lax.axis_index("tp")
    s = lax.axis_index("pp")
    has_left, has_right = z > 0, z < last
    has_prev, has_next = s > 0, s < pp - 1
    half = pp // 2
    front = s < half

    def on(cond, fn):
        pl.when(cond)(fn)

    def remote(src, dst, ss, rs, to):
        return pltpu.make_async_remote_copy(src_ref=src, dst_ref=dst, send_sem=ss, recv_sem=rs, device_id=to, device_id_type=MESH)

    def neighbour(way):
        return {"tp": jnp.minimum(z + 1, last) if way == 0 else jnp.maximum(z - 1, 0)}

    def ag_copy(c, h, way, first=None):
        b = jnp.clip(z - h if way == 0 else z + h, 0, last)
        src = (first if first is not None else xin.at[0]) if h == 0 else xfull.at[c % NX, b]
        return remote(src, xfull.at[c % NX, b], ag_ss.at[c % NS, way, h], ag_rs.at[c % NS, way, h], neighbour(way))

    def ag_sends(h, way):
        return has_right & (z >= h) if way == 0 else has_left & (z + h <= last)

    def ag_gets(h, way):
        return z - 1 - h >= 0 if way == 0 else z + 1 + h <= last

    def rs_copy(c, h, way):
        d = jnp.clip(z + last - h if way == 0 else z - last + h, 0, last)
        return remote(part.at[c % NP, d], rbuf.at[c % NR, way, h], rs_ss.at[c % NS, way, h], rs_rs.at[c % NS, way, h], neighbour(way))

    def rs_sends(h, way):
        return z <= h if way == 0 else last - z <= h

    def rs_sends_all(h, way):
        return rs_sends(h, way) & (has_right if way == 0 else has_left)

    def rs_gets(h, way):
        return has_left & (z - 1 <= h) if way == 0 else has_right & (last - 1 - z <= h)

    def fwd_copy(v):
        return remote(xin.at[v], xin.at[v], fwd_sem.at[v], xin_sem.at[v], {"pp": jnp.minimum(s + 1, pp - 1)})

    def turn_copy(v):
        return remote(xin.at[v], xlate.at[v - (nc - nl)], fwd_sem.at[v], xin_sem.at[v + nl], {"pp": 0})

    def next_late_copy(v):
        return remote(xlate.at[v - nc], xlate.at[v - nc], fwd_sem.at[v], xin_sem.at[v], {"pp": jnp.minimum(s + 1, pp - 1)})

    def home_copy(v):
        return remote(xlate.at[v - nc], xin.at[v - nl], home_sem.at[v - nc], xin_sem.at[v - nl], {"pp": jnp.minimum(s + half, pp - 1)})

    own = [wq_hbm, wk_hbm, wv_hbm, ln_hbm, wup_hbm, wo_hbm, wdn_hbm]
    late = [lq_hbm, lk_hbm, lv_hbm, lln_hbm, lup_hbm, lo_hbm, ldn_hbm]
    held = [wqkv.at[:, pl.ds(0, qd)], wqkv.at[:, pl.ds(qd, qd)], wqkv.at[:, pl.ds(2 * qd, qd)], ln_ref, wup, wod.at[pl.ds(0, qd)], wod.at[pl.ds(qd, ff)]]
    weight_copies = [pltpu.make_async_copy(src, dst, w_sem.at[k]) for k, (src, dst) in enumerate(zip(own, held))]
    swap_copies = [pltpu.make_async_copy(src, dst, w_sem.at[k]) for k, (src, dst) in enumerate(zip(late, held))]
    lend_copies = [remote(src, dst, lw_ss.at[k], lw_rs.at[k], {"pp": jnp.maximum(s - half, 0)}) for k, (src, dst) in enumerate(zip(own, late))]

    barrier = pltpu.get_barrier_semaphore()
    for there, to in ((has_left, neighbour(1)), (has_right, neighbour(0)), (has_prev, {"pp": jnp.maximum(s - 1, 0)}), (has_next, {"pp": jnp.minimum(s + 1, pp - 1)}), (front, {"pp": jnp.minimum(s + half, pp - 1)}), (s >= half, {"pp": jnp.maximum(s - half, 0)})):
        @pl.when(there)
        def _(to=to):
            pl.semaphore_signal(barrier, inc=1, device_id=to, device_id_type=MESH)

    def load(c):
        return pltpu.make_async_copy(x_hbm.at[c], xin.at[c], xin_sem.at[c])

    for c in range(AHEAD):
        on(s == 0, load(c).start)
    for copy in weight_copies:
        copy.start()

    for way, alone in ((0, z == 0), (1, z == last)):
        @pl.when(alone)
        def _(way=way):
            for k in range(NR):
                rbuf[k, way, last - 1] = jnp.zeros(rbuf.shape[3:], rbuf.dtype)

    row = lax.broadcasted_iota(jnp.int32, (rows, rows), 0)
    col = lax.broadcasted_iota(jnp.int32, (rows, rows), 1)
    same = row % rb // tok == col % rb // tok
    later = row // rb * tok + row % tok >= col // rb * tok + col % tok
    mask_ref[...] = jnp.where(same, jnp.where(later, 0.0, -1e30), -3e38)
    for b in range(tp):
        for q in range(rb // tok):
            to, of = slice(b * rb + q * tok, b * rb + (q + 1) * tok), slice(b * tok, (b + 1) * tok)
            cos_ref[to] = cos_tab[of]
            sin_ref[to] = sin_tab[of]

    pl.semaphore_wait(barrier, has_left.astype(jnp.int32) + has_right.astype(jnp.int32) + has_prev.astype(jnp.int32) + has_next.astype(jnp.int32) + 1)

    @pl.when(s >= half)
    def _():
        for copy in lend_copies:
            copy.start()

    def in_its_place(c, fn):
        on(c < nc, lambda: fn(xin.at[c]))
        on(c >= nc, lambda: fn(xlate.at[c - nc]))

    def ag_start(c):
        on((s == 0) & (c + AHEAD < nc), lambda: load(c + AHEAD).start())
        pltpu.make_async_copy(x_hbm.at[0], xin.at[0], xin_sem.at[c]).wait()

        def send(place):
            for way in (0, 1):
                on(ag_sends(0, way), ag_copy(c, 0, way, place).start)
            xfull[c % NX, z] = place[...]
        in_its_place(c, send)

    def ag_hop(c, h):
        for way in (0, 1):
            on(ag_gets(h - 1, way), ag_copy(c, h - 1, way).wait_recv)
            if h < last:
                on(ag_sends(h, way), ag_copy(c, h, way).start)

    def ag_drain(c):
        for h in range(last):
            for way in (0, 1):
                on(ag_sends(h, way), ag_copy(c, h, way).wait_send)

    def rs_hop(c, h):
        for way in (0, 1):
            @pl.when(rs_sends_all(h, way))
            def _(way=way):
                if h > 0:
                    @pl.when(rs_gets(h - 1, way))
                    def _():
                        rs_copy(c, h - 1, way).wait_recv()
                        d = z + last - h if way == 0 else z - last + h
                        mine = part[c % NP, d].astype(jnp.float32)
                        part[c % NP, d] = (mine + rbuf[c % NR, way, h - 1].astype(jnp.float32)).astype(part.dtype)
                rs_copy(c, h, way).start()

    def rs_drain(c):
        for h in range(last):
            for way in (0, 1):
                on(rs_sends_all(h, way), rs_copy(c, h, way).wait_send)

    def finish(c):
        for way in (0, 1):
            on(rs_gets(last - 1, way), rs_copy(c, last - 1, way).wait_recv)
        f32 = jnp.float32

        def add(place):
            total = place[...].astype(f32) + part[c % NP, z].astype(f32)
            total = total + rbuf[c % NR, 0, last - 1].astype(f32) + rbuf[c % NR, 1, last - 1].astype(f32)
            place[...] = total.astype(xin.dtype)
        in_its_place(c, add)
        turns = (s == half - 1) & (c >= nc - nl)
        on(has_next & (c < nc) & ~turns, lambda: fwd_copy(c).start())
        on(turns & (c < nc), lambda: turn_copy(c).start())
        on((s < half - 1) & (c >= nc), lambda: next_late_copy(c).start())
        on(front & (c >= nc), lambda: home_copy(c).start())

    lt = min(rb, 32)
    per_block = rb // lt

    def norms(c):
        def tile(t, carry):
            x_f32 = xfull[c % NX, t // per_block, pl.ds((t % per_block) * lt, lt)].astype(jnp.float32)
            row_mean = jnp.mean(x_f32, axis=-1, keepdims=True)
            centred = x_f32 - row_mean
            variance = jnp.mean(centred * centred, axis=-1, keepdims=True)
            unit = centred * lax.rsqrt(variance + LN_EPS)
            at = pl.ds(pl.multiple_of(t * lt, lt), lt)
            ha[at] = (unit * ln_ref[0:1] + ln_ref[1:2]).astype(ha.dtype)
            hm[at] = (unit * ln_ref[2:3] + ln_ref[3:4]).astype(hm.dtype)
            return carry
        lax.fori_loop(0, rows // lt, tile, 0, unroll=2)

    def cols(n):
        return pl.ds(pl.multiple_of(n * NT, NT), NT)

    per_tile = NT // hd

    def projections():
        def rotated(n, carry):
            y = jnp.dot(ha[...], wqkv[:, cols(n)], preferred_element_type=jnp.float32)
            for j in range(per_tile):
                head = y[:, j * hd:(j + 1) * hd]
                turned = head * cos_ref[...] + pltpu.roll(head, hd // 2, 1) * sin_ref[...]
                qkv[n * per_tile + j] = turned.astype(qkv.dtype)
            return carry
        lax.fori_loop(0, 2 * qd // NT, rotated, 0, unroll=2)

        def plain(n, carry):
            y = jnp.dot(ha[...], wqkv[:, cols(n)], preferred_element_type=jnp.float32)
            for j in range(per_tile):
                qkv[n * per_tile + j] = y[:, j * hd:(j + 1) * hd].astype(qkv.dtype)
            return carry
        lax.fori_loop(2 * qd // NT, 3 * qd // NT, plain, 0, unroll=True)

    def attention():
        for h in range(heads):
            scores = lax.dot_general(qkv[h], qkv[heads + h], (((1,), (1,)), ((), ())), preferred_element_type=jnp.float32) * (hd ** -0.5)
            floor = mask_ref[...]
            scores = jnp.where(floor == 0.0, scores, floor)
            raised = jnp.exp(scores - jnp.max(scores, axis=-1, keepdims=True))
            probs = (raised * (1.0 / jnp.sum(raised, axis=-1, keepdims=True))).astype(qkv.dtype)
            act[:, h * hd:(h + 1) * hd] = jnp.dot(probs, qkv[2 * heads + h], preferred_element_type=jnp.float32).astype(act.dtype)

    def mlp_up():
        def tile(n, carry):
            u = jnp.dot(hm[...], wup[:, cols(n)], preferred_element_type=jnp.float32)
            g = 0.5 * u * (1.0 + lax.erf(u * (0.5 ** 0.5)))
            act[:, pl.ds(pl.multiple_of(qd + n * NT, NT), NT)] = g.astype(act.dtype)
            return carry
        lax.fori_loop(0, ff // NT, tile, 0, unroll=2)

    def project_out(c):
        def tile(n, carry):
            o = jnp.dot(act[...], wod[:, cols(n)], preferred_element_type=jnp.float32).astype(part.dtype)
            for b in range(tp):
                part[c % NP, b, :, cols(n)] = o[b * rb:(b + 1) * rb]
            return carry
        lax.fori_loop(0, d_model // NT, tile, 0, unroll=2)

    def holds(c):
        return (c >= 0) & (c < nc)

    def weights_ready(c, ks):
        @pl.when((c == 0) | (c == nc))
        def _():
            for k in ks:
                weight_copies[k].wait()

    def swap_weights(c, ks):
        @pl.when(front & (c == nc - 1))
        def _():
            for k in ks:
                lend_copies[k].wait_recv()
                swap_copies[k].start()

    def heads_step(c, lo):
        weights_ready(c, (0, 1, 2, 3))
        norms(c)
        projections()
        swap_weights(c, (0, 1, 2, 3))
        attention()

    def up_step(c, lo):
        weights_ready(c, (4,))
        mlp_up()
        swap_weights(c, (4,))

    def out_step(c, lo):
        weights_ready(c, (5, 6))
        ag_drain(c)
        on(c - NP >= lo, lambda: rs_drain(c - NP))
        project_out(c)
        swap_weights(c, (5, 6))

    steps = {
        "gather0": lambda c, lo: ag_start(c),
        "gather1": lambda c, lo: ag_hop(c, 1),
        "gather2": lambda c, lo: ag_hop(c, 2),
        "arrive": lambda c, lo: ag_hop(c, last),
        "heads": heads_step,
        "up": up_step,
        "out": out_step,
        "scatter0": lambda c, lo: rs_hop(c, 0),
        "scatter1": lambda c, lo: rs_hop(c, 1),
        "scatter2": lambda c, lo: rs_hop(c, 2),
        "finish": lambda c, lo: finish(c),
    }
    span = max(behind for _, behind in TURN)

    def segment(k, carry):
        lo = k * nc
        hi = jnp.where(front, jnp.where(k == 0, nc, nc + nl), jnp.where(k == 0, nc - nl, nc))

        def turn(i, carry):
            for name, behind in TURN:
                c = i - behind
                on((c >= lo) & (c < hi), functools.partial(steps[name], c, lo))
            return carry

        lax.fori_loop(lo, jnp.where(hi > lo, hi + span, lo), turn, 0)
        for back in range(1, NP + 1):
            on(hi - back >= lo, lambda: rs_drain(hi - back))
        return carry

    lax.fori_loop(0, 2, segment, 0)

    @pl.when(has_next)
    def _():
        def sent(v, carry):
            fwd_copy(v).wait_send()
            return carry
        lax.fori_loop(0, jnp.where(s < half - 1, nc, nc - nl), sent, 0)

    for k in range(nl):
        on(s == half - 1, turn_copy(nc - nl + k).wait_send)
        on(s < half - 1, next_late_copy(nc + k).wait_send)
        on(front, home_copy(nc + k).wait_send)

    @pl.when(s >= half)
    def _():
        for copy in lend_copies:
            copy.wait_send()
        for k in range(nl):
            c = nc - nl + k
            pltpu.make_async_copy(x_hbm.at[0], xin.at[0], xin_sem.at[c]).wait()


def solution(mesh):
    tp, pp = mesh.shape["tp"], mesh.shape["pp"]

    def stage_body(x_in, ln_params, w_q, w_k, w_v, w_o, w_up, w_down):
        num_micro, batch_dim, tok, d_model = x_in.shape
        heads, hd = w_k.shape[2:]
        ff = w_up.shape[2]
        seqs = batch_dim // CHUNKS_PER_MICRO
        nc = num_micro * CHUNKS_PER_MICRO
        rb = seqs * tok
        rows = tp * rb
        qd = heads * hd
        bf16, f32 = jnp.bfloat16, jnp.float32

        cos_tab, sin_tab = rope_tables(tp * tok, hd)
        cos_full = jnp.concatenate([cos_tab, cos_tab], axis=-1)
        sin_full = jnp.concatenate([-sin_tab, sin_tab], axis=-1)

        any_spec = pl.BlockSpec(memory_space=pl.ANY)
        vmem_spec = pl.BlockSpec(memory_space=pltpu.VMEM)
        dma = pltpu.SemaphoreType.DMA
        flops = 2 * num_micro * tp * batch_dim * tok * (3 * qd * d_model + qd * d_model + 2 * ff * d_model)
        out, *_ = pl.pallas_call(
            functools.partial(pipeline_kernel, (nc, LATE, tp, pp, heads, hd, tok)),
            out_shape=[pltpu.VMEM((nc, rb, d_model), bf16)] + [jax.ShapeDtypeStruct((d_model, qd), bf16)] * 3 + [
                jax.ShapeDtypeStruct((4, d_model), f32), jax.ShapeDtypeStruct((d_model, ff), bf16),
                jax.ShapeDtypeStruct((qd, d_model), bf16), jax.ShapeDtypeStruct((ff, d_model), bf16)],
            in_specs=[any_spec, vmem_spec, vmem_spec] + [any_spec] * 7,
            out_specs=[vmem_spec] + [any_spec] * 7,
            scratch_shapes=[
                pltpu.VMEM((d_model, 3 * qd), bf16),
                pltpu.VMEM((4, d_model), f32),
                pltpu.VMEM((d_model, ff), bf16),
                pltpu.VMEM((qd + ff, d_model), bf16),
                pltpu.VMEM((LATE, rb, d_model), bf16),
                pltpu.VMEM((NX, tp, rb, d_model), bf16),
                pltpu.VMEM((NR, 2, tp - 1, rb, d_model), bf16),
                pltpu.VMEM((NP, tp, rb, d_model), bf16),
                pltpu.VMEM((rows, d_model), bf16),
                pltpu.VMEM((rows, d_model), bf16),
                pltpu.VMEM((3 * heads, rows, hd), bf16),
                pltpu.VMEM((rows, qd + ff), bf16),
                pltpu.VMEM((rows, rows), f32),
                pltpu.VMEM((rows, hd), f32),
                pltpu.VMEM((rows, hd), f32),
                dma((7,)),
                dma((nc + LATE,)),
                dma((NS, 2, tp - 1)),
                dma((NS, 2, tp - 1)),
                dma((NS, 2, tp - 1)),
                dma((NS, 2, tp - 1)),
                dma((nc + LATE,)),
                dma((LATE,)),
                dma((7,)),
                dma((7,)),
            ],
            compiler_params=pltpu.CompilerParams(collective_id=0, has_side_effects=True, vmem_limit_bytes=52 * 2 ** 20),
            cost_estimate=pl.CostEstimate(flops=flops, bytes_accessed=50 * 2 ** 20, transcendentals=0),
            name="pipeline",
        )(x_in.reshape(nc, rb, d_model), cos_full, sin_full, w_q.reshape(d_model, qd), w_k.reshape(d_model, qd), w_v.reshape(d_model, qd), ln_params[0], w_up[0], w_o.reshape(qd, d_model), w_down[0])
        return out.reshape(1, num_micro, batch_dim, tok, d_model)

    in_specs = (P(None, "dp", "tp", None), P("pp", None, None), P("pp", None, "tp", None, None), P("pp", None, "tp", None), P("pp", None, "tp", None), P("pp", "tp", None, None, None), P("pp", None, "tp"), P("pp", "tp", None))
    return jax.shard_map(stage_body, mesh=mesh, in_specs=in_specs, out_specs=P("pp", None, "dp", "tp", None), check_vma=False)
```

```python
import functools

import jax
import jax.numpy as jnp
from jax import lax
from jax.experimental import pallas as pl
from jax.experimental.pallas import tpu as pltpu
from jax.sharding import PartitionSpec as P

LN_EPS = 1e-5
ROPE_BASE = 10000.0
CHUNKS_PER_MICRO = 8
NT = 256
NX, NR, NP, NS = 4, 4, 3, 4
LATE = 3
AHEAD = 4
TURN = (("gather0", 0), ("scatter1", 3), ("gather2", 1), ("up", 2), ("finish", 4), ("out", 2), ("scatter0", 2), ("lay_q", 0), ("gather1", 0), ("lay_k", 0), ("lay_v", 1), ("arrive", 1), ("scatter2", 3), ("heads", 1))
MESH = pl.DeviceIdType.MESH


def rope_tables(seq_len, head_dim):
    positions = jnp.arange(seq_len, dtype=jnp.float32)
    inv_freq = ROPE_BASE ** (-2.0 * jnp.arange(head_dim // 2, dtype=jnp.float32) / head_dim)
    angles = positions[:, None] * inv_freq[None, :]
    return jnp.cos(angles), jnp.sin(angles)


def pipeline_kernel(dims, x_hbm, cos_tab, sin_tab, wq_hbm, wk_hbm, wv_hbm, ln_hbm, wup_hbm, wo_hbm, wdn_hbm,
                    xin, lq_hbm, lk_hbm, lv_hbm, lln_hbm, lup_hbm, lo_hbm, ldn_hbm,
                    raw, wqkv, ln_ref, wup, wod, xlate, xfull, rbuf, part, ha, hm, qkv, act, mask_ref, cos_ref, sin_ref,
                    w_sem, xin_sem, ag_ss, ag_rs, rs_ss, rs_rs, fwd_sem, home_sem, lw_ss, lw_rs):
    nc, nl, tp, pp, heads, hd, tok = dims
    rb, d_model = xin.shape[1:]
    rows = tp * rb
    ff = wup.shape[1]
    qd = heads * hd
    last = tp - 1
    z = lax.axis_index("tp")
    s = lax.axis_index("pp")
    has_left, has_right = z > 0, z < last
    has_prev, has_next = s > 0, s < pp - 1
    half = pp // 2
    front = s < half

    def on(cond, fn):
        pl.when(cond)(fn)

    def remote(src, dst, ss, rs, to):
        return pltpu.make_async_remote_copy(src_ref=src, dst_ref=dst, send_sem=ss, recv_sem=rs, device_id=to, device_id_type=MESH)

    def neighbour(way):
        return {"tp": jnp.minimum(z + 1, last) if way == 0 else jnp.maximum(z - 1, 0)}

    def ag_copy(c, h, way, first=None):
        b = jnp.clip(z - h if way == 0 else z + h, 0, last)
        src = (first if first is not None else xin.at[0]) if h == 0 else xfull.at[c % NX, b]
        return remote(src, xfull.at[c % NX, b], ag_ss.at[c % NS, way, h], ag_rs.at[c % NS, way, h], neighbour(way))

    def ag_sends(h, way):
        return has_right & (z >= h) if way == 0 else has_left & (z + h <= last)

    def ag_gets(h, way):
        return z - 1 - h >= 0 if way == 0 else z + 1 + h <= last

    def rs_copy(c, h, way):
        d = jnp.clip(z + last - h if way == 0 else z - last + h, 0, last)
        return remote(part.at[c % NP, d], rbuf.at[c % NR, way, h], rs_ss.at[c % NS, way, h], rs_rs.at[c % NS, way, h], neighbour(way))

    def rs_sends(h, way):
        return z <= h if way == 0 else last - z <= h

    def rs_sends_all(h, way):
        return rs_sends(h, way) & (has_right if way == 0 else has_left)

    def rs_gets(h, way):
        return has_left & (z - 1 <= h) if way == 0 else has_right & (last - 1 - z <= h)

    def fwd_copy(v):
        return remote(xin.at[v], xin.at[v], fwd_sem.at[v], xin_sem.at[v], {"pp": jnp.minimum(s + 1, pp - 1)})

    def turn_copy(v):
        return remote(xin.at[v], xlate.at[v - (nc - nl)], fwd_sem.at[v], xin_sem.at[v + nl], {"pp": 0})

    def next_late_copy(v):
        return remote(xlate.at[v - nc], xlate.at[v - nc], fwd_sem.at[v], xin_sem.at[v], {"pp": jnp.minimum(s + 1, pp - 1)})

    def home_copy(v):
        return remote(xlate.at[v - nc], xin.at[v - nl], home_sem.at[v - nc], xin_sem.at[v - nl], {"pp": jnp.minimum(s + half, pp - 1)})

    own = [wq_hbm, wk_hbm, wv_hbm, ln_hbm, wup_hbm, wo_hbm, wdn_hbm]
    late = [lq_hbm, lk_hbm, lv_hbm, lln_hbm, lup_hbm, lo_hbm, ldn_hbm]
    held = [wqkv.at[:, pl.ds(0, qd)], wqkv.at[:, pl.ds(qd, qd)], wqkv.at[:, pl.ds(2 * qd, qd)], ln_ref, wup, wod.at[pl.ds(0, qd)], wod.at[pl.ds(qd, ff)]]
    weight_copies = [pltpu.make_async_copy(src, dst, w_sem.at[k]) for k, (src, dst) in enumerate(zip(own, [raw.at[0], raw.at[1], raw.at[2]] + held[3:]))]
    swap_copies = [pltpu.make_async_copy(src, dst, w_sem.at[k]) for k, (src, dst) in enumerate(zip(late, held))]
    lend_copies = [remote(src, dst, lw_ss.at[k], lw_rs.at[k], {"pp": jnp.maximum(s - half, 0)}) for k, (src, dst) in enumerate(zip(held[:3] + own[3:], late))]

    barrier = pltpu.get_barrier_semaphore()
    for there, to in ((has_left, neighbour(1)), (has_right, neighbour(0)), (has_prev, {"pp": jnp.maximum(s - 1, 0)}), (has_next, {"pp": jnp.minimum(s + 1, pp - 1)}), (front, {"pp": jnp.minimum(s + half, pp - 1)}), (s >= half, {"pp": jnp.maximum(s - half, 0)})):
        @pl.when(there)
        def _(to=to):
            pl.semaphore_signal(barrier, inc=1, device_id=to, device_id_type=MESH)

    def load(c):
        return pltpu.make_async_copy(x_hbm.at[c], xin.at[c], xin_sem.at[c])

    for c in range(AHEAD):
        on(s == 0, load(c).start)
    for copy in weight_copies:
        copy.start()

    lay_rows = 64

    def lay(k):
        weight_copies[k].wait()

        def some(t, carry):
            at = pl.ds(pl.multiple_of(t * lay_rows, lay_rows), lay_rows)
            wqkv[at, k * qd:(k + 1) * qd] = raw[k, at].reshape(lay_rows, qd)
            return carry
        lax.fori_loop(0, d_model // lay_rows, some, 0)

    @pl.when(s > 0)
    def _():
        for k in range(3):
            lay(k)

    for way, alone in ((0, z == 0), (1, z == last)):
        @pl.when(alone)
        def _(way=way):
            for k in range(NR):
                rbuf[k, way, last - 1] = jnp.zeros(rbuf.shape[3:], rbuf.dtype)

    row = lax.broadcasted_iota(jnp.int32, (rows, rows), 0)
    col = lax.broadcasted_iota(jnp.int32, (rows, rows), 1)
    same = row % rb // tok == col % rb // tok
    later = row // rb * tok + row % tok >= col // rb * tok + col % tok
    mask_ref[...] = jnp.where(same, jnp.where(later, 0.0, -1e30), -3e38)
    for b in range(tp):
        for q in range(rb // tok):
            to, of = slice(b * rb + q * tok, b * rb + (q + 1) * tok), slice(b * tok, (b + 1) * tok)
            cos_ref[to] = cos_tab[of]
            sin_ref[to] = sin_tab[of]

    pl.semaphore_wait(barrier, has_left.astype(jnp.int32) + has_right.astype(jnp.int32) + has_prev.astype(jnp.int32) + has_next.astype(jnp.int32) + 1)

    @pl.when(s >= half)
    def _():
        for copy in lend_copies:
            copy.start()

    def in_its_place(c, fn):
        on(c < nc, lambda: fn(xin.at[c]))
        on(c >= nc, lambda: fn(xlate.at[c - nc]))

    def ag_start(c):
        on((s == 0) & (c + AHEAD < nc), lambda: load(c + AHEAD).start())
        pltpu.make_async_copy(x_hbm.at[0], xin.at[0], xin_sem.at[c]).wait()

        def send(place):
            for way in (0, 1):
                on(ag_sends(0, way), ag_copy(c, 0, way, place).start)
            xfull[c % NX, z] = place[...]
        in_its_place(c, send)

    def ag_hop(c, h):
        for way in (0, 1):
            on(ag_gets(h - 1, way), ag_copy(c, h - 1, way).wait_recv)
            if h < last:
                on(ag_sends(h, way), ag_copy(c, h, way).start)

    def ag_drain(c):
        for h in range(last):
            for way in (0, 1):
                on(ag_sends(h, way), ag_copy(c, h, way).wait_send)

    def rs_hop(c, h):
        for way in (0, 1):
            @pl.when(rs_sends_all(h, way))
            def _(way=way):
                if h > 0:
                    @pl.when(rs_gets(h - 1, way))
                    def _():
                        rs_copy(c, h - 1, way).wait_recv()
                        d = z + last - h if way == 0 else z - last + h
                        mine = part[c % NP, d].astype(jnp.float32)
                        part[c % NP, d] = (mine + rbuf[c % NR, way, h - 1].astype(jnp.float32)).astype(part.dtype)
                rs_copy(c, h, way).start()

    def rs_drain(c):
        for h in range(last):
            for way in (0, 1):
                on(rs_sends_all(h, way), rs_copy(c, h, way).wait_send)

    def finish(c):
        for way in (0, 1):
            on(rs_gets(last - 1, way), rs_copy(c, last - 1, way).wait_recv)
        f32 = jnp.float32

        def add(place):
            total = place[...].astype(f32) + part[c % NP, z].astype(f32)
            total = total + rbuf[c % NR, 0, last - 1].astype(f32) + rbuf[c % NR, 1, last - 1].astype(f32)
            place[...] = total.astype(xin.dtype)
        in_its_place(c, add)
        turns = (s == half - 1) & (c >= nc - nl)
        on(has_next & (c < nc) & ~turns, lambda: fwd_copy(c).start())
        on(turns & (c < nc), lambda: turn_copy(c).start())
        on((s < half - 1) & (c >= nc), lambda: next_late_copy(c).start())
        on(front & (c >= nc), lambda: home_copy(c).start())

    lt = min(rb, 32)
    per_block = rb // lt

    def norms(c):
        def tile(t, carry):
            x_f32 = xfull[c % NX, t // per_block, pl.ds((t % per_block) * lt, lt)].astype(jnp.float32)
            row_mean = jnp.mean(x_f32, axis=-1, keepdims=True)
            centred = x_f32 - row_mean
            variance = jnp.mean(centred * centred, axis=-1, keepdims=True)
            unit = centred * lax.rsqrt(variance + LN_EPS)
            at = pl.ds(pl.multiple_of(t * lt, lt), lt)
            ha[at] = (unit * ln_ref[0:1] + ln_ref[1:2]).astype(ha.dtype)
            hm[at] = (unit * ln_ref[2:3] + ln_ref[3:4]).astype(hm.dtype)
            return carry
        lax.fori_loop(0, rows // lt, tile, 0, unroll=2)

    def cols(n):
        return pl.ds(pl.multiple_of(n * NT, NT), NT)

    per_tile = NT // hd

    def projections():
        def rotated(n, carry):
            y = jnp.dot(ha[...], wqkv[:, cols(n)], preferred_element_type=jnp.float32)
            for j in range(per_tile):
                head = y[:, j * hd:(j + 1) * hd]
                turned = head * cos_ref[...] + pltpu.roll(head, hd // 2, 1) * sin_ref[...]
                qkv[n * per_tile + j] = turned.astype(qkv.dtype)
            return carry
        lax.fori_loop(0, 2 * qd // NT, rotated, 0, unroll=2)

        def plain(n, carry):
            y = jnp.dot(ha[...], wqkv[:, cols(n)], preferred_element_type=jnp.float32)
            for j in range(per_tile):
                qkv[n * per_tile + j] = y[:, j * hd:(j + 1) * hd].astype(qkv.dtype)
            return carry
        lax.fori_loop(2 * qd // NT, 3 * qd // NT, plain, 0, unroll=True)

    def attention():
        for h in range(heads):
            scores = lax.dot_general(qkv[h], qkv[heads + h], (((1,), (1,)), ((), ())), preferred_element_type=jnp.float32) * (hd ** -0.5)
            floor = mask_ref[...]
            scores = jnp.where(floor == 0.0, scores, floor)
            raised = jnp.exp(scores - jnp.max(scores, axis=-1, keepdims=True))
            probs = (raised * (1.0 / jnp.sum(raised, axis=-1, keepdims=True))).astype(qkv.dtype)
            act[:, h * hd:(h + 1) * hd] = jnp.dot(probs, qkv[2 * heads + h], preferred_element_type=jnp.float32).astype(act.dtype)

    def mlp_up():
        def tile(n, carry):
            u = jnp.dot(hm[...], wup[:, cols(n)], preferred_element_type=jnp.float32)
            g = 0.5 * u * (1.0 + lax.erf(u * (0.5 ** 0.5)))
            act[:, pl.ds(pl.multiple_of(qd + n * NT, NT), NT)] = g.astype(act.dtype)
            return carry
        lax.fori_loop(0, ff // NT, tile, 0, unroll=2)

    def project_out(c):
        def tile(n, carry):
            o = jnp.dot(act[...], wod[:, cols(n)], preferred_element_type=jnp.float32).astype(part.dtype)
            for b in range(tp):
                part[c % NP, b, :, cols(n)] = o[b * rb:(b + 1) * rb]
            return carry
        lax.fori_loop(0, d_model // NT, tile, 0, unroll=2)

    def holds(c):
        return (c >= 0) & (c < nc)

    def weights_ready(c, ks):
        @pl.when((c == 0) | (c == nc))
        def _():
            for k in ks:
                weight_copies[k].wait()

    def swap_weights(c, ks):
        @pl.when(front & (c == nc - 1))
        def _():
            for k in ks:
                lend_copies[k].wait_recv()
                swap_copies[k].start()

    def heads_step(c, lo):
        @pl.when(c == nc)
        def _():
            for k in range(3):
                swap_copies[k].wait()
        weights_ready(c, (3,))
        norms(c)
        projections()
        swap_weights(c, (0, 1, 2, 3))
        attention()

    def up_step(c, lo):
        weights_ready(c, (4,))
        mlp_up()
        swap_weights(c, (4,))

    def out_step(c, lo):
        weights_ready(c, (5, 6))
        ag_drain(c)
        on(c - NP >= lo, lambda: rs_drain(c - NP))
        project_out(c)
        swap_weights(c, (5, 6))

    steps = {
        "gather0": lambda c, lo: ag_start(c),
        "gather1": lambda c, lo: ag_hop(c, 1),
        "gather2": lambda c, lo: ag_hop(c, 2),
        "lay_q": lambda c, lo: on((s == 0) & (c == 0), lambda: lay(0)),
        "lay_k": lambda c, lo: on((s == 0) & (c == 0), lambda: lay(1)),
        "lay_v": lambda c, lo: on((s == 0) & (c == 0), lambda: lay(2)),
        "arrive": lambda c, lo: ag_hop(c, last),
        "heads": heads_step,
        "up": up_step,
        "out": out_step,
        "scatter0": lambda c, lo: rs_hop(c, 0),
        "scatter1": lambda c, lo: rs_hop(c, 1),
        "scatter2": lambda c, lo: rs_hop(c, 2),
        "finish": lambda c, lo: finish(c),
    }
    span = max(behind for _, behind in TURN)

    def segment(k, carry):
        lo = k * nc
        hi = jnp.where(front, jnp.where(k == 0, nc, nc + nl), jnp.where(k == 0, nc - nl, nc))

        def turn(i, carry):
            for name, behind in TURN:
                c = i - behind
                on((c >= lo) & (c < hi), functools.partial(steps[name], c, lo))
            return carry

        lax.fori_loop(lo, jnp.where(hi > lo, hi + span, lo), turn, 0)
        for back in range(1, NP + 1):
            on(hi - back >= lo, lambda: rs_drain(hi - back))
        return carry

    lax.fori_loop(0, 2, segment, 0)

    @pl.when(has_next)
    def _():
        def sent(v, carry):
            fwd_copy(v).wait_send()
            return carry
        lax.fori_loop(0, jnp.where(s < half - 1, nc, nc - nl), sent, 0)

    for k in range(nl):
        on(s == half - 1, turn_copy(nc - nl + k).wait_send)
        on(s < half - 1, next_late_copy(nc + k).wait_send)
        on(front, home_copy(nc + k).wait_send)

    @pl.when(s >= half)
    def _():
        for copy in lend_copies:
            copy.wait_send()
        for k in range(nl):
            c = nc - nl + k
            pltpu.make_async_copy(x_hbm.at[0], xin.at[0], xin_sem.at[c]).wait()


def solution(mesh):
    tp, pp = mesh.shape["tp"], mesh.shape["pp"]

    def stage_body(x_in, ln_params, w_q, w_k, w_v, w_o, w_up, w_down):
        num_micro, batch_dim, tok, d_model = x_in.shape
        heads, hd = w_k.shape[2:]
        ff = w_up.shape[2]
        seqs = batch_dim // CHUNKS_PER_MICRO
        nc = num_micro * CHUNKS_PER_MICRO
        rb = seqs * tok
        rows = tp * rb
        qd = heads * hd
        bf16, f32 = jnp.bfloat16, jnp.float32

        cos_tab, sin_tab = rope_tables(tp * tok, hd)
        cos_full = jnp.concatenate([cos_tab, cos_tab], axis=-1)
        sin_full = jnp.concatenate([-sin_tab, sin_tab], axis=-1)

        any_spec = pl.BlockSpec(memory_space=pl.ANY)
        vmem_spec = pl.BlockSpec(memory_space=pltpu.VMEM)
        dma = pltpu.SemaphoreType.DMA
        flops = 2 * num_micro * tp * batch_dim * tok * (3 * qd * d_model + qd * d_model + 2 * ff * d_model)
        out, *_ = pl.pallas_call(
            functools.partial(pipeline_kernel, (nc, LATE, tp, pp, heads, hd, tok)),
            out_shape=[pltpu.VMEM((nc, rb, d_model), bf16)] + [jax.ShapeDtypeStruct((d_model, qd), bf16)] * 3 + [
                jax.ShapeDtypeStruct((4, d_model), f32), jax.ShapeDtypeStruct((d_model, ff), bf16),
                jax.ShapeDtypeStruct((qd, d_model), bf16), jax.ShapeDtypeStruct((ff, d_model), bf16)],
            in_specs=[any_spec, vmem_spec, vmem_spec] + [any_spec] * 7,
            out_specs=[vmem_spec] + [any_spec] * 7,
            scratch_shapes=[
                pltpu.VMEM((3, d_model, heads, hd), bf16),
                pltpu.VMEM((d_model, 3 * qd), bf16),
                pltpu.VMEM((4, d_model), f32),
                pltpu.VMEM((d_model, ff), bf16),
                pltpu.VMEM((qd + ff, d_model), bf16),
                pltpu.VMEM((LATE, rb, d_model), bf16),
                pltpu.VMEM((NX, tp, rb, d_model), bf16),
                pltpu.VMEM((NR, 2, tp - 1, rb, d_model), bf16),
                pltpu.VMEM((NP, tp, rb, d_model), bf16),
                pltpu.VMEM((rows, d_model), bf16),
                pltpu.VMEM((rows, d_model), bf16),
                pltpu.VMEM((3 * heads, rows, hd), bf16),
                pltpu.VMEM((rows, qd + ff), bf16),
                pltpu.VMEM((rows, rows), f32),
                pltpu.VMEM((rows, hd), f32),
                pltpu.VMEM((rows, hd), f32),
                dma((7,)),
                dma((nc + LATE,)),
                dma((NS, 2, tp - 1)),
                dma((NS, 2, tp - 1)),
                dma((NS, 2, tp - 1)),
                dma((NS, 2, tp - 1)),
                dma((nc + LATE,)),
                dma((LATE,)),
                dma((7,)),
                dma((7,)),
            ],
            compiler_params=pltpu.CompilerParams(collective_id=0, has_side_effects=True, vmem_limit_bytes=52 * 2 ** 20),
            cost_estimate=pl.CostEstimate(flops=flops, bytes_accessed=50 * 2 ** 20, transcendentals=0),
            name="pipeline",
        )(x_in.reshape(nc, rb, d_model), cos_full, sin_full, w_q.reshape(d_model, heads, hd), w_k[0], w_v[0], ln_params[0], w_up[0], w_o.reshape(qd, d_model), w_down[0])
        return out.reshape(1, num_micro, batch_dim, tok, d_model)

    in_specs = (P(None, "dp", "tp", None), P("pp", None, None), P("pp", None, "tp", None, None), P("pp", None, "tp", None), P("pp", None, "tp", None), P("pp", "tp", None, None, None), P("pp", None, "tp"), P("pp", "tp", None))
    return jax.shard_map(stage_body, mesh=mesh, in_specs=in_specs, out_specs=P("pp", None, "dp", "tp", None), check_vma=False)
```

```python
import functools

import jax
import jax.numpy as jnp
from jax import lax
from jax.experimental import pallas as pl
from jax.experimental.pallas import tpu as pltpu
from jax.sharding import PartitionSpec as P

LN_EPS = 1e-5
ROPE_BASE = 10000.0
CHUNKS_PER_MICRO = 8
NT = 256
NX, NR, NP, NS = 4, 4, 3, 4
LATE = 4
EARLY = 16
AHEAD = 4
TURN = (("gather0", 0), ("arrive", 2), ("scatter2", 4), ("heads", 2), ("gather2", 1), ("lay_v", 1), ("scatter1", 3), ("up", 2), ("lay_q", 0), ("gather1", 0), ("lay_k", 0), ("out", 2), ("scatter0", 2), ("finish", 4))
MESH = pl.DeviceIdType.MESH


def rope_tables(seq_len, head_dim):
    positions = jnp.arange(seq_len, dtype=jnp.float32)
    inv_freq = ROPE_BASE ** (-2.0 * jnp.arange(head_dim // 2, dtype=jnp.float32) / head_dim)
    angles = positions[:, None] * inv_freq[None, :]
    return jnp.cos(angles), jnp.sin(angles)


def pipeline_kernel(dims, x_hbm, cos_tab, sin_tab, wq_hbm, wk_hbm, wv_hbm, ln_hbm, wup_hbm, wo_hbm, wdn_hbm,
                    xin, lq_hbm, lk_hbm, lv_hbm, lln_hbm, lup_hbm, lo_hbm, ldn_hbm,
                    raw, wqkv, ln_ref, wup, wod, xlate, early, xfull, rbuf, part, ha, hm, qkv, act, mask_ref, cos_ref, sin_ref,
                    w_sem, xin_sem, ag_ss, ag_rs, rs_ss, rs_rs, fwd_sem, home_sem, lw_ss, lw_rs, es_ss, es_rs, eh_ss, eh_rs):
    nc, nl, ne, tp, pp, heads, hd, tok = dims
    rb, d_model = xin.shape[1:]
    rows = tp * rb
    ff = wup.shape[1]
    qd = heads * hd
    last = tp - 1
    z = lax.axis_index("tp")
    s = lax.axis_index("pp")
    has_left, has_right = z > 0, z < last
    has_prev, has_next = s > 0, s < pp - 1
    half = pp // 2
    front = s < half

    def on(cond, fn):
        pl.when(cond)(fn)

    def remote(src, dst, ss, rs, to):
        return pltpu.make_async_remote_copy(src_ref=src, dst_ref=dst, send_sem=ss, recv_sem=rs, device_id=to, device_id_type=MESH)

    def neighbour(way):
        return {"tp": jnp.minimum(z + 1, last) if way == 0 else jnp.maximum(z - 1, 0)}

    def ag_copy(c, h, way, first=None):
        b = jnp.clip(z - h if way == 0 else z + h, 0, last)
        src = (first if first is not None else xin.at[0]) if h == 0 else xfull.at[c % NX, b]
        return remote(src, xfull.at[c % NX, b], ag_ss.at[c % NS, way, h], ag_rs.at[c % NS, way, h], neighbour(way))

    def ag_sends(h, way):
        return has_right & (z >= h) if way == 0 else has_left & (z + h <= last)

    def ag_gets(h, way):
        return z - 1 - h >= 0 if way == 0 else z + 1 + h <= last

    def rs_copy(c, h, way):
        d = jnp.clip(z + last - h if way == 0 else z - last + h, 0, last)
        return remote(part.at[c % NP, d], rbuf.at[c % NR, way, h], rs_ss.at[c % NS, way, h], rs_rs.at[c % NS, way, h], neighbour(way))

    def rs_sends(h, way):
        return z <= h if way == 0 else last - z <= h

    def rs_sends_all(h, way):
        return rs_sends(h, way) & (has_right if way == 0 else has_left)

    def rs_gets(h, way):
        return has_left & (z - 1 <= h) if way == 0 else has_right & (last - 1 - z <= h)

    def fwd_copy(v):
        return remote(xin.at[v], xin.at[v], fwd_sem.at[v], xin_sem.at[v], {"pp": jnp.minimum(s + 1, pp - 1)})

    def turn_copy(v):
        return remote(xin.at[v], xlate.at[v - (nc - nl)], fwd_sem.at[v], xin_sem.at[v + nl], {"pp": 0})

    def next_late_copy(v):
        return remote(xlate.at[v - nc], xlate.at[v - nc], fwd_sem.at[v], xin_sem.at[v], {"pp": jnp.minimum(s + 1, pp - 1)})

    def home_copy(v):
        return remote(xlate.at[v - nc], xin.at[v - nl], home_sem.at[v - nc], xin_sem.at[v - nl], {"pp": jnp.minimum(s + half, pp - 1)})

    own = [wq_hbm, wk_hbm, wv_hbm, ln_hbm, wup_hbm, wo_hbm, wdn_hbm]
    late = [lq_hbm, lk_hbm, lv_hbm, lln_hbm, lup_hbm, lo_hbm, ldn_hbm]
    held = [wqkv.at[:, pl.ds(0, qd)], wqkv.at[:, pl.ds(qd, qd)], wqkv.at[:, pl.ds(2 * qd, qd)], ln_ref, wup, wod.at[pl.ds(0, qd)], wod.at[pl.ds(qd, ff)]]
    weight_copies = [pltpu.make_async_copy(src, dst, w_sem.at[k]) for k, (src, dst) in enumerate(zip(own, [raw.at[0], raw.at[1], raw.at[2]] + held[3:]))]
    swap_copies = [pltpu.make_async_copy(src, dst, w_sem.at[k]) for k, (src, dst) in enumerate(zip(late, held))]
    lend_copies = [remote(src, dst, lw_ss.at[k], lw_rs.at[k], {"pp": jnp.maximum(s - half, 0)}) for k, (src, dst) in enumerate(zip(held[:3] + own[3:], late))]

    helper = s == pp - 1

    def other(j):
        return lax.rem(z + j, tp)

    def is_early(c):
        return (s == 0) & (c >= 1) & (c <= ne)

    def share_copy(c, j):
        return remote(x_hbm.at[c], early.at[c - 1, z], es_ss.at[c - 1, j], es_rs.at[c - 1, z], {"tp": other(j)})

    def got_copy(c, j):
        return remote(x_hbm.at[c], early.at[c - 1, other(j)], es_ss.at[c - 1, j], es_rs.at[c - 1, other(j)], {"tp": other(j)})

    def hand_copy(c, j):
        b = other(j)
        return remote(early.at[c - 1, b], early.at[c - 1, b], eh_ss.at[c - 1, b], eh_rs.at[c - 1, b], {"pp": 0})

    barrier = pltpu.get_barrier_semaphore()
    for j in range(1, tp):
        pl.semaphore_signal(barrier, inc=1, device_id={"tp": other(j)}, device_id_type=MESH)
    for j in range(1, pp):
        pl.semaphore_signal(barrier, inc=1, device_id={"pp": lax.rem(s + j, pp)}, device_id_type=MESH)

    def load(c):
        return pltpu.make_async_copy(x_hbm.at[c], xin.at[c], xin_sem.at[c])

    for c in range(AHEAD):
        on(s == 0, load(c).start)
    for copy in weight_copies:
        copy.start()

    lay_rows = 64

    def lay(k):
        weight_copies[k].wait()

        def some(t, carry):
            at = pl.ds(pl.multiple_of(t * lay_rows, lay_rows), lay_rows)
            wqkv[at, k * qd:(k + 1) * qd] = raw[k, at].reshape(lay_rows, qd)
            return carry
        lax.fori_loop(0, d_model // lay_rows, some, 0)

    @pl.when(s > 0)
    def _():
        for k in range(3):
            lay(k)

    for way, alone in ((0, z == 0), (1, z == last)):
        @pl.when(alone)
        def _(way=way):
            for k in range(NR):
                rbuf[k, way, last - 1] = jnp.zeros(rbuf.shape[3:], rbuf.dtype)

    row = lax.broadcasted_iota(jnp.int32, (rows, rows), 0)
    col = lax.broadcasted_iota(jnp.int32, (rows, rows), 1)
    same = row % rb // tok == col % rb // tok
    later = row // rb * tok + row % tok >= col // rb * tok + col % tok
    mask_ref[...] = jnp.where(same, jnp.where(later, 0.0, -1e30), -3e38)
    for b in range(tp):
        for q in range(rb // tok):
            to, of = slice(b * rb + q * tok, b * rb + (q + 1) * tok), slice(b * tok, (b + 1) * tok)
            cos_ref[to] = cos_tab[of]
            sin_ref[to] = sin_tab[of]

    pl.semaphore_wait(barrier, tp - 1 + pp - 1)

    def lend():
        for copy in lend_copies:
            copy.start()

    @pl.when(helper)
    def _():
        def share(c, carry):
            for j in range(1, tp):
                share_copy(c, j).start()
            return carry
        lax.fori_loop(1, ne + 1, share, 0)

        def hand(c, carry):
            for j in range(1, tp):
                got_copy(c, j).wait_recv()
                hand_copy(c, j).start()
            return carry
        lax.fori_loop(1, ne + 1, hand, 0)
        lend()

    def in_its_place(c, fn):
        on(c < nc, lambda: fn(xin.at[c]))
        on(c >= nc, lambda: fn(xlate.at[c - nc]))

    def ag_start(c):
        on((s == 0) & (c + AHEAD < nc), lambda: load(c + AHEAD).start())
        pltpu.make_async_copy(x_hbm.at[0], xin.at[0], xin_sem.at[c]).wait()
        on((s >= half) & ~helper & (c == 2), lend)

        def send(place):
            for way in (0, 1):
                on(ag_sends(0, way) & ~is_early(c), ag_copy(c, 0, way, place).start)
            xfull[c % NX, z] = place[...]
        in_its_place(c, send)

    def ag_hop(c, h):
        @pl.when(~is_early(c))
        def _():
            for way in (0, 1):
                on(ag_gets(h - 1, way), ag_copy(c, h - 1, way).wait_recv)
                if h < last:
                    on(ag_sends(h, way), ag_copy(c, h, way).start)

        if h == last:
            @pl.when(is_early(c))
            def _():
                for j in range(1, tp):
                    hand_copy(c, j).wait_recv()
                    xfull[c % NX, other(j)] = early[c - 1, other(j)]

    def ag_drain(c):
        @pl.when(~is_early(c))
        def _():
            for h in range(last):
                for way in (0, 1):
                    on(ag_sends(h, way), ag_copy(c, h, way).wait_send)

    def rs_hop(c, h):
        for way in (0, 1):
            @pl.when(rs_sends_all(h, way))
            def _(way=way):
                if h > 0:
                    @pl.when(rs_gets(h - 1, way))
                    def _():
                        rs_copy(c, h - 1, way).wait_recv()
                        d = z + last - h if way == 0 else z - last + h
                        mine = part[c % NP, d].astype(jnp.float32)
                        part[c % NP, d] = (mine + rbuf[c % NR, way, h - 1].astype(jnp.float32)).astype(part.dtype)
                rs_copy(c, h, way).start()

    def rs_drain(c):
        for h in range(last):
            for way in (0, 1):
                on(rs_sends_all(h, way), rs_copy(c, h, way).wait_send)

    def finish(c):
        for way in (0, 1):
            on(rs_gets(last - 1, way), rs_copy(c, last - 1, way).wait_recv)
        f32 = jnp.float32

        def add(place):
            total = place[...].astype(f32) + part[c % NP, z].astype(f32)
            total = total + rbuf[c % NR, 0, last - 1].astype(f32) + rbuf[c % NR, 1, last - 1].astype(f32)
            place[...] = total.astype(xin.dtype)
        in_its_place(c, add)
        turns = (s == half - 1) & (c >= nc - nl)
        on(has_next & (c < nc) & ~turns, lambda: fwd_copy(c).start())
        on(turns & (c < nc), lambda: turn_copy(c).start())
        on((s < half - 1) & (c >= nc), lambda: next_late_copy(c).start())
        on(front & (c >= nc), lambda: home_copy(c).start())

    lt = min(rb, 32)
    per_block = rb // lt

    def norms(c):
        def tile(t, carry):
            x_f32 = xfull[c % NX, t // per_block, pl.ds((t % per_block) * lt, lt)].astype(jnp.float32)
            row_mean = jnp.mean(x_f32, axis=-1, keepdims=True)
            centred = x_f32 - row_mean
            variance = jnp.mean(centred * centred, axis=-1, keepdims=True)
            unit = centred * lax.rsqrt(variance + LN_EPS)
            at = pl.ds(pl.multiple_of(t * lt, lt), lt)
            ha[at] = (unit * ln_ref[0:1] + ln_ref[1:2]).astype(ha.dtype)
            hm[at] = (unit * ln_ref[2:3] + ln_ref[3:4]).astype(hm.dtype)
            return carry
        lax.fori_loop(0, rows // lt, tile, 0, unroll=2)

    def cols(n):
        return pl.ds(pl.multiple_of(n * NT, NT), NT)

    per_tile = NT // hd

    def projections():
        def rotated(n, carry):
            y = jnp.dot(ha[...], wqkv[:, cols(n)], preferred_element_type=jnp.float32)
            for j in range(per_tile):
                head = y[:, j * hd:(j + 1) * hd]
                turned = head * cos_ref[...] + pltpu.roll(head, hd // 2, 1) * sin_ref[...]
                qkv[n * per_tile + j] = turned.astype(qkv.dtype)
            return carry
        lax.fori_loop(0, 2 * qd // NT, rotated, 0, unroll=2)

        def plain(n, carry):
            y = jnp.dot(ha[...], wqkv[:, cols(n)], preferred_element_type=jnp.float32)
            for j in range(per_tile):
                qkv[n * per_tile + j] = y[:, j * hd:(j + 1) * hd].astype(qkv.dtype)
            return carry
        lax.fori_loop(2 * qd // NT, 3 * qd // NT, plain, 0, unroll=True)

    def attention():
        for h in range(heads):
            scores = lax.dot_general(qkv[h], qkv[heads + h], (((1,), (1,)), ((), ())), preferred_element_type=jnp.float32) * (hd ** -0.5)
            floor = mask_ref[...]
            scores = jnp.where(floor == 0.0, scores, floor)
            raised = jnp.exp(scores - jnp.max(scores, axis=-1, keepdims=True))
            probs = (raised * (1.0 / jnp.sum(raised, axis=-1, keepdims=True))).astype(qkv.dtype)
            act[:, h * hd:(h + 1) * hd] = jnp.dot(probs, qkv[2 * heads + h], preferred_element_type=jnp.float32).astype(act.dtype)

    def mlp_up():
        def tile(n, carry):
            u = jnp.dot(hm[...], wup[:, cols(n)], preferred_element_type=jnp.float32)
            g = 0.5 * u * (1.0 + lax.erf(u * (0.5 ** 0.5)))
            act[:, pl.ds(pl.multiple_of(qd + n * NT, NT), NT)] = g.astype(act.dtype)
            return carry
        lax.fori_loop(0, ff // NT, tile, 0, unroll=2)

    def project_out(c):
        def tile(n, carry):
            o = jnp.dot(act[...], wod[:, cols(n)], preferred_element_type=jnp.float32).astype(part.dtype)
            for b in range(tp):
                part[c % NP, b, :, cols(n)] = o[b * rb:(b + 1) * rb]
            return carry
        lax.fori_loop(0, d_model // NT, tile, 0, unroll=2)

    def holds(c):
        return (c >= 0) & (c < nc)

    def weights_ready(c, ks):
        @pl.when((c == 0) | (c == nc))
        def _():
            for k in ks:
                weight_copies[k].wait()

    def swap_weights(c, ks):
        @pl.when(front & (c == nc - 1))
        def _():
            for k in ks:
                lend_copies[k].wait_recv()
                swap_copies[k].start()

    def heads_step(c, lo):
        @pl.when(c == nc)
        def _():
            for k in range(3):
                swap_copies[k].wait()
        weights_ready(c, (3,))
        norms(c)
        projections()
        swap_weights(c, (0, 1, 2, 3))
        attention()

    def up_step(c, lo):
        weights_ready(c, (4,))
        mlp_up()
        swap_weights(c, (4,))

    def out_step(c, lo):
        weights_ready(c, (5, 6))
        ag_drain(c)
        on(c - NP >= lo, lambda: rs_drain(c - NP))
        project_out(c)
        swap_weights(c, (5, 6))

    steps = {
        "gather0": lambda c, lo: ag_start(c),
        "gather1": lambda c, lo: ag_hop(c, 1),
        "gather2": lambda c, lo: ag_hop(c, 2),
        "lay_q": lambda c, lo: on((s == 0) & (c == 0), lambda: lay(0)),
        "lay_k": lambda c, lo: on((s == 0) & (c == 0), lambda: lay(1)),
        "lay_v": lambda c, lo: on((s == 0) & (c == 0), lambda: lay(2)),
        "arrive": lambda c, lo: ag_hop(c, last),
        "heads": heads_step,
        "up": up_step,
        "out": out_step,
        "scatter0": lambda c, lo: rs_hop(c, 0),
        "scatter1": lambda c, lo: rs_hop(c, 1),
        "scatter2": lambda c, lo: rs_hop(c, 2),
        "finish": lambda c, lo: finish(c),
    }
    span = max(behind for _, behind in TURN)

    def segment(k, carry):
        lo = k * nc
        hi = jnp.where(front, jnp.where(k == 0, nc, nc + nl), jnp.where(k == 0, nc - nl, nc))

        def turn(i, carry):
            for name, behind in TURN:
                c = i - behind
                on((c >= lo) & (c < hi), functools.partial(steps[name], c, lo))
            return carry

        lax.fori_loop(lo, jnp.where(hi > lo, hi + span, lo), turn, 0)
        for back in range(1, NP + 1):
            on(hi - back >= lo, lambda: rs_drain(hi - back))
        return carry

    lax.fori_loop(0, 2, segment, 0)

    @pl.when(has_next)
    def _():
        def sent(v, carry):
            fwd_copy(v).wait_send()
            return carry
        lax.fori_loop(0, jnp.where(s < half - 1, nc, nc - nl), sent, 0)

    for k in range(nl):
        on(s == half - 1, turn_copy(nc - nl + k).wait_send)
        on(s < half - 1, next_late_copy(nc + k).wait_send)
        on(front, home_copy(nc + k).wait_send)

    @pl.when(helper)
    def _():
        def sent_early(c, carry):
            for j in range(1, tp):
                share_copy(c, j).wait_send()
                hand_copy(c, j).wait_send()
            return carry
        lax.fori_loop(1, ne + 1, sent_early, 0)

    @pl.when(s >= half)
    def _():
        for copy in lend_copies:
            copy.wait_send()
        for k in range(nl):
            c = nc - nl + k
            pltpu.make_async_copy(x_hbm.at[0], xin.at[0], xin_sem.at[c]).wait()


def solution(mesh):
    tp, pp = mesh.shape["tp"], mesh.shape["pp"]

    def stage_body(x_in, ln_params, w_q, w_k, w_v, w_o, w_up, w_down):
        num_micro, batch_dim, tok, d_model = x_in.shape
        heads, hd = w_k.shape[2:]
        ff = w_up.shape[2]
        seqs = batch_dim // CHUNKS_PER_MICRO
        nc = num_micro * CHUNKS_PER_MICRO
        rb = seqs * tok
        rows = tp * rb
        qd = heads * hd
        bf16, f32 = jnp.bfloat16, jnp.float32

        cos_tab, sin_tab = rope_tables(tp * tok, hd)
        cos_full = jnp.concatenate([cos_tab, cos_tab], axis=-1)
        sin_full = jnp.concatenate([-sin_tab, sin_tab], axis=-1)

        any_spec = pl.BlockSpec(memory_space=pl.ANY)
        vmem_spec = pl.BlockSpec(memory_space=pltpu.VMEM)
        dma = pltpu.SemaphoreType.DMA
        flops = 2 * num_micro * tp * batch_dim * tok * (3 * qd * d_model + qd * d_model + 2 * ff * d_model)
        out, *_ = pl.pallas_call(
            functools.partial(pipeline_kernel, (nc, LATE, EARLY, tp, pp, heads, hd, tok)),
            out_shape=[pltpu.VMEM((nc, rb, d_model), bf16)] + [jax.ShapeDtypeStruct((d_model, qd), bf16)] * 3 + [
                jax.ShapeDtypeStruct((4, d_model), f32), jax.ShapeDtypeStruct((d_model, ff), bf16),
                jax.ShapeDtypeStruct((qd, d_model), bf16), jax.ShapeDtypeStruct((ff, d_model), bf16)],
            in_specs=[any_spec, vmem_spec, vmem_spec] + [any_spec] * 7,
            out_specs=[vmem_spec] + [any_spec] * 7,
            scratch_shapes=[
                pltpu.VMEM((3, d_model, heads, hd), bf16),
                pltpu.VMEM((d_model, 3 * qd), bf16),
                pltpu.VMEM((4, d_model), f32),
                pltpu.VMEM((d_model, ff), bf16),
                pltpu.VMEM((qd + ff, d_model), bf16),
                pltpu.VMEM((LATE, rb, d_model), bf16),
                pltpu.VMEM((EARLY, tp, rb, d_model), bf16),
                pltpu.VMEM((NX, tp, rb, d_model), bf16),
                pltpu.VMEM((NR, 2, tp - 1, rb, d_model), bf16),
                pltpu.VMEM((NP, tp, rb, d_model), bf16),
                pltpu.VMEM((rows, d_model), bf16),
                pltpu.VMEM((rows, d_model), bf16),
                pltpu.VMEM((3 * heads, rows, hd), bf16),
                pltpu.VMEM((rows, qd + ff), bf16),
                pltpu.VMEM((rows, rows), f32),
                pltpu.VMEM((rows, hd), f32),
                pltpu.VMEM((rows, hd), f32),
                dma((7,)),
                dma((nc + LATE,)),
                dma((NS, 2, tp - 1)),
                dma((NS, 2, tp - 1)),
                dma((NS, 2, tp - 1)),
                dma((NS, 2, tp - 1)),
                dma((nc + LATE,)),
                dma((LATE,)),
                dma((7,)),
                dma((7,)),
                dma((EARLY, tp)),
                dma((EARLY, tp)),
                dma((EARLY, tp)),
                dma((EARLY, tp)),
            ],
            compiler_params=pltpu.CompilerParams(collective_id=0, has_side_effects=True, vmem_limit_bytes=52 * 2 ** 20),
            cost_estimate=pl.CostEstimate(flops=flops, bytes_accessed=50 * 2 ** 20, transcendentals=0),
            name="pipeline",
        )(x_in.reshape(nc, rb, d_model), cos_full, sin_full, w_q.reshape(d_model, heads, hd), w_k[0], w_v[0], ln_params[0], w_up[0], w_o.reshape(qd, d_model), w_down[0])
        return out.reshape(1, num_micro, batch_dim, tok, d_model)

    in_specs = (P(None, "dp", "tp", None), P("pp", None, None), P("pp", None, "tp", None, None), P("pp", None, "tp", None), P("pp", None, "tp", None), P("pp", "tp", None, None, None), P("pp", None, "tp"), P("pp", "tp", None))
    return jax.shard_map(stage_body, mesh=mesh, in_specs=in_specs, out_specs=P("pp", None, "dp", "tp", None), check_vma=False)
```

```python
import functools

import jax
import jax.numpy as jnp
from jax import lax
from jax.experimental import pallas as pl
from jax.experimental.pallas import tpu as pltpu
from jax.sharding import PartitionSpec as P

LN_EPS = 1e-5
ROPE_BASE = 10000.0
CHUNKS_PER_MICRO = 8
NT = 256
NX, NR, NP, NS = 4, 4, 3, 4
LATE = 3
EARLY = 16
AHEAD = 4
TURN = (("gather0", 0), ("scatter1", 3), ("gather2", 1), ("up", 2), ("finish", 4), ("out", 2), ("scatter0", 2), ("lay_q", 0), ("gather1", 0), ("lay_k", 0), ("lay_v", 1), ("arrive", 1), ("scatter2", 3), ("heads", 1))
MESH = pl.DeviceIdType.MESH


def rope_tables(seq_len, head_dim):
    positions = jnp.arange(seq_len, dtype=jnp.float32)
    inv_freq = ROPE_BASE ** (-2.0 * jnp.arange(head_dim // 2, dtype=jnp.float32) / head_dim)
    angles = positions[:, None] * inv_freq[None, :]
    return jnp.cos(angles), jnp.sin(angles)


def pipeline_kernel(dims, x_hbm, cos_tab, sin_tab, wq_hbm, wk_hbm, wv_hbm, ln_hbm, wup_hbm, wo_hbm, wdn_hbm,
                    xin, lq_hbm, lk_hbm, lv_hbm, lln_hbm, lup_hbm, lo_hbm, ldn_hbm,
                    raw, wqkv, ln_ref, wup, wod, xlate, early, xfull, rbuf, part, ha, hm, qkv, act, mask_ref, cos_ref, sin_ref,
                    w_sem, xin_sem, ag_ss, ag_rs, rs_ss, rs_rs, fwd_sem, home_sem, lw_ss, lw_rs, es_ss, es_rs, eh_ss, eh_rs):
    nc, nl, ne, tp, pp, heads, hd, tok = dims
    rb, d_model = xin.shape[1:]
    rows = tp * rb
    ff = wup.shape[1]
    qd = heads * hd
    last = tp - 1
    z = lax.axis_index("tp")
    s = lax.axis_index("pp")
    has_left, has_right = z > 0, z < last
    has_prev, has_next = s > 0, s < pp - 1
    half = pp // 2
    front = s < half

    def on(cond, fn):
        pl.when(cond)(fn)

    def remote(src, dst, ss, rs, to):
        return pltpu.make_async_remote_copy(src_ref=src, dst_ref=dst, send_sem=ss, recv_sem=rs, device_id=to, device_id_type=MESH)

    def neighbour(way):
        return {"tp": jnp.minimum(z + 1, last) if way == 0 else jnp.maximum(z - 1, 0)}

    def ag_copy(c, h, way, first=None):
        b = jnp.clip(z - h if way == 0 else z + h, 0, last)
        src = (first if first is not None else xin.at[0]) if h == 0 else xfull.at[c % NX, b]
        return remote(src, xfull.at[c % NX, b], ag_ss.at[c % NS, way, h], ag_rs.at[c % NS, way, h], neighbour(way))

    def ag_sends(h, way):
        return has_right & (z >= h) if way == 0 else has_left & (z + h <= last)

    def ag_gets(h, way):
        return z - 1 - h >= 0 if way == 0 else z + 1 + h <= last

    def rs_copy(c, h, way):
        d = jnp.clip(z + last - h if way == 0 else z - last + h, 0, last)
        return remote(part.at[c % NP, d], rbuf.at[c % NR, way, h], rs_ss.at[c % NS, way, h], rs_rs.at[c % NS, way, h], neighbour(way))

    def rs_sends(h, way):
        return z <= h if way == 0 else last - z <= h

    def rs_sends_all(h, way):
        return rs_sends(h, way) & (has_right if way == 0 else has_left)

    def rs_gets(h, way):
        return has_left & (z - 1 <= h) if way == 0 else has_right & (last - 1 - z <= h)

    def fwd_copy(v):
        return remote(xin.at[v], xin.at[v], fwd_sem.at[v], xin_sem.at[v], {"pp": jnp.minimum(s + 1, pp - 1)})

    def turn_copy(v):
        return remote(xin.at[v], xlate.at[v - (nc - nl)], fwd_sem.at[v], xin_sem.at[v + nl], {"pp": 0})

    def next_late_copy(v):
        return remote(xlate.at[v - nc], xlate.at[v - nc], fwd_sem.at[v], xin_sem.at[v], {"pp": jnp.minimum(s + 1, pp - 1)})

    def home_copy(v):
        return remote(xlate.at[v - nc], xin.at[v - nl], home_sem.at[v - nc], xin_sem.at[v - nl], {"pp": jnp.minimum(s + half, pp - 1)})

    own = [wq_hbm, wk_hbm, wv_hbm, ln_hbm, wup_hbm, wo_hbm, wdn_hbm]
    late = [lq_hbm, lk_hbm, lv_hbm, lln_hbm, lup_hbm, lo_hbm, ldn_hbm]
    held = [wqkv.at[:, pl.ds(0, qd)], wqkv.at[:, pl.ds(qd, qd)], wqkv.at[:, pl.ds(2 * qd, qd)], ln_ref, wup, wod.at[pl.ds(0, qd)], wod.at[pl.ds(qd, ff)]]
    weight_copies = [pltpu.make_async_copy(src, dst, w_sem.at[k]) for k, (src, dst) in enumerate(zip(own, [raw.at[0], raw.at[1], raw.at[2]] + held[3:]))]
    swap_copies = [pltpu.make_async_copy(src, dst, w_sem.at[k]) for k, (src, dst) in enumerate(zip(late, held))]
    lend_copies = [remote(src, dst, lw_ss.at[k], lw_rs.at[k], {"pp": jnp.maximum(s - half, 0)}) for k, (src, dst) in enumerate(zip(held[:3] + own[3:], late))]

    helper = s == pp - 1

    def is_early(c):
        return (s == 0) & (c >= 1) & (c <= ne)

    def share_copy(c, h, way):
        b = jnp.clip(z - h if way == 0 else z + h, 0, last)
        src = x_hbm.at[c] if h == 0 else early.at[c - 1, b]
        return remote(src, early.at[c - 1, b], es_ss.at[c - 1, way, h], es_rs.at[c - 1, way, h], neighbour(way))

    def hand_copy(c, b):
        return remote(early.at[c - 1, b], early.at[c - 1, b], eh_ss.at[c - 1, b], eh_rs.at[c - 1, b], {"pp": 0})

    def share_hop(c, h):
        for way in (0, 1):
            if h > 0:
                @pl.when(ag_gets(h - 1, way))
                def _(way=way):
                    share_copy(c, h - 1, way).wait_recv()
                    if h < last:
                        on(ag_sends(h, way), share_copy(c, h, way).start)
                    hand_copy(c, z - h if way == 0 else z + h).start()
            else:
                on(ag_sends(0, way), share_copy(c, 0, way).start)

    barrier = pltpu.get_barrier_semaphore()
    for j in range(1, tp):
        pl.semaphore_signal(barrier, inc=1, device_id={"tp": lax.rem(z + j, tp)}, device_id_type=MESH)
    for j in range(1, pp):
        pl.semaphore_signal(barrier, inc=1, device_id={"pp": lax.rem(s + j, pp)}, device_id_type=MESH)

    def load(c):
        return pltpu.make_async_copy(x_hbm.at[c], xin.at[c], xin_sem.at[c])

    for c in range(AHEAD):
        on(s == 0, load(c).start)
    for copy in weight_copies:
        copy.start()

    lay_rows = 64

    def lay(k):
        weight_copies[k].wait()

        def some(t, carry):
            at = pl.ds(pl.multiple_of(t * lay_rows, lay_rows), lay_rows)
            wqkv[at, k * qd:(k + 1) * qd] = raw[k, at].reshape(lay_rows, qd)
            return carry
        lax.fori_loop(0, d_model // lay_rows, some, 0)

    @pl.when(s > 0)
    def _():
        for k in range(3):
            lay(k)

    for way, alone in ((0, z == 0), (1, z == last)):
        @pl.when(alone)
        def _(way=way):
            for k in range(NR):
                rbuf[k, way, last - 1] = jnp.zeros(rbuf.shape[3:], rbuf.dtype)

    row = lax.broadcasted_iota(jnp.int32, (rows, rows), 0)
    col = lax.broadcasted_iota(jnp.int32, (rows, rows), 1)
    same = row % rb // tok == col % rb // tok
    later = row // rb * tok + row % tok >= col // rb * tok + col % tok
    mask_ref[...] = jnp.where(same, jnp.where(later, 0.0, -1e30), -3e38)
    for b in range(tp):
        for q in range(rb // tok):
            to, of = slice(b * rb + q * tok, b * rb + (q + 1) * tok), slice(b * tok, (b + 1) * tok)
            cos_ref[to] = cos_tab[of]
            sin_ref[to] = sin_tab[of]

    pl.semaphore_wait(barrier, tp - 1 + pp - 1)

    def lend():
        for copy in lend_copies:
            copy.start()

    @pl.when(helper)
    def _():
        def share(i, carry):
            for h in range(tp):
                on((i - h >= 1) & (i - h <= ne), functools.partial(share_hop, i - h, h))
            return carry
        lax.fori_loop(1, ne + tp, share, 0)
        lend()

    def in_its_place(c, fn):
        on(c < nc, lambda: fn(xin.at[c]))
        on(c >= nc, lambda: fn(xlate.at[c - nc]))

    def ag_start(c):
        on((s == 0) & (c + AHEAD < nc), lambda: load(c + AHEAD).start())
        pltpu.make_async_copy(x_hbm.at[0], xin.at[0], xin_sem.at[c]).wait()
        on((s >= half) & ~helper & (c == 2), lend)

        def send(place):
            for way in (0, 1):
                on(ag_sends(0, way) & ~is_early(c), ag_copy(c, 0, way, place).start)
            xfull[c % NX, z] = place[...]
        in_its_place(c, send)

    def ag_hop(c, h):
        @pl.when(~is_early(c))
        def _():
            for way in (0, 1):
                on(ag_gets(h - 1, way), ag_copy(c, h - 1, way).wait_recv)
                if h < last:
                    on(ag_sends(h, way), ag_copy(c, h, way).start)

        if h == last:
            @pl.when(is_early(c))
            def _():
                for j in range(1, tp):
                    b = lax.rem(z + j, tp)
                    hand_copy(c, b).wait_recv()
                    xfull[c % NX, b] = early[c - 1, b]

    def ag_drain(c):
        @pl.when(~is_early(c))
        def _():
            for h in range(last):
                for way in (0, 1):
                    on(ag_sends(h, way), ag_copy(c, h, way).wait_send)

    def rs_hop(c, h):
        for way in (0, 1):
            @pl.when(rs_sends_all(h, way))
            def _(way=way):
                if h > 0:
                    @pl.when(rs_gets(h - 1, way))
                    def _():
                        rs_copy(c, h - 1, way).wait_recv()
                        d = z + last - h if way == 0 else z - last + h
                        mine = part[c % NP, d].astype(jnp.float32)
                        part[c % NP, d] = (mine + rbuf[c % NR, way, h - 1].astype(jnp.float32)).astype(part.dtype)
                rs_copy(c, h, way).start()

    def rs_drain(c):
        for h in range(last):
            for way in (0, 1):
                on(rs_sends_all(h, way), rs_copy(c, h, way).wait_send)

    def finish(c):
        for way in (0, 1):
            on(rs_gets(last - 1, way), rs_copy(c, last - 1, way).wait_recv)
        f32 = jnp.float32

        def add(place):
            total = place[...].astype(f32) + part[c % NP, z].astype(f32)
            total = total + rbuf[c % NR, 0, last - 1].astype(f32) + rbuf[c % NR, 1, last - 1].astype(f32)
            place[...] = total.astype(xin.dtype)
        in_its_place(c, add)
        turns = (s == half - 1) & (c >= nc - nl)
        on(has_next & (c < nc) & ~turns, lambda: fwd_copy(c).start())
        on(turns & (c < nc), lambda: turn_copy(c).start())
        on((s < half - 1) & (c >= nc), lambda: next_late_copy(c).start())
        on(front & (c >= nc), lambda: home_copy(c).start())

    lt = min(rb, 32)
    per_block = rb // lt

    def norms(c):
        def tile(t, carry):
            x_f32 = xfull[c % NX, t // per_block, pl.ds((t % per_block) * lt, lt)].astype(jnp.float32)
            row_mean = jnp.mean(x_f32, axis=-1, keepdims=True)
            centred = x_f32 - row_mean
            variance = jnp.mean(centred * centred, axis=-1, keepdims=True)
            unit = centred * lax.rsqrt(variance + LN_EPS)
            at = pl.ds(pl.multiple_of(t * lt, lt), lt)
            ha[at] = (unit * ln_ref[0:1] + ln_ref[1:2]).astype(ha.dtype)
            hm[at] = (unit * ln_ref[2:3] + ln_ref[3:4]).astype(hm.dtype)
            return carry
        lax.fori_loop(0, rows // lt, tile, 0, unroll=2)

    def cols(n):
        return pl.ds(pl.multiple_of(n * NT, NT), NT)

    per_tile = NT // hd

    def projections():
        def rotated(n, carry):
            y = jnp.dot(ha[...], wqkv[:, cols(n)], preferred_element_type=jnp.float32)
            for j in range(per_tile):
                head = y[:, j * hd:(j + 1) * hd]
                turned = head * cos_ref[...] + pltpu.roll(head, hd // 2, 1) * sin_ref[...]
                qkv[n * per_tile + j] = turned.astype(qkv.dtype)
            return carry
        lax.fori_loop(0, 2 * qd // NT, rotated, 0, unroll=2)

        def plain(n, carry):
            y = jnp.dot(ha[...], wqkv[:, cols(n)], preferred_element_type=jnp.float32)
            for j in range(per_tile):
                qkv[n * per_tile + j] = y[:, j * hd:(j + 1) * hd].astype(qkv.dtype)
            return carry
        lax.fori_loop(2 * qd // NT, 3 * qd // NT, plain, 0, unroll=True)

    def attention():
        for h in range(heads):
            scores = lax.dot_general(qkv[h], qkv[heads + h], (((1,), (1,)), ((), ())), preferred_element_type=jnp.float32) * (hd ** -0.5)
            floor = mask_ref[...]
            scores = jnp.where(floor == 0.0, scores, floor)
            raised = jnp.exp(scores - jnp.max(scores, axis=-1, keepdims=True))
            probs = (raised * (1.0 / jnp.sum(raised, axis=-1, keepdims=True))).astype(qkv.dtype)
            act[:, h * hd:(h + 1) * hd] = jnp.dot(probs, qkv[2 * heads + h], preferred_element_type=jnp.float32).astype(act.dtype)

    def mlp_up():
        def tile(n, carry):
            u = jnp.dot(hm[...], wup[:, cols(n)], preferred_element_type=jnp.float32)
            g = 0.5 * u * (1.0 + lax.erf(u * (0.5 ** 0.5)))
            act[:, pl.ds(pl.multiple_of(qd + n * NT, NT), NT)] = g.astype(act.dtype)
            return carry
        lax.fori_loop(0, ff // NT, tile, 0, unroll=2)

    def project_out(c):
        def tile(n, carry):
            o = jnp.dot(act[...], wod[:, cols(n)], preferred_element_type=jnp.float32).astype(part.dtype)
            for b in range(tp):
                part[c % NP, b, :, cols(n)] = o[b * rb:(b + 1) * rb]
            return carry
        lax.fori_loop(0, d_model // NT, tile, 0, unroll=2)

    def holds(c):
        return (c >= 0) & (c < nc)

    def weights_ready(c, ks):
        @pl.when((c == 0) | (c == nc))
        def _():
            for k in ks:
                weight_copies[k].wait()

    def swap_weights(c, ks):
        @pl.when(front & (c == nc - 1))
        def _():
            for k in ks:
                lend_copies[k].wait_recv()
                swap_copies[k].start()

    def heads_step(c, lo):
        @pl.when(c == nc)
        def _():
            for k in range(3):
                swap_copies[k].wait()
        weights_ready(c, (3,))
        norms(c)
        projections()
        swap_weights(c, (0, 1, 2, 3))
        attention()

    def up_step(c, lo):
        weights_ready(c, (4,))
        mlp_up()
        swap_weights(c, (4,))

    def out_step(c, lo):
        weights_ready(c, (5, 6))
        ag_drain(c)
        on(c - NP >= lo, lambda: rs_drain(c - NP))
        project_out(c)
        swap_weights(c, (5, 6))

    steps = {
        "gather0": lambda c, lo: ag_start(c),
        "gather1": lambda c, lo: ag_hop(c, 1),
        "gather2": lambda c, lo: ag_hop(c, 2),
        "lay_q": lambda c, lo: on((s == 0) & (c == 0), lambda: lay(0)),
        "lay_k": lambda c, lo: on((s == 0) & (c == 0), lambda: lay(1)),
        "lay_v": lambda c, lo: on((s == 0) & (c == 0), lambda: lay(2)),
        "arrive": lambda c, lo: ag_hop(c, last),
        "heads": heads_step,
        "up": up_step,
        "out": out_step,
        "scatter0": lambda c, lo: rs_hop(c, 0),
        "scatter1": lambda c, lo: rs_hop(c, 1),
        "scatter2": lambda c, lo: rs_hop(c, 2),
        "finish": lambda c, lo: finish(c),
    }
    span = max(behind for _, behind in TURN)

    def segment(k, carry):
        lo = k * nc
        hi = jnp.where(front, jnp.where(k == 0, nc, nc + nl), jnp.where(k == 0, nc - nl, nc))

        def turn(i, carry):
            for name, behind in TURN:
                c = i - behind
                on((c >= lo) & (c < hi), functools.partial(steps[name], c, lo))
            return carry

        lax.fori_loop(lo, jnp.where(hi > lo, hi + span, lo), turn, 0)
        for back in range(1, NP + 1):
            on(hi - back >= lo, lambda: rs_drain(hi - back))
        return carry

    lax.fori_loop(0, 2, segment, 0)

    @pl.when(has_next)
    def _():
        def sent(v, carry):
            fwd_copy(v).wait_send()
            return carry
        lax.fori_loop(0, jnp.where(s < half - 1, nc, nc - nl), sent, 0)

    for k in range(nl):
        on(s == half - 1, turn_copy(nc - nl + k).wait_send)
        on(s < half - 1, next_late_copy(nc + k).wait_send)
        on(front, home_copy(nc + k).wait_send)

    @pl.when(helper)
    def _():
        def sent_early(c, carry):
            for h in range(last):
                for way in (0, 1):
                    on(ag_sends(h, way), share_copy(c, h, way).wait_send)
            for j in range(1, tp):
                hand_copy(c, lax.rem(z + j, tp)).wait_send()
            return carry
        lax.fori_loop(1, ne + 1, sent_early, 0)

    @pl.when(s >= half)
    def _():
        for copy in lend_copies:
            copy.wait_send()
        for k in range(nl):
            c = nc - nl + k
            pltpu.make_async_copy(x_hbm.at[0], xin.at[0], xin_sem.at[c]).wait()


def solution(mesh):
    tp, pp = mesh.shape["tp"], mesh.shape["pp"]

    def stage_body(x_in, ln_params, w_q, w_k, w_v, w_o, w_up, w_down):
        num_micro, batch_dim, tok, d_model = x_in.shape
        heads, hd = w_k.shape[2:]
        ff = w_up.shape[2]
        seqs = batch_dim // CHUNKS_PER_MICRO
        nc = num_micro * CHUNKS_PER_MICRO
        rb = seqs * tok
        rows = tp * rb
        qd = heads * hd
        bf16, f32 = jnp.bfloat16, jnp.float32

        cos_tab, sin_tab = rope_tables(tp * tok, hd)
        cos_full = jnp.concatenate([cos_tab, cos_tab], axis=-1)
        sin_full = jnp.concatenate([-sin_tab, sin_tab], axis=-1)

        any_spec = pl.BlockSpec(memory_space=pl.ANY)
        vmem_spec = pl.BlockSpec(memory_space=pltpu.VMEM)
        dma = pltpu.SemaphoreType.DMA
        flops = 2 * num_micro * tp * batch_dim * tok * (3 * qd * d_model + qd * d_model + 2 * ff * d_model)
        out, *_ = pl.pallas_call(
            functools.partial(pipeline_kernel, (nc, LATE, EARLY, tp, pp, heads, hd, tok)),
            out_shape=[pltpu.VMEM((nc, rb, d_model), bf16)] + [jax.ShapeDtypeStruct((d_model, qd), bf16)] * 3 + [
                jax.ShapeDtypeStruct((4, d_model), f32), jax.ShapeDtypeStruct((d_model, ff), bf16),
                jax.ShapeDtypeStruct((qd, d_model), bf16), jax.ShapeDtypeStruct((ff, d_model), bf16)],
            in_specs=[any_spec, vmem_spec, vmem_spec] + [any_spec] * 7,
            out_specs=[vmem_spec] + [any_spec] * 7,
            scratch_shapes=[
                pltpu.VMEM((3, d_model, heads, hd), bf16),
                pltpu.VMEM((d_model, 3 * qd), bf16),
                pltpu.VMEM((4, d_model), f32),
                pltpu.VMEM((d_model, ff), bf16),
                pltpu.VMEM((qd + ff, d_model), bf16),
                pltpu.VMEM((LATE, rb, d_model), bf16),
                pltpu.VMEM((EARLY, tp, rb, d_model), bf16),
                pltpu.VMEM((NX, tp, rb, d_model), bf16),
                pltpu.VMEM((NR, 2, tp - 1, rb, d_model), bf16),
                pltpu.VMEM((NP, tp, rb, d_model), bf16),
                pltpu.VMEM((rows, d_model), bf16),
                pltpu.VMEM((rows, d_model), bf16),
                pltpu.VMEM((3 * heads, rows, hd), bf16),
                pltpu.VMEM((rows, qd + ff), bf16),
                pltpu.VMEM((rows, rows), f32),
                pltpu.VMEM((rows, hd), f32),
                pltpu.VMEM((rows, hd), f32),
                dma((7,)),
                dma((nc + LATE,)),
                dma((NS, 2, tp - 1)),
                dma((NS, 2, tp - 1)),
                dma((NS, 2, tp - 1)),
                dma((NS, 2, tp - 1)),
                dma((nc + LATE,)),
                dma((LATE,)),
                dma((7,)),
                dma((7,)),
                dma((EARLY, 2, tp - 1)),
                dma((EARLY, 2, tp - 1)),
                dma((EARLY, tp)),
                dma((EARLY, tp)),
            ],
            compiler_params=pltpu.CompilerParams(collective_id=0, has_side_effects=True, vmem_limit_bytes=52 * 2 ** 20),
            cost_estimate=pl.CostEstimate(flops=flops, bytes_accessed=50 * 2 ** 20, transcendentals=0),
            name="pipeline",
        )(x_in.reshape(nc, rb, d_model), cos_full, sin_full, w_q.reshape(d_model, heads, hd), w_k[0], w_v[0], ln_params[0], w_up[0], w_o.reshape(qd, d_model), w_down[0])
        return out.reshape(1, num_micro, batch_dim, tok, d_model)

    in_specs = (P(None, "dp", "tp", None), P("pp", None, None), P("pp", None, "tp", None, None), P("pp", None, "tp", None), P("pp", None, "tp", None), P("pp", "tp", None, None, None), P("pp", None, "tp"), P("pp", "tp", None))
    return jax.shard_map(stage_body, mesh=mesh, in_specs=in_specs, out_specs=P("pp", None, "dp", "tp", None), check_vma=False)
```

```python
import functools

import jax
import jax.numpy as jnp
from jax import lax
from jax.experimental import pallas as pl
from jax.experimental.pallas import tpu as pltpu
from jax.sharding import PartitionSpec as P

LN_EPS = 1e-5
ROPE_BASE = 10000.0
CHUNKS_PER_MICRO = 8
NT = 256
NX, NR, NP, NS = 4, 4, 3, 4
LATE = 5
EARLY = 24
AHEAD = 4
TURN = (("gather0", 0), ("arrive", 2), ("scatter2", 4), ("heads", 2), ("gather2", 1), ("lay_v", 1), ("scatter1", 3), ("up", 2), ("lay_q", 0), ("gather1", 0), ("lay_k", 0), ("out", 2), ("scatter0", 2), ("finish", 4))
MESH = pl.DeviceIdType.MESH


def rope_tables(seq_len, head_dim):
    positions = jnp.arange(seq_len, dtype=jnp.float32)
    inv_freq = ROPE_BASE ** (-2.0 * jnp.arange(head_dim // 2, dtype=jnp.float32) / head_dim)
    angles = positions[:, None] * inv_freq[None, :]
    return jnp.cos(angles), jnp.sin(angles)


def pipeline_kernel(dims, x_hbm, cos_tab, sin_tab, wq_hbm, wk_hbm, wv_hbm, ln_hbm, wup_hbm, wo_hbm, wdn_hbm,
                    xin, lq_hbm, lk_hbm, lv_hbm, lln_hbm, lup_hbm, lo_hbm, ldn_hbm,
                    raw, wqkv, ln_ref, wup, wod, xlate, early, xfull, rbuf, part, ha, hm, qkv, act, mask_ref, cos_ref, sin_ref,
                    w_sem, xin_sem, ag_ss, ag_rs, rs_ss, rs_rs, fwd_sem, home_sem, lw_ss, lw_rs, es_ss, es_rs, eh_ss, eh_rs):
    nc, nl, ne, tp, pp, heads, hd, tok = dims
    rb, d_model = xin.shape[1:]
    rows = tp * rb
    ff = wup.shape[1]
    qd = heads * hd
    last = tp - 1
    z = lax.axis_index("tp")
    s = lax.axis_index("pp")
    has_left, has_right = z > 0, z < last
    has_prev, has_next = s > 0, s < pp - 1
    half = pp // 2
    front = s < half

    def on(cond, fn):
        pl.when(cond)(fn)

    def remote(src, dst, ss, rs, to):
        return pltpu.make_async_remote_copy(src_ref=src, dst_ref=dst, send_sem=ss, recv_sem=rs, device_id=to, device_id_type=MESH)

    def neighbour(way):
        return {"tp": jnp.minimum(z + 1, last) if way == 0 else jnp.maximum(z - 1, 0)}

    def ag_copy(c, h, way, first=None):
        b = jnp.clip(z - h if way == 0 else z + h, 0, last)
        src = (first if first is not None else xin.at[0]) if h == 0 else xfull.at[c % NX, b]
        return remote(src, xfull.at[c % NX, b], ag_ss.at[c % NS, way, h], ag_rs.at[c % NS, way, h], neighbour(way))

    def ag_sends(h, way):
        return has_right & (z >= h) if way == 0 else has_left & (z + h <= last)

    def ag_gets(h, way):
        return z - 1 - h >= 0 if way == 0 else z + 1 + h <= last

    def rs_copy(c, h, way):
        d = jnp.clip(z + last - h if way == 0 else z - last + h, 0, last)
        return remote(part.at[c % NP, d], rbuf.at[c % NR, way, h], rs_ss.at[c % NS, way, h], rs_rs.at[c % NS, way, h], neighbour(way))

    def rs_sends(h, way):
        return z <= h if way == 0 else last - z <= h

    def rs_sends_all(h, way):
        return rs_sends(h, way) & (has_right if way == 0 else has_left)

    def rs_gets(h, way):
        return has_left & (z - 1 <= h) if way == 0 else has_right & (last - 1 - z <= h)

    def fwd_copy(v):
        return remote(xin.at[v], xin.at[v], fwd_sem.at[v], xin_sem.at[v], {"pp": jnp.minimum(s + 1, pp - 1)})

    def turn_copy(v):
        return remote(xin.at[v], xlate.at[v - (nc - nl)], fwd_sem.at[v], xin_sem.at[v + nl], {"pp": 0})

    def next_late_copy(v):
        return remote(xlate.at[v - nc], xlate.at[v - nc], fwd_sem.at[v], xin_sem.at[v], {"pp": jnp.minimum(s + 1, pp - 1)})

    def home_copy(v):
        return remote(xlate.at[v - nc], xin.at[v - nl], home_sem.at[v - nc], xin_sem.at[v - nl], {"pp": jnp.minimum(s + half, pp - 1)})

    own = [wq_hbm, wk_hbm, wv_hbm, ln_hbm, wup_hbm, wo_hbm, wdn_hbm]
    late = [lq_hbm, lk_hbm, lv_hbm, lln_hbm, lup_hbm, lo_hbm, ldn_hbm]
    held = [wqkv.at[:, pl.ds(0, qd)], wqkv.at[:, pl.ds(qd, qd)], wqkv.at[:, pl.ds(2 * qd, qd)], ln_ref, wup, wod.at[pl.ds(0, qd)], wod.at[pl.ds(qd, ff)]]
    weight_copies = [pltpu.make_async_copy(src, dst, w_sem.at[k]) for k, (src, dst) in enumerate(zip(own, [raw.at[0], raw.at[1], raw.at[2]] + held[3:]))]
    swap_copies = [pltpu.make_async_copy(src, dst, w_sem.at[k]) for k, (src, dst) in enumerate(zip(late, held))]
    lend_copies = [remote(src, dst, lw_ss.at[k], lw_rs.at[k], {"pp": jnp.maximum(s - half, 0)}) for k, (src, dst) in enumerate(zip(held[:3] + own[3:], late))]

    helper = s == pp - 1

    def is_early(c):
        return (s == 0) & (c >= 1) & (c <= ne)

    def share_copy(c, h, way):
        b = jnp.clip(z - h if way == 0 else z + h, 0, last)
        src = x_hbm.at[c] if h == 0 else early.at[c - 1, b]
        return remote(src, early.at[c - 1, b], es_ss.at[c - 1, way, h], es_rs.at[c - 1, way, h], neighbour(way))

    def hand_copy(c, b):
        return remote(early.at[c - 1, b], early.at[c - 1, b], eh_ss.at[c - 1, b], eh_rs.at[c - 1, b], {"pp": 0})

    def share_hop(c, h):
        for way in (0, 1):
            if h > 0:
                @pl.when(ag_gets(h - 1, way))
                def _(way=way):
                    share_copy(c, h - 1, way).wait_recv()
                    if h < last:
                        on(ag_sends(h, way), share_copy(c, h, way).start)
                    hand_copy(c, z - h if way == 0 else z + h).start()
            else:
                on(ag_sends(0, way), share_copy(c, 0, way).start)

    barrier = pltpu.get_barrier_semaphore()
    for j in range(1, tp):
        pl.semaphore_signal(barrier, inc=1, device_id={"tp": lax.rem(z + j, tp)}, device_id_type=MESH)
    for j in range(1, pp):
        pl.semaphore_signal(barrier, inc=1, device_id={"pp": lax.rem(s + j, pp)}, device_id_type=MESH)

    def load(c):
        return pltpu.make_async_copy(x_hbm.at[c], xin.at[c], xin_sem.at[c])

    for c in range(AHEAD):
        on(s == 0, load(c).start)
    for copy in weight_copies:
        copy.start()

    lay_rows = 64

    def lay(k):
        weight_copies[k].wait()

        def some(t, carry):
            at = pl.ds(pl.multiple_of(t * lay_rows, lay_rows), lay_rows)
            wqkv[at, k * qd:(k + 1) * qd] = raw[k, at].reshape(lay_rows, qd)
            return carry
        lax.fori_loop(0, d_model // lay_rows, some, 0)

    @pl.when(s > 0)
    def _():
        for k in range(3):
            lay(k)

    for way, alone in ((0, z == 0), (1, z == last)):
        @pl.when(alone)
        def _(way=way):
            for k in range(NR):
                rbuf[k, way, last - 1] = jnp.zeros(rbuf.shape[3:], rbuf.dtype)

    row = lax.broadcasted_iota(jnp.int32, (rows, rows), 0)
    col = lax.broadcasted_iota(jnp.int32, (rows, rows), 1)
    same = row % rb // tok == col % rb // tok
    later = row // rb * tok + row % tok >= col // rb * tok + col % tok
    mask_ref[...] = jnp.where(same, jnp.where(later, 0.0, -1e30), -3e38)
    for b in range(tp):
        for q in range(rb // tok):
            to, of = slice(b * rb + q * tok, b * rb + (q + 1) * tok), slice(b * tok, (b + 1) * tok)
            cos_ref[to] = cos_tab[of]
            sin_ref[to] = sin_tab[of]

    pl.semaphore_wait(barrier, tp - 1 + pp - 1)

    def lend():
        for copy in lend_copies:
            copy.start()

    @pl.when(helper)
    def _():
        def share(i, carry):
            for h in range(tp):
                on((i - h >= 1) & (i - h <= ne), functools.partial(share_hop, i - h, h))
            return carry
        lax.fori_loop(1, ne + tp, share, 0)
        lend()

    def in_its_place(c, fn):
        on(c < nc, lambda: fn(xin.at[c]))
        on(c >= nc, lambda: fn(xlate.at[c - nc]))

    def ag_start(c):
        on((s == 0) & (c + AHEAD < nc), lambda: load(c + AHEAD).start())
        pltpu.make_async_copy(x_hbm.at[0], xin.at[0], xin_sem.at[c]).wait()
        on((s >= half) & ~helper & (c == 2), lend)

        def send(place):
            for way in (0, 1):
                on(ag_sends(0, way) & ~is_early(c), ag_copy(c, 0, way, place).start)
            xfull[c % NX, z] = place[...]
        in_its_place(c, send)

    def ag_hop(c, h):
        @pl.when(~is_early(c))
        def _():
            for way in (0, 1):
                on(ag_gets(h - 1, way), ag_copy(c, h - 1, way).wait_recv)
                if h < last:
                    on(ag_sends(h, way), ag_copy(c, h, way).start)

        if h == last:
            @pl.when(is_early(c))
            def _():
                for j in range(1, tp):
                    b = lax.rem(z + j, tp)
                    hand_copy(c, b).wait_recv()
                    xfull[c % NX, b] = early[c - 1, b]

    def ag_drain(c):
        @pl.when(~is_early(c))
        def _():
            for h in range(last):
                for way in (0, 1):
                    on(ag_sends(h, way), ag_copy(c, h, way).wait_send)

    def rs_hop(c, h):
        for way in (0, 1):
            @pl.when(rs_sends_all(h, way))
            def _(way=way):
                if h > 0:
                    @pl.when(rs_gets(h - 1, way))
                    def _():
                        rs_copy(c, h - 1, way).wait_recv()
                        d = z + last - h if way == 0 else z - last + h
                        mine = part[c % NP, d].astype(jnp.float32)
                        part[c % NP, d] = (mine + rbuf[c % NR, way, h - 1].astype(jnp.float32)).astype(part.dtype)
                rs_copy(c, h, way).start()

    def rs_drain(c):
        for h in range(last):
            for way in (0, 1):
                on(rs_sends_all(h, way), rs_copy(c, h, way).wait_send)

    def finish(c):
        for way in (0, 1):
            on(rs_gets(last - 1, way), rs_copy(c, last - 1, way).wait_recv)
        f32 = jnp.float32

        def add(place):
            total = place[...].astype(f32) + part[c % NP, z].astype(f32)
            total = total + rbuf[c % NR, 0, last - 1].astype(f32) + rbuf[c % NR, 1, last - 1].astype(f32)
            place[...] = total.astype(xin.dtype)
        in_its_place(c, add)
        turns = (s == half - 1) & (c >= nc - nl)
        on(has_next & (c < nc) & ~turns, lambda: fwd_copy(c).start())
        on(turns & (c < nc), lambda: turn_copy(c).start())
        on((s < half - 1) & (c >= nc), lambda: next_late_copy(c).start())
        on(front & (c >= nc), lambda: home_copy(c).start())

    lt = min(rb, 32)
    per_block = rb // lt

    def norms(c):
        def tile(t, carry):
            x_f32 = xfull[c % NX, t // per_block, pl.ds((t % per_block) * lt, lt)].astype(jnp.float32)
            row_mean = jnp.mean(x_f32, axis=-1, keepdims=True)
            centred = x_f32 - row_mean
            variance = jnp.mean(centred * centred, axis=-1, keepdims=True)
            unit = centred * lax.rsqrt(variance + LN_EPS)
            at = pl.ds(pl.multiple_of(t * lt, lt), lt)
            ha[at] = (unit * ln_ref[0:1] + ln_ref[1:2]).astype(ha.dtype)
            hm[at] = (unit * ln_ref[2:3] + ln_ref[3:4]).astype(hm.dtype)
            return carry
        lax.fori_loop(0, rows // lt, tile, 0, unroll=2)

    def cols(n):
        return pl.ds(pl.multiple_of(n * NT, NT), NT)

    per_tile = NT // hd

    def projections():
        def rotated(n, carry):
            y = jnp.dot(ha[...], wqkv[:, cols(n)], preferred_element_type=jnp.float32)
            for j in range(per_tile):
                head = y[:, j * hd:(j + 1) * hd]
                turned = head * cos_ref[...] + pltpu.roll(head, hd // 2, 1) * sin_ref[...]
                qkv[n * per_tile + j] = turned.astype(qkv.dtype)
            return carry
        lax.fori_loop(0, 2 * qd // NT, rotated, 0, unroll=2)

        def plain(n, carry):
            y = jnp.dot(ha[...], wqkv[:, cols(n)], preferred_element_type=jnp.float32)
            for j in range(per_tile):
                qkv[n * per_tile + j] = y[:, j * hd:(j + 1) * hd].astype(qkv.dtype)
            return carry
        lax.fori_loop(2 * qd // NT, 3 * qd // NT, plain, 0, unroll=True)

    def attention():
        for h in range(heads):
            scores = lax.dot_general(qkv[h], qkv[heads + h], (((1,), (1,)), ((), ())), preferred_element_type=jnp.float32) * (hd ** -0.5)
            floor = mask_ref[...]
            scores = jnp.where(floor == 0.0, scores, floor)
            raised = jnp.exp(scores - jnp.max(scores, axis=-1, keepdims=True))
            probs = (raised * (1.0 / jnp.sum(raised, axis=-1, keepdims=True))).astype(qkv.dtype)
            act[:, h * hd:(h + 1) * hd] = jnp.dot(probs, qkv[2 * heads + h], preferred_element_type=jnp.float32).astype(act.dtype)

    def mlp_up():
        def tile(n, carry):
            u = jnp.dot(hm[...], wup[:, cols(n)], preferred_element_type=jnp.float32)
            g = 0.5 * u * (1.0 + lax.erf(u * (0.5 ** 0.5)))
            act[:, pl.ds(pl.multiple_of(qd + n * NT, NT), NT)] = g.astype(act.dtype)
            return carry
        lax.fori_loop(0, ff // NT, tile, 0, unroll=2)

    def project_out(c):
        def tile(n, carry):
            o = jnp.dot(act[...], wod[:, cols(n)], preferred_element_type=jnp.float32).astype(part.dtype)
            for b in range(tp):
                part[c % NP, b, :, cols(n)] = o[b * rb:(b + 1) * rb]
            return carry
        lax.fori_loop(0, d_model // NT, tile, 0, unroll=2)

    def holds(c):
        return (c >= 0) & (c < nc)

    def weights_ready(c, ks):
        @pl.when((c == 0) | (c == nc))
        def _():
            for k in ks:
                weight_copies[k].wait()

    def swap_weights(c, ks):
        @pl.when(front & (c == nc - 1))
        def _():
            for k in ks:
                lend_copies[k].wait_recv()
                swap_copies[k].start()

    def heads_step(c, lo):
        @pl.when(c == nc)
        def _():
            for k in range(3):
                swap_copies[k].wait()
        weights_ready(c, (3,))
        norms(c)
        projections()
        swap_weights(c, (0, 1, 2, 3))
        attention()

    def up_step(c, lo):
        weights_ready(c, (4,))
        mlp_up()
        swap_weights(c, (4,))

    def out_step(c, lo):
        weights_ready(c, (5, 6))
        ag_drain(c)
        on(c - NP >= lo, lambda: rs_drain(c - NP))
        project_out(c)
        swap_weights(c, (5, 6))

    steps = {
        "gather0": lambda c, lo: ag_start(c),
        "gather1": lambda c, lo: ag_hop(c, 1),
        "gather2": lambda c, lo: ag_hop(c, 2),
        "lay_q": lambda c, lo: on((s == 0) & (c == 0), lambda: lay(0)),
        "lay_k": lambda c, lo: on((s == 0) & (c == 0), lambda: lay(1)),
        "lay_v": lambda c, lo: on((s == 0) & (c == 0), lambda: lay(2)),
        "arrive": lambda c, lo: ag_hop(c, last),
        "heads": heads_step,
        "up": up_step,
        "out": out_step,
        "scatter0": lambda c, lo: rs_hop(c, 0),
        "scatter1": lambda c, lo: rs_hop(c, 1),
        "scatter2": lambda c, lo: rs_hop(c, 2),
        "finish": lambda c, lo: finish(c),
    }
    span = max(behind for _, behind in TURN)

    def segment(k, carry):
        lo = k * nc
        hi = jnp.where(front, jnp.where(k == 0, nc, nc + nl), jnp.where(k == 0, nc - nl, nc))

        def turn(i, carry):
            for name, behind in TURN:
                c = i - behind
                on((c >= lo) & (c < hi), functools.partial(steps[name], c, lo))
            return carry

        lax.fori_loop(lo, jnp.where(hi > lo, hi + span, lo), turn, 0)
        for back in range(1, NP + 1):
            on(hi - back >= lo, lambda: rs_drain(hi - back))
        return carry

    lax.fori_loop(0, 2, segment, 0)

    @pl.when(has_next)
    def _():
        def sent(v, carry):
            fwd_copy(v).wait_send()
            return carry
        lax.fori_loop(0, jnp.where(s < half - 1, nc, nc - nl), sent, 0)

    for k in range(nl):
        on(s == half - 1, turn_copy(nc - nl + k).wait_send)
        on(s < half - 1, next_late_copy(nc + k).wait_send)
        on(front, home_copy(nc + k).wait_send)

    @pl.when(helper)
    def _():
        def sent_early(c, carry):
            for h in range(last):
                for way in (0, 1):
                    on(ag_sends(h, way), share_copy(c, h, way).wait_send)
            for j in range(1, tp):
                hand_copy(c, lax.rem(z + j, tp)).wait_send()
            return carry
        lax.fori_loop(1, ne + 1, sent_early, 0)

    @pl.when(s >= half)
    def _():
        for copy in lend_copies:
            copy.wait_send()
        for k in range(nl):
            c = nc - nl + k
            pltpu.make_async_copy(x_hbm.at[0], xin.at[0], xin_sem.at[c]).wait()


def solution(mesh):
    tp, pp = mesh.shape["tp"], mesh.shape["pp"]

    def stage_body(x_in, ln_params, w_q, w_k, w_v, w_o, w_up, w_down):
        num_micro, batch_dim, tok, d_model = x_in.shape
        heads, hd = w_k.shape[2:]
        ff = w_up.shape[2]
        seqs = batch_dim // CHUNKS_PER_MICRO
        nc = num_micro * CHUNKS_PER_MICRO
        rb = seqs * tok
        rows = tp * rb
        qd = heads * hd
        bf16, f32 = jnp.bfloat16, jnp.float32

        cos_tab, sin_tab = rope_tables(tp * tok, hd)
        cos_full = jnp.concatenate([cos_tab, cos_tab], axis=-1)
        sin_full = jnp.concatenate([-sin_tab, sin_tab], axis=-1)

        any_spec = pl.BlockSpec(memory_space=pl.ANY)
        vmem_spec = pl.BlockSpec(memory_space=pltpu.VMEM)
        dma = pltpu.SemaphoreType.DMA
        flops = 2 * num_micro * tp * batch_dim * tok * (3 * qd * d_model + qd * d_model + 2 * ff * d_model)
        out, *_ = pl.pallas_call(
            functools.partial(pipeline_kernel, (nc, LATE, EARLY, tp, pp, heads, hd, tok)),
            out_shape=[pltpu.VMEM((nc, rb, d_model), bf16)] + [jax.ShapeDtypeStruct((d_model, qd), bf16)] * 3 + [
                jax.ShapeDtypeStruct((4, d_model), f32), jax.ShapeDtypeStruct((d_model, ff), bf16),
                jax.ShapeDtypeStruct((qd, d_model), bf16), jax.ShapeDtypeStruct((ff, d_model), bf16)],
            in_specs=[any_spec, vmem_spec, vmem_spec] + [any_spec] * 7,
            out_specs=[vmem_spec] + [any_spec] * 7,
            scratch_shapes=[
                pltpu.VMEM((3, d_model, heads, hd), bf16),
                pltpu.VMEM((d_model, 3 * qd), bf16),
                pltpu.VMEM((4, d_model), f32),
                pltpu.VMEM((d_model, ff), bf16),
                pltpu.VMEM((qd + ff, d_model), bf16),
                pltpu.VMEM((LATE, rb, d_model), bf16),
                pltpu.VMEM((EARLY, tp, rb, d_model), bf16),
                pltpu.VMEM((NX, tp, rb, d_model), bf16),
                pltpu.VMEM((NR, 2, tp - 1, rb, d_model), bf16),
                pltpu.VMEM((NP, tp, rb, d_model), bf16),
                pltpu.VMEM((rows, d_model), bf16),
                pltpu.VMEM((rows, d_model), bf16),
                pltpu.VMEM((3 * heads, rows, hd), bf16),
                pltpu.VMEM((rows, qd + ff), bf16),
                pltpu.VMEM((rows, rows), f32),
                pltpu.VMEM((rows, hd), f32),
                pltpu.VMEM((rows, hd), f32),
                dma((7,)),
                dma((nc + LATE,)),
                dma((NS, 2, tp - 1)),
                dma((NS, 2, tp - 1)),
                dma((NS, 2, tp - 1)),
                dma((NS, 2, tp - 1)),
                dma((nc + LATE,)),
                dma((LATE,)),
                dma((7,)),
                dma((7,)),
                dma((EARLY, 2, tp - 1)),
                dma((EARLY, 2, tp - 1)),
                dma((EARLY, tp)),
                dma((EARLY, tp)),
            ],
            compiler_params=pltpu.CompilerParams(collective_id=0, has_side_effects=True, vmem_limit_bytes=54 * 2 ** 20),
            cost_estimate=pl.CostEstimate(flops=flops, bytes_accessed=50 * 2 ** 20, transcendentals=0),
            name="pipeline",
        )(x_in.reshape(nc, rb, d_model), cos_full, sin_full, w_q.reshape(d_model, heads, hd), w_k[0], w_v[0], ln_params[0], w_up[0], w_o.reshape(qd, d_model), w_down[0])
        return out.reshape(1, num_micro, batch_dim, tok, d_model)

    in_specs = (P(None, "dp", "tp", None), P("pp", None, None), P("pp", None, "tp", None, None), P("pp", None, "tp", None), P("pp", None, "tp", None), P("pp", "tp", None, None, None), P("pp", None, "tp"), P("pp", "tp", None))
    return jax.shard_map(stage_body, mesh=mesh, in_specs=in_specs, out_specs=P("pp", None, "dp", "tp", None), check_vma=False)
```

```python
import functools

import jax
import jax.numpy as jnp
from jax import lax
from jax.experimental import pallas as pl
from jax.experimental.pallas import tpu as pltpu
from jax.sharding import PartitionSpec as P

LN_EPS = 1e-5
ROPE_BASE = 10000.0
CHUNKS_PER_MICRO = 8
NT = 256
NX, NR, NP, NS = 4, 4, 3, 4
LATE = 4
EARLY = 24
LEND_AT = 8
AHEAD = 4
TURN = (("gather0", 0), ("scatter1", 3), ("gather2", 1), ("up", 2), ("finish", 4), ("out", 2), ("scatter0", 2), ("lay_q", 0), ("gather1", 0), ("lay_k", 0), ("lay_v", 1), ("arrive", 1), ("scatter2", 3), ("heads", 1))
MESH = pl.DeviceIdType.MESH


def rope_tables(seq_len, head_dim):
    positions = jnp.arange(seq_len, dtype=jnp.float32)
    inv_freq = ROPE_BASE ** (-2.0 * jnp.arange(head_dim // 2, dtype=jnp.float32) / head_dim)
    angles = positions[:, None] * inv_freq[None, :]
    return jnp.cos(angles), jnp.sin(angles)


def pipeline_kernel(dims, x_hbm, cos_tab, sin_tab, wq_hbm, wk_hbm, wv_hbm, ln_hbm, wup_hbm, wo_hbm, wdn_hbm,
                    xin, lq_hbm, lk_hbm, lv_hbm, lln_hbm, lup_hbm, lo_hbm, ldn_hbm,
                    raw, wqkv, ln_ref, wup, wod, xlate, early, xfull, rbuf, part, ha, hm, qkv, act, mask_ref, cos_ref, sin_ref,
                    w_sem, xin_sem, ag_ss, ag_rs, rs_ss, rs_rs, fwd_sem, home_sem, lw_ss, lw_rs, es_ss, es_rs, eh_ss, eh_rs):
    nc, nl, ne, tp, pp, heads, hd, tok = dims
    rb, d_model = xin.shape[1:]
    rows = tp * rb
    ff = wup.shape[1]
    qd = heads * hd
    last = tp - 1
    z = lax.axis_index("tp")
    s = lax.axis_index("pp")
    has_left, has_right = z > 0, z < last
    has_prev, has_next = s > 0, s < pp - 1
    half = pp // 2
    front = s < half

    def on(cond, fn):
        pl.when(cond)(fn)

    def remote(src, dst, ss, rs, to):
        return pltpu.make_async_remote_copy(src_ref=src, dst_ref=dst, send_sem=ss, recv_sem=rs, device_id=to, device_id_type=MESH)

    def neighbour(way):
        return {"tp": jnp.minimum(z + 1, last) if way == 0 else jnp.maximum(z - 1, 0)}

    def ag_copy(c, h, way, first=None):
        b = jnp.clip(z - h if way == 0 else z + h, 0, last)
        src = (first if first is not None else xin.at[0]) if h == 0 else xfull.at[c % NX, b]
        return remote(src, xfull.at[c % NX, b], ag_ss.at[c % NS, way, h], ag_rs.at[c % NS, way, h], neighbour(way))

    def ag_sends(h, way):
        return has_right & (z >= h) if way == 0 else has_left & (z + h <= last)

    def ag_gets(h, way):
        return z - 1 - h >= 0 if way == 0 else z + 1 + h <= last

    def rs_copy(c, h, way):
        d = jnp.clip(z + last - h if way == 0 else z - last + h, 0, last)
        return remote(part.at[c % NP, d], rbuf.at[c % NR, way, h], rs_ss.at[c % NS, way, h], rs_rs.at[c % NS, way, h], neighbour(way))

    def rs_sends(h, way):
        return z <= h if way == 0 else last - z <= h

    def rs_sends_all(h, way):
        return rs_sends(h, way) & (has_right if way == 0 else has_left)

    def rs_gets(h, way):
        return has_left & (z - 1 <= h) if way == 0 else has_right & (last - 1 - z <= h)

    def fwd_copy(v):
        return remote(xin.at[v], xin.at[v], fwd_sem.at[v], xin_sem.at[v], {"pp": jnp.minimum(s + 1, pp - 1)})

    def turn_copy(v):
        return remote(xin.at[v], xlate.at[v - (nc - nl)], fwd_sem.at[v], xin_sem.at[v + nl], {"pp": 0})

    def next_late_copy(v):
        return remote(xlate.at[v - nc], xlate.at[v - nc], fwd_sem.at[v], xin_sem.at[v], {"pp": jnp.minimum(s + 1, pp - 1)})

    def home_copy(v):
        return remote(xlate.at[v - nc], xin.at[v - nl], home_sem.at[v - nc], xin_sem.at[v - nl], {"pp": jnp.minimum(s + half, pp - 1)})

    own = [wq_hbm, wk_hbm, wv_hbm, ln_hbm, wup_hbm, wo_hbm, wdn_hbm]
    late = [lq_hbm, lk_hbm, lv_hbm, lln_hbm, lup_hbm, lo_hbm, ldn_hbm]
    held = [wqkv.at[:, pl.ds(0, qd)], wqkv.at[:, pl.ds(qd, qd)], wqkv.at[:, pl.ds(2 * qd, qd)], ln_ref, wup, wod.at[pl.ds(0, qd)], wod.at[pl.ds(qd, ff)]]
    weight_copies = [pltpu.make_async_copy(src, dst, w_sem.at[k]) for k, (src, dst) in enumerate(zip(own, [raw.at[0], raw.at[1], raw.at[2]] + held[3:]))]
    swap_copies = [pltpu.make_async_copy(src, dst, w_sem.at[k]) for k, (src, dst) in enumerate(zip(late, held))]
    lend_copies = [remote(src, dst, lw_ss.at[k], lw_rs.at[k], {"pp": jnp.maximum(s - half, 0)}) for k, (src, dst) in enumerate(zip(held[:3] + own[3:], late))]

    helper = s == pp - 1

    def is_early(c):
        return (s == 0) & (c >= 1) & (c <= ne)

    def share_copy(c, h, way):
        b = jnp.clip(z - h if way == 0 else z + h, 0, last)
        src = x_hbm.at[c] if h == 0 else early.at[c - 1, b]
        return remote(src, early.at[c - 1, b], es_ss.at[c - 1, way, h], es_rs.at[c - 1, way, h], neighbour(way))

    def hand_copy(c, b):
        return remote(early.at[c - 1, b], early.at[c - 1, b], eh_ss.at[c - 1, b], eh_rs.at[c - 1, b], {"pp": 0})

    def share_hop(c, h):
        for way in (0, 1):
            if h > 0:
                @pl.when(ag_gets(h - 1, way))
                def _(way=way):
                    share_copy(c, h - 1, way).wait_recv()
                    if h < last:
                        on(ag_sends(h, way), share_copy(c, h, way).start)
                    hand_copy(c, z - h if way == 0 else z + h).start()
            else:
                on(ag_sends(0, way), share_copy(c, 0, way).start)

    barrier = pltpu.get_barrier_semaphore()
    for j in range(1, tp):
        pl.semaphore_signal(barrier, inc=1, device_id={"tp": lax.rem(z + j, tp)}, device_id_type=MESH)
    for j in range(1, pp):
        pl.semaphore_signal(barrier, inc=1, device_id={"pp": lax.rem(s + j, pp)}, device_id_type=MESH)

    def load(c):
        return pltpu.make_async_copy(x_hbm.at[c], xin.at[c], xin_sem.at[c])

    for c in range(AHEAD):
        on(s == 0, load(c).start)
    for copy in weight_copies:
        copy.start()

    lay_rows = 64

    def lay(k):
        weight_copies[k].wait()

        def some(t, carry):
            at = pl.ds(pl.multiple_of(t * lay_rows, lay_rows), lay_rows)
            wqkv[at, k * qd:(k + 1) * qd] = raw[k, at].reshape(lay_rows, qd)
            return carry
        lax.fori_loop(0, d_model // lay_rows, some, 0)

    @pl.when(s > 0)
    def _():
        for k in range(3):
            lay(k)

    for way, alone in ((0, z == 0), (1, z == last)):
        @pl.when(alone)
        def _(way=way):
            for k in range(NR):
                rbuf[k, way, last - 1] = jnp.zeros(rbuf.shape[3:], rbuf.dtype)

    row = lax.broadcasted_iota(jnp.int32, (rows, rows), 0)
    col = lax.broadcasted_iota(jnp.int32, (rows, rows), 1)
    same = row % rb // tok == col % rb // tok
    later = row // rb * tok + row % tok >= col // rb * tok + col % tok
    mask_ref[...] = jnp.where(same, jnp.where(later, 0.0, -1e30), -3e38)
    for b in range(tp):
        for q in range(rb // tok):
            to, of = slice(b * rb + q * tok, b * rb + (q + 1) * tok), slice(b * tok, (b + 1) * tok)
            cos_ref[to] = cos_tab[of]
            sin_ref[to] = sin_tab[of]

    pl.semaphore_wait(barrier, tp - 1 + pp - 1)

    def lend():
        for copy in lend_copies:
            copy.start()

    @pl.when(helper)
    def _():
        def share(i, carry):
            for h in range(tp):
                on((i - h >= 1) & (i - h <= ne), functools.partial(share_hop, i - h, h))
            return carry
        lax.fori_loop(1, ne + tp, share, 0)

    def in_its_place(c, fn):
        on(c < nc, lambda: fn(xin.at[c]))
        on(c >= nc, lambda: fn(xlate.at[c - nc]))

    def ag_start(c):
        on((s == 0) & (c + AHEAD < nc), lambda: load(c + AHEAD).start())
        pltpu.make_async_copy(x_hbm.at[0], xin.at[0], xin_sem.at[c]).wait()
        on((s >= half) & (c == LEND_AT), lend)

        def send(place):
            for way in (0, 1):
                on(ag_sends(0, way) & ~is_early(c), ag_copy(c, 0, way, place).start)
            xfull[c % NX, z] = place[...]
        in_its_place(c, send)

    def ag_hop(c, h):
        @pl.when(~is_early(c))
        def _():
            for way in (0, 1):
                on(ag_gets(h - 1, way), ag_copy(c, h - 1, way).wait_recv)
                if h < last:
                    on(ag_sends(h, way), ag_copy(c, h, way).start)

        if h == last:
            @pl.when(is_early(c))
            def _():
                for j in range(1, tp):
                    b = lax.rem(z + j, tp)
                    hand_copy(c, b).wait_recv()
                    xfull[c % NX, b] = early[c - 1, b]

    def ag_drain(c):
        @pl.when(~is_early(c))
        def _():
            for h in range(last):
                for way in (0, 1):
                    on(ag_sends(h, way), ag_copy(c, h, way).wait_send)

    def rs_hop(c, h):
        for way in (0, 1):
            @pl.when(rs_sends_all(h, way))
            def _(way=way):
                if h > 0:
                    @pl.when(rs_gets(h - 1, way))
                    def _():
                        rs_copy(c, h - 1, way).wait_recv()
                        d = z + last - h if way == 0 else z - last + h
                        mine = part[c % NP, d].astype(jnp.float32)
                        part[c % NP, d] = (mine + rbuf[c % NR, way, h - 1].astype(jnp.float32)).astype(part.dtype)
                rs_copy(c, h, way).start()

    def rs_drain(c):
        for h in range(last):
            for way in (0, 1):
                on(rs_sends_all(h, way), rs_copy(c, h, way).wait_send)

    def finish(c):
        for way in (0, 1):
            on(rs_gets(last - 1, way), rs_copy(c, last - 1, way).wait_recv)
        f32 = jnp.float32

        def add(place):
            total = place[...].astype(f32) + part[c % NP, z].astype(f32)
            total = total + rbuf[c % NR, 0, last - 1].astype(f32) + rbuf[c % NR, 1, last - 1].astype(f32)
            place[...] = total.astype(xin.dtype)
        in_its_place(c, add)
        turns = (s == half - 1) & (c >= nc - nl)
        on(has_next & (c < nc) & ~turns, lambda: fwd_copy(c).start())
        on(turns & (c < nc), lambda: turn_copy(c).start())
        on((s < half - 1) & (c >= nc), lambda: next_late_copy(c).start())
        on(front & (c >= nc), lambda: home_copy(c).start())

    lt = min(rb, 32)
    per_block = rb // lt

    def norms(c):
        def tile(t, carry):
            x_f32 = xfull[c % NX, t // per_block, pl.ds((t % per_block) * lt, lt)].astype(jnp.float32)
            row_mean = jnp.mean(x_f32, axis=-1, keepdims=True)
            centred = x_f32 - row_mean
            variance = jnp.mean(centred * centred, axis=-1, keepdims=True)
            unit = centred * lax.rsqrt(variance + LN_EPS)
            at = pl.ds(pl.multiple_of(t * lt, lt), lt)
            ha[at] = (unit * ln_ref[0:1] + ln_ref[1:2]).astype(ha.dtype)
            hm[at] = (unit * ln_ref[2:3] + ln_ref[3:4]).astype(hm.dtype)
            return carry
        lax.fori_loop(0, rows // lt, tile, 0, unroll=2)

    def cols(n):
        return pl.ds(pl.multiple_of(n * NT, NT), NT)

    per_tile = NT // hd

    def projections():
        def rotated(n, carry):
            y = jnp.dot(ha[...], wqkv[:, cols(n)], preferred_element_type=jnp.float32)
            for j in range(per_tile):
                head = y[:, j * hd:(j + 1) * hd]
                turned = head * cos_ref[...] + pltpu.roll(head, hd // 2, 1) * sin_ref[...]
                qkv[n * per_tile + j] = turned.astype(qkv.dtype)
            return carry
        lax.fori_loop(0, 2 * qd // NT, rotated, 0, unroll=2)

        def plain(n, carry):
            y = jnp.dot(ha[...], wqkv[:, cols(n)], preferred_element_type=jnp.float32)
            for j in range(per_tile):
                qkv[n * per_tile + j] = y[:, j * hd:(j + 1) * hd].astype(qkv.dtype)
            return carry
        lax.fori_loop(2 * qd // NT, 3 * qd // NT, plain, 0, unroll=True)

    def attention():
        for h in range(heads):
            scores = lax.dot_general(qkv[h], qkv[heads + h], (((1,), (1,)), ((), ())), preferred_element_type=jnp.float32) * (hd ** -0.5)
            floor = mask_ref[...]
            scores = jnp.where(floor == 0.0, scores, floor)
            raised = jnp.exp(scores - jnp.max(scores, axis=-1, keepdims=True))
            probs = (raised * (1.0 / jnp.sum(raised, axis=-1, keepdims=True))).astype(qkv.dtype)
            act[:, h * hd:(h + 1) * hd] = jnp.dot(probs, qkv[2 * heads + h], preferred_element_type=jnp.float32).astype(act.dtype)

    def mlp_up():
        def tile(n, carry):
            u = jnp.dot(hm[...], wup[:, cols(n)], preferred_element_type=jnp.float32)
            g = 0.5 * u * (1.0 + lax.erf(u * (0.5 ** 0.5)))
            act[:, pl.ds(pl.multiple_of(qd + n * NT, NT), NT)] = g.astype(act.dtype)
            return carry
        lax.fori_loop(0, ff // NT, tile, 0, unroll=2)

    def project_out(c):
        def tile(n, carry):
            o = jnp.dot(act[...], wod[:, cols(n)], preferred_element_type=jnp.float32).astype(part.dtype)
            for b in range(tp):
                part[c % NP, b, :, cols(n)] = o[b * rb:(b + 1) * rb]
            return carry
        lax.fori_loop(0, d_model // NT, tile, 0, unroll=2)

    def holds(c):
        return (c >= 0) & (c < nc)

    def weights_ready(c, ks):
        @pl.when((c == 0) | (c == nc))
        def _():
            for k in ks:
                weight_copies[k].wait()

    def swap_weights(c, ks):
        @pl.when(front & (c == nc - 1))
        def _():
            for k in ks:
                lend_copies[k].wait_recv()
                swap_copies[k].start()

    def heads_step(c, lo):
        @pl.when(c == nc)
        def _():
            for k in range(3):
                swap_copies[k].wait()
        weights_ready(c, (3,))
        norms(c)
        projections()
        swap_weights(c, (0, 1, 2, 3))
        attention()

    def up_step(c, lo):
        weights_ready(c, (4,))
        mlp_up()
        swap_weights(c, (4,))

    def out_step(c, lo):
        weights_ready(c, (5, 6))
        ag_drain(c)
        on(c - NP >= lo, lambda: rs_drain(c - NP))
        project_out(c)
        swap_weights(c, (5, 6))

    steps = {
        "gather0": lambda c, lo: ag_start(c),
        "gather1": lambda c, lo: ag_hop(c, 1),
        "gather2": lambda c, lo: ag_hop(c, 2),
        "lay_q": lambda c, lo: on((s == 0) & (c == 0), lambda: lay(0)),
        "lay_k": lambda c, lo: on((s == 0) & (c == 0), lambda: lay(1)),
        "lay_v": lambda c, lo: on((s == 0) & (c == 0), lambda: lay(2)),
        "arrive": lambda c, lo: ag_hop(c, last),
        "heads": heads_step,
        "up": up_step,
        "out": out_step,
        "scatter0": lambda c, lo: rs_hop(c, 0),
        "scatter1": lambda c, lo: rs_hop(c, 1),
        "scatter2": lambda c, lo: rs_hop(c, 2),
        "finish": lambda c, lo: finish(c),
    }
    span = max(behind for _, behind in TURN)

    def segment(k, carry):
        lo = k * nc
        hi = jnp.where(front, jnp.where(k == 0, nc, nc + nl), jnp.where(k == 0, nc - nl, nc))

        def turn(i, carry):
            for name, behind in TURN:
                c = i - behind
                on((c >= lo) & (c < hi), functools.partial(steps[name], c, lo))
            return carry

        lax.fori_loop(lo, jnp.where(hi > lo, hi + span, lo), turn, 0)
        for back in range(1, NP + 1):
            on(hi - back >= lo, lambda: rs_drain(hi - back))
        return carry

    lax.fori_loop(0, 2, segment, 0)

    @pl.when(has_next)
    def _():
        def sent(v, carry):
            fwd_copy(v).wait_send()
            return carry
        lax.fori_loop(0, jnp.where(s < half - 1, nc, nc - nl), sent, 0)

    for k in range(nl):
        on(s == half - 1, turn_copy(nc - nl + k).wait_send)
        on(s < half - 1, next_late_copy(nc + k).wait_send)
        on(front, home_copy(nc + k).wait_send)

    @pl.when(helper)
    def _():
        def sent_early(c, carry):
            for h in range(last):
                for way in (0, 1):
                    on(ag_sends(h, way), share_copy(c, h, way).wait_send)
            for j in range(1, tp):
                hand_copy(c, lax.rem(z + j, tp)).wait_send()
            return carry
        lax.fori_loop(1, ne + 1, sent_early, 0)

    @pl.when(s >= half)
    def _():
        for copy in lend_copies:
            copy.wait_send()
        for k in range(nl):
            c = nc - nl + k
            pltpu.make_async_copy(x_hbm.at[0], xin.at[0], xin_sem.at[c]).wait()


def solution(mesh):
    tp, pp = mesh.shape["tp"], mesh.shape["pp"]

    def stage_body(x_in, ln_params, w_q, w_k, w_v, w_o, w_up, w_down):
        num_micro, batch_dim, tok, d_model = x_in.shape
        heads, hd = w_k.shape[2:]
        ff = w_up.shape[2]
        seqs = batch_dim // CHUNKS_PER_MICRO
        nc = num_micro * CHUNKS_PER_MICRO
        rb = seqs * tok
        rows = tp * rb
        qd = heads * hd
        bf16, f32 = jnp.bfloat16, jnp.float32

        cos_tab, sin_tab = rope_tables(tp * tok, hd)
        cos_full = jnp.concatenate([cos_tab, cos_tab], axis=-1)
        sin_full = jnp.concatenate([-sin_tab, sin_tab], axis=-1)

        any_spec = pl.BlockSpec(memory_space=pl.ANY)
        vmem_spec = pl.BlockSpec(memory_space=pltpu.VMEM)
        dma = pltpu.SemaphoreType.DMA
        flops = 2 * num_micro * tp * batch_dim * tok * (3 * qd * d_model + qd * d_model + 2 * ff * d_model)
        out, *_ = pl.pallas_call(
            functools.partial(pipeline_kernel, (nc, LATE, EARLY, tp, pp, heads, hd, tok)),
            out_shape=[pltpu.VMEM((nc, rb, d_model), bf16)] + [jax.ShapeDtypeStruct((d_model, qd), bf16)] * 3 + [
                jax.ShapeDtypeStruct((4, d_model), f32), jax.ShapeDtypeStruct((d_model, ff), bf16),
                jax.ShapeDtypeStruct((qd, d_model), bf16), jax.ShapeDtypeStruct((ff, d_model), bf16)],
            in_specs=[any_spec, vmem_spec, vmem_spec] + [any_spec] * 7,
            out_specs=[vmem_spec] + [any_spec] * 7,
            scratch_shapes=[
                pltpu.VMEM((3, d_model, heads, hd), bf16),
                pltpu.VMEM((d_model, 3 * qd), bf16),
                pltpu.VMEM((4, d_model), f32),
                pltpu.VMEM((d_model, ff), bf16),
                pltpu.VMEM((qd + ff, d_model), bf16),
                pltpu.VMEM((LATE, rb, d_model), bf16),
                pltpu.VMEM((EARLY, tp, rb, d_model), bf16),
                pltpu.VMEM((NX, tp, rb, d_model), bf16),
                pltpu.VMEM((NR, 2, tp - 1, rb, d_model), bf16),
                pltpu.VMEM((NP, tp, rb, d_model), bf16),
                pltpu.VMEM((rows, d_model), bf16),
                pltpu.VMEM((rows, d_model), bf16),
                pltpu.VMEM((3 * heads, rows, hd), bf16),
                pltpu.VMEM((rows, qd + ff), bf16),
                pltpu.VMEM((rows, rows), f32),
                pltpu.VMEM((rows, hd), f32),
                pltpu.VMEM((rows, hd), f32),
                dma((7,)),
                dma((nc + LATE,)),
                dma((NS, 2, tp - 1)),
                dma((NS, 2, tp - 1)),
                dma((NS, 2, tp - 1)),
                dma((NS, 2, tp - 1)),
                dma((nc + LATE,)),
                dma((LATE,)),
                dma((7,)),
                dma((7,)),
                dma((EARLY, 2, tp - 1)),
                dma((EARLY, 2, tp - 1)),
                dma((EARLY, tp)),
                dma((EARLY, tp)),
            ],
            compiler_params=pltpu.CompilerParams(collective_id=0, has_side_effects=True, vmem_limit_bytes=54 * 2 ** 20),
            cost_estimate=pl.CostEstimate(flops=flops, bytes_accessed=50 * 2 ** 20, transcendentals=0),
            name="pipeline",
        )(x_in.reshape(nc, rb, d_model), cos_full, sin_full, w_q.reshape(d_model, heads, hd), w_k[0], w_v[0], ln_params[0], w_up[0], w_o.reshape(qd, d_model), w_down[0])
        return out.reshape(1, num_micro, batch_dim, tok, d_model)

    in_specs = (P(None, "dp", "tp", None), P("pp", None, None), P("pp", None, "tp", None, None), P("pp", None, "tp", None), P("pp", None, "tp", None), P("pp", "tp", None, None, None), P("pp", None, "tp"), P("pp", "tp", None))
    return jax.shard_map(stage_body, mesh=mesh, in_specs=in_specs, out_specs=P("pp", None, "dp", "tp", None), check_vma=False)
```

```python
import functools

import jax
import jax.numpy as jnp
from jax import lax
from jax.experimental import pallas as pl
from jax.experimental.pallas import tpu as pltpu
from jax.sharding import PartitionSpec as P

LN_EPS = 1e-5
ROPE_BASE = 10000.0
CHUNKS_PER_MICRO = 8
NT = 256
NX, NR, NP, NS = 4, 4, 3, 4
LATE = 5
EARLY = 24
LEND_AT = (5, 12)
AHEAD = 4
TURN = (("gather0", 0), ("arrive", 2), ("scatter2", 4), ("heads", 2), ("gather2", 1), ("lay_v", 1), ("scatter1", 3), ("up", 2), ("lay_q", 0), ("gather1", 0), ("lay_k", 0), ("out", 2), ("scatter0", 2), ("finish", 4))
MESH = pl.DeviceIdType.MESH


def rope_tables(seq_len, head_dim):
    positions = jnp.arange(seq_len, dtype=jnp.float32)
    inv_freq = ROPE_BASE ** (-2.0 * jnp.arange(head_dim // 2, dtype=jnp.float32) / head_dim)
    angles = positions[:, None] * inv_freq[None, :]
    return jnp.cos(angles), jnp.sin(angles)


def pipeline_kernel(dims, x_hbm, cos_tab, sin_tab, wq_hbm, wk_hbm, wv_hbm, ln_hbm, wup_hbm, wo_hbm, wdn_hbm,
                    xin, lq_hbm, lk_hbm, lv_hbm, lln_hbm, lup_hbm, lo_hbm, ldn_hbm,
                    raw, wqkv, ln_ref, wup, wod, xlate, early, xfull, rbuf, part, ha, hm, qkv, act, mask_ref, cos_ref, sin_ref,
                    w_sem, xin_sem, ag_ss, ag_rs, rs_ss, rs_rs, fwd_sem, home_sem, lw_ss, lw_rs, es_ss, es_rs, eh_ss, eh_rs):
    nc, nl, ne, tp, pp, heads, hd, tok = dims
    rb, d_model = xin.shape[1:]
    rows = tp * rb
    ff = wup.shape[1]
    qd = heads * hd
    last = tp - 1
    z = lax.axis_index("tp")
    s = lax.axis_index("pp")
    has_left, has_right = z > 0, z < last
    has_prev, has_next = s > 0, s < pp - 1
    half = pp // 2
    front = s < half

    def on(cond, fn):
        pl.when(cond)(fn)

    def remote(src, dst, ss, rs, to):
        return pltpu.make_async_remote_copy(src_ref=src, dst_ref=dst, send_sem=ss, recv_sem=rs, device_id=to, device_id_type=MESH)

    def neighbour(way):
        return {"tp": jnp.minimum(z + 1, last) if way == 0 else jnp.maximum(z - 1, 0)}

    def ag_copy(c, h, way, first=None):
        b = jnp.clip(z - h if way == 0 else z + h, 0, last)
        src = (first if first is not None else xin.at[0]) if h == 0 else xfull.at[c % NX, b]
        return remote(src, xfull.at[c % NX, b], ag_ss.at[c % NS, way, h], ag_rs.at[c % NS, way, h], neighbour(way))

    def ag_sends(h, way):
        return has_right & (z >= h) if way == 0 else has_left & (z + h <= last)

    def ag_gets(h, way):
        return z - 1 - h >= 0 if way == 0 else z + 1 + h <= last

    def rs_copy(c, h, way):
        d = jnp.clip(z + last - h if way == 0 else z - last + h, 0, last)
        return remote(part.at[c % NP, d], rbuf.at[c % NR, way, h], rs_ss.at[c % NS, way, h], rs_rs.at[c % NS, way, h], neighbour(way))

    def rs_sends(h, way):
        return z <= h if way == 0 else last - z <= h

    def rs_sends_all(h, way):
        return rs_sends(h, way) & (has_right if way == 0 else has_left)

    def rs_gets(h, way):
        return has_left & (z - 1 <= h) if way == 0 else has_right & (last - 1 - z <= h)

    def fwd_copy(v):
        return remote(xin.at[v], xin.at[v], fwd_sem.at[v], xin_sem.at[v], {"pp": jnp.minimum(s + 1, pp - 1)})

    def turn_copy(v):
        return remote(xin.at[v], xlate.at[v - (nc - nl)], fwd_sem.at[v], xin_sem.at[v + nl], {"pp": 0})

    def next_late_copy(v):
        return remote(xlate.at[v - nc], xlate.at[v - nc], fwd_sem.at[v], xin_sem.at[v], {"pp": jnp.minimum(s + 1, pp - 1)})

    def home_copy(v):
        return remote(xlate.at[v - nc], xin.at[v - nl], home_sem.at[v - nc], xin_sem.at[v - nl], {"pp": jnp.minimum(s + half, pp - 1)})

    own = [wq_hbm, wk_hbm, wv_hbm, ln_hbm, wup_hbm, wo_hbm, wdn_hbm]
    late = [lq_hbm, lk_hbm, lv_hbm, lln_hbm, lup_hbm, lo_hbm, ldn_hbm]
    held = [wqkv.at[:, pl.ds(0, qd)], wqkv.at[:, pl.ds(qd, qd)], wqkv.at[:, pl.ds(2 * qd, qd)], ln_ref, wup, wod.at[pl.ds(0, qd)], wod.at[pl.ds(qd, ff)]]
    weight_copies = [pltpu.make_async_copy(src, dst, w_sem.at[k]) for k, (src, dst) in enumerate(zip(own, [raw.at[0], raw.at[1], raw.at[2]] + held[3:]))]
    swap_copies = [pltpu.make_async_copy(src, dst, w_sem.at[k]) for k, (src, dst) in enumerate(zip(late, held))]
    lend_copies = [remote(src, dst, lw_ss.at[k], lw_rs.at[k], {"pp": jnp.maximum(s - half, 0)}) for k, (src, dst) in enumerate(zip(held[:3] + own[3:], late))]

    helper = s == pp - 1

    def is_early(c):
        return (s == 0) & (c >= 1) & (c <= ne)

    def share_copy(c, h, way):
        b = jnp.clip(z - h if way == 0 else z + h, 0, last)
        src = x_hbm.at[c] if h == 0 else early.at[c - 1, b]
        return remote(src, early.at[c - 1, b], es_ss.at[c - 1, way, h], es_rs.at[c - 1, way, h], neighbour(way))

    def hand_copy(c, b):
        return remote(early.at[c - 1, b], early.at[c - 1, b], eh_ss.at[c - 1, b], eh_rs.at[c - 1, b], {"pp": 0})

    def share_hop(c, h):
        for way in (0, 1):
            if h > 0:
                @pl.when(ag_gets(h - 1, way))
                def _(way=way):
                    share_copy(c, h - 1, way).wait_recv()
                    if h < last:
                        on(ag_sends(h, way), share_copy(c, h, way).start)
                    hand_copy(c, z - h if way == 0 else z + h).start()
            else:
                on(ag_sends(0, way), share_copy(c, 0, way).start)

    barrier = pltpu.get_barrier_semaphore()
    for j in range(1, tp):
        pl.semaphore_signal(barrier, inc=1, device_id={"tp": lax.rem(z + j, tp)}, device_id_type=MESH)
    for j in range(1, pp):
        pl.semaphore_signal(barrier, inc=1, device_id={"pp": lax.rem(s + j, pp)}, device_id_type=MESH)

    def load(c):
        return pltpu.make_async_copy(x_hbm.at[c], xin.at[c], xin_sem.at[c])

    for c in range(AHEAD):
        on(s == 0, load(c).start)
    for copy in weight_copies:
        copy.start()

    lay_rows = 64

    def lay(k):
        weight_copies[k].wait()

        def some(t, carry):
            at = pl.ds(pl.multiple_of(t * lay_rows, lay_rows), lay_rows)
            wqkv[at, k * qd:(k + 1) * qd] = raw[k, at].reshape(lay_rows, qd)
            return carry
        lax.fori_loop(0, d_model // lay_rows, some, 0)

    @pl.when(s > 0)
    def _():
        for k in range(3):
            lay(k)

    for way, alone in ((0, z == 0), (1, z == last)):
        @pl.when(alone)
        def _(way=way):
            for k in range(NR):
                rbuf[k, way, last - 1] = jnp.zeros(rbuf.shape[3:], rbuf.dtype)

    row = lax.broadcasted_iota(jnp.int32, (rows, rows), 0)
    col = lax.broadcasted_iota(jnp.int32, (rows, rows), 1)
    same = row % rb // tok == col % rb // tok
    later = row // rb * tok + row % tok >= col // rb * tok + col % tok
    mask_ref[...] = jnp.where(same, jnp.where(later, 0.0, -1e30), -3e38)
    for b in range(tp):
        for q in range(rb // tok):
            to, of = slice(b * rb + q * tok, b * rb + (q + 1) * tok), slice(b * tok, (b + 1) * tok)
            cos_ref[to] = cos_tab[of]
            sin_ref[to] = sin_tab[of]

    pl.semaphore_wait(barrier, tp - 1 + pp - 1)

    def lend():
        for copy in lend_copies:
            copy.start()

    @pl.when(helper)
    def _():
        def share(i, carry):
            for h in range(tp):
                on((i - h >= 1) & (i - h <= ne), functools.partial(share_hop, i - h, h))
            return carry
        lax.fori_loop(1, ne + tp, share, 0)

    def in_its_place(c, fn):
        on(c < nc, lambda: fn(xin.at[c]))
        on(c >= nc, lambda: fn(xlate.at[c - nc]))

    def ag_start(c):
        on((s == 0) & (c + AHEAD < nc), lambda: load(c + AHEAD).start())
        pltpu.make_async_copy(x_hbm.at[0], xin.at[0], xin_sem.at[c]).wait()
        for k in range(half):
            on((s == half + k) & (c == LEND_AT[k]), lend)

        def send(place):
            for way in (0, 1):
                on(ag_sends(0, way) & ~is_early(c), ag_copy(c, 0, way, place).start)
            xfull[c % NX, z] = place[...]
        in_its_place(c, send)

    def ag_hop(c, h):
        @pl.when(~is_early(c))
        def _():
            for way in (0, 1):
                on(ag_gets(h - 1, way), ag_copy(c, h - 1, way).wait_recv)
                if h < last:
                    on(ag_sends(h, way), ag_copy(c, h, way).start)

        if h == last:
            @pl.when(is_early(c))
            def _():
                for j in range(1, tp):
                    b = lax.rem(z + j, tp)
                    hand_copy(c, b).wait_recv()
                    xfull[c % NX, b] = early[c - 1, b]

    def ag_drain(c):
        @pl.when(~is_early(c))
        def _():
            for h in range(last):
                for way in (0, 1):
                    on(ag_sends(h, way), ag_copy(c, h, way).wait_send)

    def rs_hop(c, h):
        for way in (0, 1):
            @pl.when(rs_sends_all(h, way))
            def _(way=way):
                if h > 0:
                    @pl.when(rs_gets(h - 1, way))
                    def _():
                        rs_copy(c, h - 1, way).wait_recv()
                        d = z + last - h if way == 0 else z - last + h
                        mine = part[c % NP, d].astype(jnp.float32)
                        part[c % NP, d] = (mine + rbuf[c % NR, way, h - 1].astype(jnp.float32)).astype(part.dtype)
                rs_copy(c, h, way).start()

    def rs_drain(c):
        for h in range(last):
            for way in (0, 1):
                on(rs_sends_all(h, way), rs_copy(c, h, way).wait_send)

    def finish(c):
        for way in (0, 1):
            on(rs_gets(last - 1, way), rs_copy(c, last - 1, way).wait_recv)
        f32 = jnp.float32

        def add(place):
            total = place[...].astype(f32) + part[c % NP, z].astype(f32)
            total = total + rbuf[c % NR, 0, last - 1].astype(f32) + rbuf[c % NR, 1, last - 1].astype(f32)
            place[...] = total.astype(xin.dtype)
        in_its_place(c, add)
        turns = (s == half - 1) & (c >= nc - nl)
        on(has_next & (c < nc) & ~turns, lambda: fwd_copy(c).start())
        on(turns & (c < nc), lambda: turn_copy(c).start())
        on((s < half - 1) & (c >= nc), lambda: next_late_copy(c).start())
        on(front & (c >= nc), lambda: home_copy(c).start())

    lt = min(rb, 32)
    per_block = rb // lt

    def norms(c):
        def tile(t, carry):
            x_f32 = xfull[c % NX, t // per_block, pl.ds((t % per_block) * lt, lt)].astype(jnp.float32)
            row_mean = jnp.mean(x_f32, axis=-1, keepdims=True)
            centred = x_f32 - row_mean
            variance = jnp.mean(centred * centred, axis=-1, keepdims=True)
            unit = centred * lax.rsqrt(variance + LN_EPS)
            at = pl.ds(pl.multiple_of(t * lt, lt), lt)
            ha[at] = (unit * ln_ref[0:1] + ln_ref[1:2]).astype(ha.dtype)
            hm[at] = (unit * ln_ref[2:3] + ln_ref[3:4]).astype(hm.dtype)
            return carry
        lax.fori_loop(0, rows // lt, tile, 0, unroll=2)

    def cols(n):
        return pl.ds(pl.multiple_of(n * NT, NT), NT)

    per_tile = NT // hd

    def projections():
        def rotated(n, carry):
            y = jnp.dot(ha[...], wqkv[:, cols(n)], preferred_element_type=jnp.float32)
            for j in range(per_tile):
                head = y[:, j * hd:(j + 1) * hd]
                turned = head * cos_ref[...] + pltpu.roll(head, hd // 2, 1) * sin_ref[...]
                qkv[n * per_tile + j] = turned.astype(qkv.dtype)
            return carry
        lax.fori_loop(0, 2 * qd // NT, rotated, 0, unroll=2)

        def plain(n, carry):
            y = jnp.dot(ha[...], wqkv[:, cols(n)], preferred_element_type=jnp.float32)
            for j in range(per_tile):
                qkv[n * per_tile + j] = y[:, j * hd:(j + 1) * hd].astype(qkv.dtype)
            return carry
        lax.fori_loop(2 * qd // NT, 3 * qd // NT, plain, 0, unroll=True)

    def attention():
        for h in range(heads):
            scores = lax.dot_general(qkv[h], qkv[heads + h], (((1,), (1,)), ((), ())), preferred_element_type=jnp.float32) * (hd ** -0.5)
            floor = mask_ref[...]
            scores = jnp.where(floor == 0.0, scores, floor)
            raised = jnp.exp(scores - jnp.max(scores, axis=-1, keepdims=True))
            probs = (raised * (1.0 / jnp.sum(raised, axis=-1, keepdims=True))).astype(qkv.dtype)
            act[:, h * hd:(h + 1) * hd] = jnp.dot(probs, qkv[2 * heads + h], preferred_element_type=jnp.float32).astype(act.dtype)

    def mlp_up():
        def tile(n, carry):
            u = jnp.dot(hm[...], wup[:, cols(n)], preferred_element_type=jnp.float32)
            g = 0.5 * u * (1.0 + lax.erf(u * (0.5 ** 0.5)))
            act[:, pl.ds(pl.multiple_of(qd + n * NT, NT), NT)] = g.astype(act.dtype)
            return carry
        lax.fori_loop(0, ff // NT, tile, 0, unroll=2)

    def project_out(c):
        def tile(n, carry):
            o = jnp.dot(act[...], wod[:, cols(n)], preferred_element_type=jnp.float32).astype(part.dtype)
            for b in range(tp):
                part[c % NP, b, :, cols(n)] = o[b * rb:(b + 1) * rb]
            return carry
        lax.fori_loop(0, d_model // NT, tile, 0, unroll=2)

    def holds(c):
        return (c >= 0) & (c < nc)

    def weights_ready(c, ks):
        @pl.when((c == 0) | (c == nc))
        def _():
            for k in ks:
                weight_copies[k].wait()

    def swap_weights(c, ks):
        @pl.when(front & (c == nc - 1))
        def _():
            for k in ks:
                lend_copies[k].wait_recv()
                swap_copies[k].start()

    def heads_step(c, lo):
        @pl.when(c == nc)
        def _():
            for k in range(3):
                swap_copies[k].wait()
        weights_ready(c, (3,))
        norms(c)
        projections()
        swap_weights(c, (0, 1, 2, 3))
        attention()

    def up_step(c, lo):
        weights_ready(c, (4,))
        mlp_up()
        swap_weights(c, (4,))

    def out_step(c, lo):
        weights_ready(c, (5, 6))
        ag_drain(c)
        on(c - NP >= lo, lambda: rs_drain(c - NP))
        project_out(c)
        swap_weights(c, (5, 6))

    steps = {
        "gather0": lambda c, lo: ag_start(c),
        "gather1": lambda c, lo: ag_hop(c, 1),
        "gather2": lambda c, lo: ag_hop(c, 2),
        "lay_q": lambda c, lo: on((s == 0) & (c == 0), lambda: lay(0)),
        "lay_k": lambda c, lo: on((s == 0) & (c == 0), lambda: lay(1)),
        "lay_v": lambda c, lo: on((s == 0) & (c == 0), lambda: lay(2)),
        "arrive": lambda c, lo: ag_hop(c, last),
        "heads": heads_step,
        "up": up_step,
        "out": out_step,
        "scatter0": lambda c, lo: rs_hop(c, 0),
        "scatter1": lambda c, lo: rs_hop(c, 1),
        "scatter2": lambda c, lo: rs_hop(c, 2),
        "finish": lambda c, lo: finish(c),
    }
    span = max(behind for _, behind in TURN)

    def segment(k, carry):
        lo = k * nc
        hi = jnp.where(front, jnp.where(k == 0, nc, nc + nl), jnp.where(k == 0, nc - nl, nc))

        def turn(i, carry):
            for name, behind in TURN:
                c = i - behind
                on((c >= lo) & (c < hi), functools.partial(steps[name], c, lo))
            return carry

        lax.fori_loop(lo, jnp.where(hi > lo, hi + span, lo), turn, 0)
        for back in range(1, NP + 1):
            on(hi - back >= lo, lambda: rs_drain(hi - back))
        return carry

    lax.fori_loop(0, 2, segment, 0)

    @pl.when(has_next)
    def _():
        def sent(v, carry):
            fwd_copy(v).wait_send()
            return carry
        lax.fori_loop(0, jnp.where(s < half - 1, nc, nc - nl), sent, 0)

    for k in range(nl):
        on(s == half - 1, turn_copy(nc - nl + k).wait_send)
        on(s < half - 1, next_late_copy(nc + k).wait_send)
        on(front, home_copy(nc + k).wait_send)

    @pl.when(helper)
    def _():
        def sent_early(c, carry):
            for h in range(last):
                for way in (0, 1):
                    on(ag_sends(h, way), share_copy(c, h, way).wait_send)
            for j in range(1, tp):
                hand_copy(c, lax.rem(z + j, tp)).wait_send()
            return carry
        lax.fori_loop(1, ne + 1, sent_early, 0)

    @pl.when(s >= half)
    def _():
        for copy in lend_copies:
            copy.wait_send()
        for k in range(nl):
            c = nc - nl + k
            pltpu.make_async_copy(x_hbm.at[0], xin.at[0], xin_sem.at[c]).wait()


def solution(mesh):
    tp, pp = mesh.shape["tp"], mesh.shape["pp"]

    def stage_body(x_in, ln_params, w_q, w_k, w_v, w_o, w_up, w_down):
        num_micro, batch_dim, tok, d_model = x_in.shape
        heads, hd = w_k.shape[2:]
        ff = w_up.shape[2]
        seqs = batch_dim // CHUNKS_PER_MICRO
        nc = num_micro * CHUNKS_PER_MICRO
        rb = seqs * tok
        rows = tp * rb
        qd = heads * hd
        bf16, f32 = jnp.bfloat16, jnp.float32

        cos_tab, sin_tab = rope_tables(tp * tok, hd)
        cos_full = jnp.concatenate([cos_tab, cos_tab], axis=-1)
        sin_full = jnp.concatenate([-sin_tab, sin_tab], axis=-1)

        any_spec = pl.BlockSpec(memory_space=pl.ANY)
        vmem_spec = pl.BlockSpec(memory_space=pltpu.VMEM)
        dma = pltpu.SemaphoreType.DMA
        flops = 2 * num_micro * tp * batch_dim * tok * (3 * qd * d_model + qd * d_model + 2 * ff * d_model)
        out, *_ = pl.pallas_call(
            functools.partial(pipeline_kernel, (nc, LATE, EARLY, tp, pp, heads, hd, tok)),
            out_shape=[pltpu.VMEM((nc, rb, d_model), bf16)] + [jax.ShapeDtypeStruct((d_model, qd), bf16)] * 3 + [
                jax.ShapeDtypeStruct((4, d_model), f32), jax.ShapeDtypeStruct((d_model, ff), bf16),
                jax.ShapeDtypeStruct((qd, d_model), bf16), jax.ShapeDtypeStruct((ff, d_model), bf16)],
            in_specs=[any_spec, vmem_spec, vmem_spec] + [any_spec] * 7,
            out_specs=[vmem_spec] + [any_spec] * 7,
            scratch_shapes=[
                pltpu.VMEM((3, d_model, heads, hd), bf16),
                pltpu.VMEM((d_model, 3 * qd), bf16),
                pltpu.VMEM((4, d_model), f32),
                pltpu.VMEM((d_model, ff), bf16),
                pltpu.VMEM((qd + ff, d_model), bf16),
                pltpu.VMEM((LATE, rb, d_model), bf16),
                pltpu.VMEM((EARLY, tp, rb, d_model), bf16),
                pltpu.VMEM((NX, tp, rb, d_model), bf16),
                pltpu.VMEM((NR, 2, tp - 1, rb, d_model), bf16),
                pltpu.VMEM((NP, tp, rb, d_model), bf16),
                pltpu.VMEM((rows, d_model), bf16),
                pltpu.VMEM((rows, d_model), bf16),
                pltpu.VMEM((3 * heads, rows, hd), bf16),
                pltpu.VMEM((rows, qd + ff), bf16),
                pltpu.VMEM((rows, rows), f32),
                pltpu.VMEM((rows, hd), f32),
                pltpu.VMEM((rows, hd), f32),
                dma((7,)),
                dma((nc + LATE,)),
                dma((NS, 2, tp - 1)),
                dma((NS, 2, tp - 1)),
                dma((NS, 2, tp - 1)),
                dma((NS, 2, tp - 1)),
                dma((nc + LATE,)),
                dma((LATE,)),
                dma((7,)),
                dma((7,)),
                dma((EARLY, 2, tp - 1)),
                dma((EARLY, 2, tp - 1)),
                dma((EARLY, tp)),
                dma((EARLY, tp)),
            ],
            compiler_params=pltpu.CompilerParams(collective_id=0, has_side_effects=True, vmem_limit_bytes=54 * 2 ** 20),
            cost_estimate=pl.CostEstimate(flops=flops, bytes_accessed=50 * 2 ** 20, transcendentals=0),
            name="pipeline",
        )(x_in.reshape(nc, rb, d_model), cos_full, sin_full, w_q.reshape(d_model, heads, hd), w_k[0], w_v[0], ln_params[0], w_up[0], w_o.reshape(qd, d_model), w_down[0])
        return out.reshape(1, num_micro, batch_dim, tok, d_model)

    in_specs = (P(None, "dp", "tp", None), P("pp", None, None), P("pp", None, "tp", None, None), P("pp", None, "tp", None), P("pp", None, "tp", None), P("pp", "tp", None, None, None), P("pp", None, "tp"), P("pp", "tp", None))
    return jax.shard_map(stage_body, mesh=mesh, in_specs=in_specs, out_specs=P("pp", None, "dp", "tp", None), check_vma=False)
```

```python
import functools

import jax
import jax.numpy as jnp
from jax import lax
from jax.experimental import pallas as pl
from jax.experimental.pallas import tpu as pltpu
from jax.sharding import PartitionSpec as P

LN_EPS = 1e-5
ROPE_BASE = 10000.0
CHUNKS_PER_MICRO = 8
NT = 256
NX, NR, NP, NS = 4, 4, 3, 4
LATE = 4
EARLY = 24
LEND_AT = (5, 12)
AHEAD = 4
TURN = (("gather0", 0), ("scatter1", 3), ("gather2", 1), ("up", 2), ("finish", 4), ("out", 2), ("scatter0", 2), ("lay_q", 0), ("gather1", 0), ("lay_k", 0), ("lay_v", 1), ("arrive", 1), ("scatter2", 3), ("heads", 1))
MESH = pl.DeviceIdType.MESH


def rope_tables(seq_len, head_dim):
    positions = jnp.arange(seq_len, dtype=jnp.float32)
    inv_freq = ROPE_BASE ** (-2.0 * jnp.arange(head_dim // 2, dtype=jnp.float32) / head_dim)
    angles = positions[:, None] * inv_freq[None, :]
    return jnp.cos(angles), jnp.sin(angles)


def pipeline_kernel(dims, x_hbm, cos_tab, sin_tab, wq_hbm, wk_hbm, wv_hbm, ln_hbm, wup_hbm, wo_hbm, wdn_hbm,
                    xin, lq_hbm, lk_hbm, lv_hbm, lln_hbm, lup_hbm, lo_hbm, ldn_hbm,
                    raw, wqkv, ln_ref, wup, wod, xlate, early, xfull, rbuf, part, ha, hm, qkv, act, mask_ref, cos_ref, sin_ref,
                    w_sem, xin_sem, ag_ss, ag_rs, rs_ss, rs_rs, fwd_sem, home_sem, lw_ss, lw_rs, es_ss, es_rs, eh_ss, eh_rs):
    nc, nl, ne, tp, pp, heads, hd, tok = dims
    rb, d_model = xin.shape[1:]
    rows = tp * rb
    ff = wup.shape[1]
    qd = heads * hd
    last = tp - 1
    z = lax.axis_index("tp")
    s = lax.axis_index("pp")
    has_left, has_right = z > 0, z < last
    has_prev, has_next = s > 0, s < pp - 1
    half = pp // 2
    front = s < half

    def on(cond, fn):
        pl.when(cond)(fn)

    def remote(src, dst, ss, rs, to):
        return pltpu.make_async_remote_copy(src_ref=src, dst_ref=dst, send_sem=ss, recv_sem=rs, device_id=to, device_id_type=MESH)

    def neighbour(way):
        return {"tp": jnp.minimum(z + 1, last) if way == 0 else jnp.maximum(z - 1, 0)}

    def ag_copy(c, h, way, first=None):
        b = jnp.clip(z - h if way == 0 else z + h, 0, last)
        src = (first if first is not None else xin.at[0]) if h == 0 else xfull.at[c % NX, b]
        return remote(src, xfull.at[c % NX, b], ag_ss.at[c % NS, way, h], ag_rs.at[c % NS, way, h], neighbour(way))

    def ag_sends(h, way):
        return has_right & (z >= h) if way == 0 else has_left & (z + h <= last)

    def ag_gets(h, way):
        return z - 1 - h >= 0 if way == 0 else z + 1 + h <= last

    def rs_copy(c, h, way):
        d = jnp.clip(z + last - h if way == 0 else z - last + h, 0, last)
        return remote(part.at[c % NP, d], rbuf.at[c % NR, way, h], rs_ss.at[c % NS, way, h], rs_rs.at[c % NS, way, h], neighbour(way))

    def rs_sends(h, way):
        return z <= h if way == 0 else last - z <= h

    def rs_sends_all(h, way):
        return rs_sends(h, way) & (has_right if way == 0 else has_left)

    def rs_gets(h, way):
        return has_left & (z - 1 <= h) if way == 0 else has_right & (last - 1 - z <= h)

    def fwd_copy(v):
        return remote(xin.at[v], xin.at[v], fwd_sem.at[v], xin_sem.at[v], {"pp": jnp.minimum(s + 1, pp - 1)})

    def turn_copy(v):
        return remote(xin.at[v], xlate.at[v - (nc - nl)], fwd_sem.at[v], xin_sem.at[v + nl], {"pp": 0})

    def next_late_copy(v):
        return remote(xlate.at[v - nc], xlate.at[v - nc], fwd_sem.at[v], xin_sem.at[v], {"pp": jnp.minimum(s + 1, pp - 1)})

    def home_copy(v):
        return remote(xlate.at[v - nc], xin.at[v - nl], home_sem.at[v - nc], xin_sem.at[v - nl], {"pp": jnp.minimum(s + half, pp - 1)})

    own = [wq_hbm, wk_hbm, wv_hbm, ln_hbm, wup_hbm, wo_hbm, wdn_hbm]
    late = [lq_hbm, lk_hbm, lv_hbm, lln_hbm, lup_hbm, lo_hbm, ldn_hbm]
    held = [wqkv.at[:, pl.ds(0, qd)], wqkv.at[:, pl.ds(qd, qd)], wqkv.at[:, pl.ds(2 * qd, qd)], ln_ref, wup, wod.at[pl.ds(0, qd)], wod.at[pl.ds(qd, ff)]]
    weight_copies = [pltpu.make_async_copy(src, dst, w_sem.at[k]) for k, (src, dst) in enumerate(zip(own, [raw.at[0], raw.at[1], raw.at[2]] + held[3:]))]
    swap_copies = [pltpu.make_async_copy(src, dst, w_sem.at[k]) for k, (src, dst) in enumerate(zip(late, held))]
    lend_copies = [remote(src, dst, lw_ss.at[k], lw_rs.at[k], {"pp": jnp.maximum(s - half, 0)}) for k, (src, dst) in enumerate(zip(held[:3] + own[3:], late))]

    helper = s == pp - 1

    def is_early(c):
        return (s == 0) & (c >= 1) & (c <= ne)

    def share_copy(c, h, way):
        b = jnp.clip(z - h if way == 0 else z + h, 0, last)
        src = x_hbm.at[c] if h == 0 else early.at[c - 1, b]
        return remote(src, early.at[c - 1, b], es_ss.at[c - 1, way, h], es_rs.at[c - 1, way, h], neighbour(way))

    def hand_copy(c, b):
        return remote(early.at[c - 1, b], early.at[c - 1, b], eh_ss.at[c - 1, b], eh_rs.at[c - 1, b], {"pp": 0})

    def share_hop(c, h):
        for way in (0, 1):
            if h > 0:
                @pl.when(ag_gets(h - 1, way))
                def _(way=way):
                    share_copy(c, h - 1, way).wait_recv()
                    if h < last:
                        on(ag_sends(h, way), share_copy(c, h, way).start)
                    hand_copy(c, z - h if way == 0 else z + h).start()
            else:
                on(ag_sends(0, way), share_copy(c, 0, way).start)

    barrier = pltpu.get_barrier_semaphore()
    for j in range(1, tp):
        pl.semaphore_signal(barrier, inc=1, device_id={"tp": lax.rem(z + j, tp)}, device_id_type=MESH)
    for j in range(1, pp):
        pl.semaphore_signal(barrier, inc=1, device_id={"pp": lax.rem(s + j, pp)}, device_id_type=MESH)

    def load(c):
        return pltpu.make_async_copy(x_hbm.at[c], xin.at[c], xin_sem.at[c])

    for c in range(AHEAD):
        on(s == 0, load(c).start)
    for copy in weight_copies:
        copy.start()

    lay_rows = 64

    def lay(k):
        weight_copies[k].wait()

        def some(t, carry):
            at = pl.ds(pl.multiple_of(t * lay_rows, lay_rows), lay_rows)
            wqkv[at, k * qd:(k + 1) * qd] = raw[k, at].reshape(lay_rows, qd)
            return carry
        lax.fori_loop(0, d_model // lay_rows, some, 0)

    @pl.when(s > 0)
    def _():
        for k in range(3):
            lay(k)

    for way, alone in ((0, z == 0), (1, z == last)):
        @pl.when(alone)
        def _(way=way):
            for k in range(NR):
                rbuf[k, way, last - 1] = jnp.zeros(rbuf.shape[3:], rbuf.dtype)

    row = lax.broadcasted_iota(jnp.int32, (rows, rows), 0)
    col = lax.broadcasted_iota(jnp.int32, (rows, rows), 1)
    same = row % rb // tok == col % rb // tok
    later = row // rb * tok + row % tok >= col // rb * tok + col % tok
    mask_ref[...] = jnp.where(same, jnp.where(later, 0.0, -1e30), -3e38)
    for b in range(tp):
        for q in range(rb // tok):
            to, of = slice(b * rb + q * tok, b * rb + (q + 1) * tok), slice(b * tok, (b + 1) * tok)
            cos_ref[to] = cos_tab[of]
            sin_ref[to] = sin_tab[of]

    pl.semaphore_wait(barrier, tp - 1 + pp - 1)

    def lend():
        for copy in lend_copies:
            copy.start()

    @pl.when(helper)
    def _():
        def share(i, carry):
            for h in range(tp):
                on((i - h >= 1) & (i - h <= ne), functools.partial(share_hop, i - h, h))
            return carry
        lax.fori_loop(1, ne + tp, share, 0)

    def in_its_place(c, fn):
        on(c < nc, lambda: fn(xin.at[c]))
        on(c >= nc, lambda: fn(xlate.at[c - nc]))

    def ag_start(c):
        on((s == 0) & (c + AHEAD < nc), lambda: load(c + AHEAD).start())
        pltpu.make_async_copy(x_hbm.at[0], xin.at[0], xin_sem.at[c]).wait()
        for k in range(half):
            on((s == half + k) & (c == LEND_AT[k]), lend)

        def send(place):
            for way in (0, 1):
                on(ag_sends(0, way) & ~is_early(c), ag_copy(c, 0, way, place).start)
            xfull[c % NX, z] = place[...]
        in_its_place(c, send)

    def ag_hop(c, h):
        @pl.when(~is_early(c))
        def _():
            for way in (0, 1):
                on(ag_gets(h - 1, way), ag_copy(c, h - 1, way).wait_recv)
                if h < last:
                    on(ag_sends(h, way), ag_copy(c, h, way).start)

        if h == last:
            @pl.when(is_early(c))
            def _():
                for j in range(1, tp):
                    b = lax.rem(z + j, tp)
                    hand_copy(c, b).wait_recv()
                    xfull[c % NX, b] = early[c - 1, b]

    def ag_drain(c):
        @pl.when(~is_early(c))
        def _():
            for h in range(last):
                for way in (0, 1):
                    on(ag_sends(h, way), ag_copy(c, h, way).wait_send)

    def rs_hop(c, h):
        for way in (0, 1):
            @pl.when(rs_sends_all(h, way))
            def _(way=way):
                if h > 0:
                    @pl.when(rs_gets(h - 1, way))
                    def _():
                        rs_copy(c, h - 1, way).wait_recv()
                        d = z + last - h if way == 0 else z - last + h
                        mine = part[c % NP, d].astype(jnp.float32)
                        part[c % NP, d] = (mine + rbuf[c % NR, way, h - 1].astype(jnp.float32)).astype(part.dtype)
                rs_copy(c, h, way).start()

    def rs_drain(c):
        for h in range(last):
            for way in (0, 1):
                on(rs_sends_all(h, way), rs_copy(c, h, way).wait_send)

    def finish(c):
        for way in (0, 1):
            on(rs_gets(last - 1, way), rs_copy(c, last - 1, way).wait_recv)
        f32 = jnp.float32

        def add(place):
            total = place[...].astype(f32) + part[c % NP, z].astype(f32)
            total = total + rbuf[c % NR, 0, last - 1].astype(f32) + rbuf[c % NR, 1, last - 1].astype(f32)
            place[...] = total.astype(xin.dtype)
        in_its_place(c, add)
        turns = (s == half - 1) & (c >= nc - nl)
        on(has_next & (c < nc) & ~turns, lambda: fwd_copy(c).start())
        on(turns & (c < nc), lambda: turn_copy(c).start())
        on((s < half - 1) & (c >= nc), lambda: next_late_copy(c).start())
        on(front & (c >= nc), lambda: home_copy(c).start())

    lt = min(rb, 32)
    per_block = rb // lt

    def norms(c):
        def tile(t, carry):
            x_f32 = xfull[c % NX, t // per_block, pl.ds((t % per_block) * lt, lt)].astype(jnp.float32)
            row_mean = jnp.mean(x_f32, axis=-1, keepdims=True)
            centred = x_f32 - row_mean
            variance = jnp.mean(centred * centred, axis=-1, keepdims=True)
            unit = centred * lax.rsqrt(variance + LN_EPS)
            at = pl.ds(pl.multiple_of(t * lt, lt), lt)
            ha[at] = (unit * ln_ref[0:1] + ln_ref[1:2]).astype(ha.dtype)
            hm[at] = (unit * ln_ref[2:3] + ln_ref[3:4]).astype(hm.dtype)
            return carry
        lax.fori_loop(0, rows // lt, tile, 0, unroll=2)

    def cols(n):
        return pl.ds(pl.multiple_of(n * NT, NT), NT)

    per_tile = NT // hd

    def projections():
        def rotated(n, carry):
            y = jnp.dot(ha[...], wqkv[:, cols(n)], preferred_element_type=jnp.float32)
            for j in range(per_tile):
                head = y[:, j * hd:(j + 1) * hd]
                turned = head * cos_ref[...] + pltpu.roll(head, hd // 2, 1) * sin_ref[...]
                qkv[n * per_tile + j] = turned.astype(qkv.dtype)
            return carry
        lax.fori_loop(0, 2 * qd // NT, rotated, 0, unroll=2)

        def plain(n, carry):
            y = jnp.dot(ha[...], wqkv[:, cols(n)], preferred_element_type=jnp.float32)
            for j in range(per_tile):
                qkv[n * per_tile + j] = y[:, j * hd:(j + 1) * hd].astype(qkv.dtype)
            return carry
        lax.fori_loop(2 * qd // NT, 3 * qd // NT, plain, 0, unroll=True)

    def attention():
        for h in range(heads):
            scores = lax.dot_general(qkv[h], qkv[heads + h], (((1,), (1,)), ((), ())), preferred_element_type=jnp.float32) * (hd ** -0.5)
            floor = mask_ref[...]
            scores = jnp.where(floor == 0.0, scores, floor)
            raised = jnp.exp(scores - jnp.max(scores, axis=-1, keepdims=True))
            probs = (raised * (1.0 / jnp.sum(raised, axis=-1, keepdims=True))).astype(qkv.dtype)
            act[:, h * hd:(h + 1) * hd] = jnp.dot(probs, qkv[2 * heads + h], preferred_element_type=jnp.float32).astype(act.dtype)

    def mlp_up():
        def tile(n, carry):
            u = jnp.dot(hm[...], wup[:, cols(n)], preferred_element_type=jnp.float32)
            g = 0.5 * u * (1.0 + lax.erf(u * (0.5 ** 0.5)))
            act[:, pl.ds(pl.multiple_of(qd + n * NT, NT), NT)] = g.astype(act.dtype)
            return carry
        lax.fori_loop(0, ff // NT, tile, 0, unroll=2)

    def project_out(c):
        def tile(n, carry):
            o = jnp.dot(act[...], wod[:, cols(n)], preferred_element_type=jnp.float32).astype(part.dtype)
            for b in range(tp):
                part[c % NP, b, :, cols(n)] = o[b * rb:(b + 1) * rb]
            return carry
        lax.fori_loop(0, d_model // NT, tile, 0, unroll=2)

    def holds(c):
        return (c >= 0) & (c < nc)

    def weights_ready(c, ks):
        @pl.when((c == 0) | (c == nc))
        def _():
            for k in ks:
                weight_copies[k].wait()

    def swap_weights(c, ks):
        @pl.when(front & (c == nc - 1))
        def _():
            for k in ks:
                lend_copies[k].wait_recv()
                swap_copies[k].start()

    def heads_step(c, lo):
        @pl.when(c == nc)
        def _():
            for k in range(3):
                swap_copies[k].wait()
        weights_ready(c, (3,))
        norms(c)
        projections()
        swap_weights(c, (0, 1, 2, 3))
        attention()

    def up_step(c, lo):
        weights_ready(c, (4,))
        mlp_up()
        swap_weights(c, (4,))

    def out_step(c, lo):
        weights_ready(c, (5, 6))
        ag_drain(c)
        on(c - NP >= lo, lambda: rs_drain(c - NP))
        project_out(c)
        swap_weights(c, (5, 6))

    steps = {
        "gather0": lambda c, lo: ag_start(c),
        "gather1": lambda c, lo: ag_hop(c, 1),
        "gather2": lambda c, lo: ag_hop(c, 2),
        "lay_q": lambda c, lo: on((s == 0) & (c == 0), lambda: lay(0)),
        "lay_k": lambda c, lo: on((s == 0) & (c == 0), lambda: lay(1)),
        "lay_v": lambda c, lo: on((s == 0) & (c == 0), lambda: lay(2)),
        "arrive": lambda c, lo: ag_hop(c, last),
        "heads": heads_step,
        "up": up_step,
        "out": out_step,
        "scatter0": lambda c, lo: rs_hop(c, 0),
        "scatter1": lambda c, lo: rs_hop(c, 1),
        "scatter2": lambda c, lo: rs_hop(c, 2),
        "finish": lambda c, lo: finish(c),
    }
    span = max(behind for _, behind in TURN)

    def segment(k, carry):
        lo = k * nc
        hi = jnp.where(front, jnp.where(k == 0, nc, nc + nl), jnp.where(k == 0, nc - nl, nc))

        def turn(i, carry):
            for name, behind in TURN:
                c = i - behind
                on((c >= lo) & (c < hi), functools.partial(steps[name], c, lo))
            return carry

        lax.fori_loop(lo, jnp.where(hi > lo, hi + span, lo), turn, 0)
        for back in range(1, NP + 1):
            on(hi - back >= lo, lambda: rs_drain(hi - back))
        return carry

    lax.fori_loop(0, 2, segment, 0)

    @pl.when(has_next)
    def _():
        def sent(v, carry):
            fwd_copy(v).wait_send()
            return carry
        lax.fori_loop(0, jnp.where(s < half - 1, nc, nc - nl), sent, 0)

    for k in range(nl):
        on(s == half - 1, turn_copy(nc - nl + k).wait_send)
        on(s < half - 1, next_late_copy(nc + k).wait_send)
        on(front, home_copy(nc + k).wait_send)

    @pl.when(helper)
    def _():
        def sent_early(c, carry):
            for h in range(last):
                for way in (0, 1):
                    on(ag_sends(h, way), share_copy(c, h, way).wait_send)
            for j in range(1, tp):
                hand_copy(c, lax.rem(z + j, tp)).wait_send()
            return carry
        lax.fori_loop(1, ne + 1, sent_early, 0)

    @pl.when(s >= half)
    def _():
        for copy in lend_copies:
            copy.wait_send()
        for k in range(nl):
            c = nc - nl + k
            pltpu.make_async_copy(x_hbm.at[0], xin.at[0], xin_sem.at[c]).wait()


def solution(mesh):
    tp, pp = mesh.shape["tp"], mesh.shape["pp"]

    def stage_body(x_in, ln_params, w_q, w_k, w_v, w_o, w_up, w_down):
        num_micro, batch_dim, tok, d_model = x_in.shape
        heads, hd = w_k.shape[2:]
        ff = w_up.shape[2]
        seqs = batch_dim // CHUNKS_PER_MICRO
        nc = num_micro * CHUNKS_PER_MICRO
        rb = seqs * tok
        rows = tp * rb
        qd = heads * hd
        bf16, f32 = jnp.bfloat16, jnp.float32

        cos_tab, sin_tab = rope_tables(tp * tok, hd)
        cos_full = jnp.concatenate([cos_tab, cos_tab], axis=-1)
        sin_full = jnp.concatenate([-sin_tab, sin_tab], axis=-1)

        any_spec = pl.BlockSpec(memory_space=pl.ANY)
        vmem_spec = pl.BlockSpec(memory_space=pltpu.VMEM)
        dma = pltpu.SemaphoreType.DMA
        flops = 2 * num_micro * tp * batch_dim * tok * (3 * qd * d_model + qd * d_model + 2 * ff * d_model)
        out, *_ = pl.pallas_call(
            functools.partial(pipeline_kernel, (nc, LATE, EARLY, tp, pp, heads, hd, tok)),
            out_shape=[pltpu.VMEM((nc, rb, d_model), bf16)] + [jax.ShapeDtypeStruct((d_model, qd), bf16)] * 3 + [
                jax.ShapeDtypeStruct((4, d_model), f32), jax.ShapeDtypeStruct((d_model, ff), bf16),
                jax.ShapeDtypeStruct((qd, d_model), bf16), jax.ShapeDtypeStruct((ff, d_model), bf16)],
            in_specs=[any_spec, vmem_spec, vmem_spec] + [any_spec] * 7,
            out_specs=[vmem_spec] + [any_spec] * 7,
            scratch_shapes=[
                pltpu.VMEM((3, d_model, heads, hd), bf16),
                pltpu.VMEM((d_model, 3 * qd), bf16),
                pltpu.VMEM((4, d_model), f32),
                pltpu.VMEM((d_model, ff), bf16),
                pltpu.VMEM((qd + ff, d_model), bf16),
                pltpu.VMEM((LATE, rb, d_model), bf16),
                pltpu.VMEM((EARLY, tp, rb, d_model), bf16),
                pltpu.VMEM((NX, tp, rb, d_model), bf16),
                pltpu.VMEM((NR, 2, tp - 1, rb, d_model), bf16),
                pltpu.VMEM((NP, tp, rb, d_model), bf16),
                pltpu.VMEM((rows, d_model), bf16),
                pltpu.VMEM((rows, d_model), bf16),
                pltpu.VMEM((3 * heads, rows, hd), bf16),
                pltpu.VMEM((rows, qd + ff), bf16),
                pltpu.VMEM((rows, rows), f32),
                pltpu.VMEM((rows, hd), f32),
                pltpu.VMEM((rows, hd), f32),
                dma((7,)),
                dma((nc + LATE,)),
                dma((NS, 2, tp - 1)),
                dma((NS, 2, tp - 1)),
                dma((NS, 2, tp - 1)),
                dma((NS, 2, tp - 1)),
                dma((nc + LATE,)),
                dma((LATE,)),
                dma((7,)),
                dma((7,)),
                dma((EARLY, 2, tp - 1)),
                dma((EARLY, 2, tp - 1)),
                dma((EARLY, tp)),
                dma((EARLY, tp)),
            ],
            compiler_params=pltpu.CompilerParams(collective_id=0, has_side_effects=True, vmem_limit_bytes=54 * 2 ** 20),
            cost_estimate=pl.CostEstimate(flops=flops, bytes_accessed=50 * 2 ** 20, transcendentals=0),
            name="pipeline",
        )(x_in.reshape(nc, rb, d_model), cos_full, sin_full, w_q.reshape(d_model, heads, hd), w_k[0], w_v[0], ln_params[0], w_up[0], w_o.reshape(qd, d_model), w_down[0])
        return out.reshape(1, num_micro, batch_dim, tok, d_model)

    in_specs = (P(None, "dp", "tp", None), P("pp", None, None), P("pp", None, "tp", None, None), P("pp", None, "tp", None), P("pp", None, "tp", None), P("pp", "tp", None, None, None), P("pp", None, "tp"), P("pp", "tp", None))
    return jax.shard_map(stage_body, mesh=mesh, in_specs=in_specs, out_specs=P("pp", None, "dp", "tp", None), check_vma=False)
```

```python
import functools

import jax
import jax.numpy as jnp
from jax import lax
from jax.experimental import pallas as pl
from jax.experimental.pallas import tpu as pltpu
from jax.sharding import PartitionSpec as P

LN_EPS = 1e-5
ROPE_BASE = 10000.0
CHUNKS_PER_MICRO = 8
NT = 256
NX, NR, NP, NS = 4, 4, 3, 4
LATE = 4
EARLY = 22
LEND_AT = 8
AHEAD = 4
TURN = (("gather0", 0), ("scatter1", 3), ("gather2", 1), ("up", 2), ("finish", 4), ("out", 2), ("lay_q", 0), ("gather1", 0), ("lay_k", 0), ("scatter0", 2), ("scatter2", 3), ("lay_v", 1), ("arrive", 1), ("heads", 1))
MESH = pl.DeviceIdType.MESH


def rope_tables(seq_len, head_dim):
    positions = jnp.arange(seq_len, dtype=jnp.float32)
    inv_freq = ROPE_BASE ** (-2.0 * jnp.arange(head_dim // 2, dtype=jnp.float32) / head_dim)
    angles = positions[:, None] * inv_freq[None, :]
    return jnp.cos(angles), jnp.sin(angles)


def pipeline_kernel(dims, x_hbm, cos_tab, sin_tab, wq_hbm, wk_hbm, wv_hbm, ln_hbm, wup_hbm, wo_hbm, wdn_hbm,
                    xin, lq_hbm, lk_hbm, lv_hbm, lln_hbm, lup_hbm, lo_hbm, ldn_hbm,
                    raw, wqkv, ln_ref, wup, wod, xlate, early, xfull, rbuf, part, ha, hm, qkv, act, mask_ref, cos_ref, sin_ref,
                    w_sem, xin_sem, ag_ss, ag_rs, rs_ss, rs_rs, fwd_sem, home_sem, lw_ss, lw_rs, es_ss, es_rs, eh_ss, eh_rs):
    nc, nl, ne, tp, pp, heads, hd, tok = dims
    rb, d_model = xin.shape[1:]
    rows = tp * rb
    ff = wup.shape[1]
    qd = heads * hd
    last = tp - 1
    z = lax.axis_index("tp")
    s = lax.axis_index("pp")
    has_left, has_right = z > 0, z < last
    has_prev, has_next = s > 0, s < pp - 1
    half = pp // 2
    front = s < half

    def on(cond, fn):
        pl.when(cond)(fn)

    def remote(src, dst, ss, rs, to):
        return pltpu.make_async_remote_copy(src_ref=src, dst_ref=dst, send_sem=ss, recv_sem=rs, device_id=to, device_id_type=MESH)

    def neighbour(way):
        return {"tp": jnp.minimum(z + 1, last) if way == 0 else jnp.maximum(z - 1, 0)}

    def ag_copy(c, h, way, first=None):
        b = jnp.clip(z - h if way == 0 else z + h, 0, last)
        src = (first if first is not None else xin.at[0]) if h == 0 else xfull.at[c % NX, b]
        return remote(src, xfull.at[c % NX, b], ag_ss.at[c % NS, way, h], ag_rs.at[c % NS, way, h], neighbour(way))

    def ag_sends(h, way):
        return has_right & (z >= h) if way == 0 else has_left & (z + h <= last)

    def ag_gets(h, way):
        return z - 1 - h >= 0 if way == 0 else z + 1 + h <= last

    def rs_copy(c, h, way):
        d = jnp.clip(z + last - h if way == 0 else z - last + h, 0, last)
        return remote(part.at[c % NP, d], rbuf.at[c % NR, way, h], rs_ss.at[c % NS, way, h], rs_rs.at[c % NS, way, h], neighbour(way))

    def rs_sends(h, way):
        return z <= h if way == 0 else last - z <= h

    def rs_sends_all(h, way):
        return rs_sends(h, way) & (has_right if way == 0 else has_left)

    def rs_gets(h, way):
        return has_left & (z - 1 <= h) if way == 0 else has_right & (last - 1 - z <= h)

    def fwd_copy(v):
        return remote(xin.at[v], xin.at[v], fwd_sem.at[v], xin_sem.at[v], {"pp": jnp.minimum(s + 1, pp - 1)})

    def turn_copy(v):
        return remote(xin.at[v], xlate.at[v - (nc - nl)], fwd_sem.at[v], xin_sem.at[v + nl], {"pp": 0})

    def next_late_copy(v):
        return remote(xlate.at[v - nc], xlate.at[v - nc], fwd_sem.at[v], xin_sem.at[v], {"pp": jnp.minimum(s + 1, pp - 1)})

    def home_copy(v):
        return remote(xlate.at[v - nc], xin.at[v - nl], home_sem.at[v - nc], xin_sem.at[v - nl], {"pp": jnp.minimum(s + half, pp - 1)})

    own = [wq_hbm, wk_hbm, wv_hbm, ln_hbm, wup_hbm, wo_hbm, wdn_hbm]
    late = [lq_hbm, lk_hbm, lv_hbm, lln_hbm, lup_hbm, lo_hbm, ldn_hbm]
    held = [wqkv.at[:, pl.ds(0, qd)], wqkv.at[:, pl.ds(qd, qd)], wqkv.at[:, pl.ds(2 * qd, qd)], ln_ref, wup, wod.at[pl.ds(0, qd)], wod.at[pl.ds(qd, ff)]]
    weight_copies = [pltpu.make_async_copy(src, dst, w_sem.at[k]) for k, (src, dst) in enumerate(zip(own, [raw.at[0], raw.at[1], raw.at[2]] + held[3:]))]
    swap_copies = [pltpu.make_async_copy(src, dst, w_sem.at[k]) for k, (src, dst) in enumerate(zip(late, held))]
    lend_copies = [remote(src, dst, lw_ss.at[k], lw_rs.at[k], {"pp": jnp.maximum(s - half, 0)}) for k, (src, dst) in enumerate(zip(held[:3] + own[3:], late))]

    helper = s == pp - 1

    def is_early(c):
        return (s == 0) & (c >= 1) & (c <= ne)

    def share_copy(c, h, way):
        b = jnp.clip(z - h if way == 0 else z + h, 0, last)
        src = x_hbm.at[c] if h == 0 else early.at[c - 1, b]
        return remote(src, early.at[c - 1, b], es_ss.at[c - 1, way, h], es_rs.at[c - 1, way, h], neighbour(way))

    def hand_copy(c, b):
        return remote(early.at[c - 1, b], early.at[c - 1, b], eh_ss.at[c - 1, b], eh_rs.at[c - 1, b], {"pp": 0})

    def share_hop(c, h):
        for way in (0, 1):
            if h > 0:
                @pl.when(ag_gets(h - 1, way))
                def _(way=way):
                    share_copy(c, h - 1, way).wait_recv()
                    if h < last:
                        on(ag_sends(h, way), share_copy(c, h, way).start)
                    hand_copy(c, z - h if way == 0 else z + h).start()
            else:
                on(ag_sends(0, way), share_copy(c, 0, way).start)

    barrier = pltpu.get_barrier_semaphore()
    for j in range(1, tp):
        pl.semaphore_signal(barrier, inc=1, device_id={"tp": lax.rem(z + j, tp)}, device_id_type=MESH)
    for j in range(1, pp):
        pl.semaphore_signal(barrier, inc=1, device_id={"pp": lax.rem(s + j, pp)}, device_id_type=MESH)

    def load(c):
        return pltpu.make_async_copy(x_hbm.at[c], xin.at[c], xin_sem.at[c])

    for c in range(AHEAD):
        on(s == 0, load(c).start)
    for copy in weight_copies:
        copy.start()

    lay_rows = 64

    def lay(k):
        weight_copies[k].wait()

        def some(t, carry):
            at = pl.ds(pl.multiple_of(t * lay_rows, lay_rows), lay_rows)
            wqkv[at, k * qd:(k + 1) * qd] = raw[k, at].reshape(lay_rows, qd)
            return carry
        lax.fori_loop(0, d_model // lay_rows, some, 0)

    @pl.when(s > 0)
    def _():
        for k in range(3):
            lay(k)

    for way, alone in ((0, z == 0), (1, z == last)):
        @pl.when(alone)
        def _(way=way):
            for k in range(NR):
                rbuf[k, way, last - 1] = jnp.zeros(rbuf.shape[3:], rbuf.dtype)

    row = lax.broadcasted_iota(jnp.int32, (rows, rows), 0)
    col = lax.broadcasted_iota(jnp.int32, (rows, rows), 1)
    same = row % rb // tok == col % rb // tok
    later = row // rb * tok + row % tok >= col // rb * tok + col % tok
    mask_ref[...] = jnp.where(same, jnp.where(later, 0.0, -1e30), -3e38)
    for b in range(tp):
        for q in range(rb // tok):
            to, of = slice(b * rb + q * tok, b * rb + (q + 1) * tok), slice(b * tok, (b + 1) * tok)
            cos_ref[to] = cos_tab[of]
            sin_ref[to] = sin_tab[of]

    pl.semaphore_wait(barrier, tp - 1 + pp - 1)

    def lend():
        for copy in lend_copies:
            copy.start()

    @pl.when(helper)
    def _():
        def share(i, carry):
            for h in range(tp):
                on((i - h >= 1) & (i - h <= ne), functools.partial(share_hop, i - h, h))
            return carry
        lax.fori_loop(1, ne + tp, share, 0)

    def in_its_place(c, fn):
        on(c < nc, lambda: fn(xin.at[c]))
        on(c >= nc, lambda: fn(xlate.at[c - nc]))

    def ag_start(c):
        on((s == 0) & (c + AHEAD < nc), lambda: load(c + AHEAD).start())
        pltpu.make_async_copy(x_hbm.at[0], xin.at[0], xin_sem.at[c]).wait()
        on((s >= half) & (c == LEND_AT), lend)

        def send(place):
            for way in (0, 1):
                on(ag_sends(0, way) & ~is_early(c), ag_copy(c, 0, way, place).start)
            xfull[c % NX, z] = place[...]
        in_its_place(c, send)

    def ag_hop(c, h):
        @pl.when(~is_early(c))
        def _():
            for way in (0, 1):
                on(ag_gets(h - 1, way), ag_copy(c, h - 1, way).wait_recv)
                if h < last:
                    on(ag_sends(h, way), ag_copy(c, h, way).start)

        if h == last:
            @pl.when(is_early(c))
            def _():
                for j in range(1, tp):
                    b = lax.rem(z + j, tp)
                    hand_copy(c, b).wait_recv()
                    xfull[c % NX, b] = early[c - 1, b]

    def ag_drain(c):
        @pl.when(~is_early(c))
        def _():
            for h in range(last):
                for way in (0, 1):
                    on(ag_sends(h, way), ag_copy(c, h, way).wait_send)

    def rs_hop(c, h):
        for way in (0, 1):
            @pl.when(rs_sends_all(h, way))
            def _(way=way):
                if h > 0:
                    @pl.when(rs_gets(h - 1, way))
                    def _():
                        rs_copy(c, h - 1, way).wait_recv()
                        d = z + last - h if way == 0 else z - last + h
                        mine = part[c % NP, d].astype(jnp.float32)
                        part[c % NP, d] = (mine + rbuf[c % NR, way, h - 1].astype(jnp.float32)).astype(part.dtype)
                rs_copy(c, h, way).start()

    def rs_drain(c):
        for h in range(last):
            for way in (0, 1):
                on(rs_sends_all(h, way), rs_copy(c, h, way).wait_send)

    def finish(c):
        for way in (0, 1):
            on(rs_gets(last - 1, way), rs_copy(c, last - 1, way).wait_recv)
        f32 = jnp.float32

        def add(place):
            total = place[...].astype(f32) + part[c % NP, z].astype(f32)
            total = total + rbuf[c % NR, 0, last - 1].astype(f32) + rbuf[c % NR, 1, last - 1].astype(f32)
            place[...] = total.astype(xin.dtype)
        in_its_place(c, add)
        turns = (s == half - 1) & (c >= nc - nl)
        on(has_next & (c < nc) & ~turns, lambda: fwd_copy(c).start())
        on(turns & (c < nc), lambda: turn_copy(c).start())
        on((s < half - 1) & (c >= nc), lambda: next_late_copy(c).start())
        on(front & (c >= nc), lambda: home_copy(c).start())

    lt = min(rb, 32)
    per_block = rb // lt

    def norms(c):
        def tile(t, carry):
            x_f32 = xfull[c % NX, t // per_block, pl.ds((t % per_block) * lt, lt)].astype(jnp.float32)
            row_mean = jnp.mean(x_f32, axis=-1, keepdims=True)
            centred = x_f32 - row_mean
            variance = jnp.mean(centred * centred, axis=-1, keepdims=True)
            unit = centred * lax.rsqrt(variance + LN_EPS)
            at = pl.ds(pl.multiple_of(t * lt, lt), lt)
            ha[at] = (unit * ln_ref[0:1] + ln_ref[1:2]).astype(ha.dtype)
            hm[at] = (unit * ln_ref[2:3] + ln_ref[3:4]).astype(hm.dtype)
            return carry
        lax.fori_loop(0, rows // lt, tile, 0, unroll=2)

    def cols(n):
        return pl.ds(pl.multiple_of(n * NT, NT), NT)

    per_tile = NT // hd

    def projections():
        def rotated(n, carry):
            y = jnp.dot(ha[...], wqkv[:, cols(n)], preferred_element_type=jnp.float32)
            for j in range(per_tile):
                head = y[:, j * hd:(j + 1) * hd]
                turned = head * cos_ref[...] + pltpu.roll(head, hd // 2, 1) * sin_ref[...]
                qkv[n * per_tile + j] = turned.astype(qkv.dtype)
            return carry
        lax.fori_loop(0, 2 * qd // NT, rotated, 0, unroll=2)

        def plain(n, carry):
            y = jnp.dot(ha[...], wqkv[:, cols(n)], preferred_element_type=jnp.float32)
            for j in range(per_tile):
                qkv[n * per_tile + j] = y[:, j * hd:(j + 1) * hd].astype(qkv.dtype)
            return carry
        lax.fori_loop(2 * qd // NT, 3 * qd // NT, plain, 0, unroll=True)

    def attention():
        for h in range(heads):
            scores = lax.dot_general(qkv[h], qkv[heads + h], (((1,), (1,)), ((), ())), preferred_element_type=jnp.float32) * (hd ** -0.5)
            floor = mask_ref[...]
            scores = jnp.where(floor == 0.0, scores, floor)
            raised = jnp.exp(scores - jnp.max(scores, axis=-1, keepdims=True))
            probs = (raised * (1.0 / jnp.sum(raised, axis=-1, keepdims=True))).astype(qkv.dtype)
            act[:, h * hd:(h + 1) * hd] = jnp.dot(probs, qkv[2 * heads + h], preferred_element_type=jnp.float32).astype(act.dtype)

    def mlp_up():
        def tile(n, carry):
            u = jnp.dot(hm[...], wup[:, cols(n)], preferred_element_type=jnp.float32)
            g = 0.5 * u * (1.0 + lax.erf(u * (0.5 ** 0.5)))
            act[:, pl.ds(pl.multiple_of(qd + n * NT, NT), NT)] = g.astype(act.dtype)
            return carry
        lax.fori_loop(0, ff // NT, tile, 0, unroll=2)

    def project_out(c):
        def tile(n, carry):
            o = jnp.dot(act[...], wod[:, cols(n)], preferred_element_type=jnp.float32).astype(part.dtype)
            for b in range(tp):
                part[c % NP, b, :, cols(n)] = o[b * rb:(b + 1) * rb]
            return carry
        lax.fori_loop(0, d_model // NT, tile, 0, unroll=2)

    def holds(c):
        return (c >= 0) & (c < nc)

    def weights_ready(c, ks):
        @pl.when((c == 0) | (c == nc))
        def _():
            for k in ks:
                weight_copies[k].wait()

    def swap_weights(c, ks):
        @pl.when(front & (c == nc - 1))
        def _():
            for k in ks:
                lend_copies[k].wait_recv()
                swap_copies[k].start()

    def heads_step(c, lo):
        @pl.when(c == nc)
        def _():
            for k in range(3):
                swap_copies[k].wait()
        weights_ready(c, (3,))
        norms(c)
        projections()
        swap_weights(c, (0, 1, 2, 3))
        attention()

    def up_step(c, lo):
        weights_ready(c, (4,))
        mlp_up()
        swap_weights(c, (4,))

    def out_step(c, lo):
        weights_ready(c, (5, 6))
        ag_drain(c)
        on(c - NP >= lo, lambda: rs_drain(c - NP))
        project_out(c)
        swap_weights(c, (5, 6))

    steps = {
        "gather0": lambda c, lo: ag_start(c),
        "gather1": lambda c, lo: ag_hop(c, 1),
        "gather2": lambda c, lo: ag_hop(c, 2),
        "lay_q": lambda c, lo: on((s == 0) & (c == 0), lambda: lay(0)),
        "lay_k": lambda c, lo: on((s == 0) & (c == 0), lambda: lay(1)),
        "lay_v": lambda c, lo: on((s == 0) & (c == 0), lambda: lay(2)),
        "arrive": lambda c, lo: ag_hop(c, last),
        "heads": heads_step,
        "up": up_step,
        "out": out_step,
        "scatter0": lambda c, lo: rs_hop(c, 0),
        "scatter1": lambda c, lo: rs_hop(c, 1),
        "scatter2": lambda c, lo: rs_hop(c, 2),
        "finish": lambda c, lo: finish(c),
    }
    span = max(behind for _, behind in TURN)

    def segment(k, carry):
        lo = k * nc
        hi = jnp.where(front, jnp.where(k == 0, nc, nc + nl), jnp.where(k == 0, nc - nl, nc))

        def turn(i, carry):
            for name, behind in TURN:
                c = i - behind
                on((c >= lo) & (c < hi), functools.partial(steps[name], c, lo))
            return carry

        lax.fori_loop(lo, jnp.where(hi > lo, hi + span, lo), turn, 0)
        for back in range(1, NP + 1):
            on(hi - back >= lo, lambda: rs_drain(hi - back))
        return carry

    lax.fori_loop(0, 2, segment, 0)

    @pl.when(has_next)
    def _():
        def sent(v, carry):
            fwd_copy(v).wait_send()
            return carry
        lax.fori_loop(0, jnp.where(s < half - 1, nc, nc - nl), sent, 0)

    for k in range(nl):
        on(s == half - 1, turn_copy(nc - nl + k).wait_send)
        on(s < half - 1, next_late_copy(nc + k).wait_send)
        on(front, home_copy(nc + k).wait_send)

    @pl.when(helper)
    def _():
        def sent_early(c, carry):
            for h in range(last):
                for way in (0, 1):
                    on(ag_sends(h, way), share_copy(c, h, way).wait_send)
            for j in range(1, tp):
                hand_copy(c, lax.rem(z + j, tp)).wait_send()
            return carry
        lax.fori_loop(1, ne + 1, sent_early, 0)

    @pl.when(s >= half)
    def _():
        for copy in lend_copies:
            copy.wait_send()
        for k in range(nl):
            c = nc - nl + k
            pltpu.make_async_copy(x_hbm.at[0], xin.at[0], xin_sem.at[c]).wait()


def solution(mesh):
    tp, pp = mesh.shape["tp"], mesh.shape["pp"]

    def stage_body(x_in, ln_params, w_q, w_k, w_v, w_o, w_up, w_down):
        num_micro, batch_dim, tok, d_model = x_in.shape
        heads, hd = w_k.shape[2:]
        ff = w_up.shape[2]
        seqs = batch_dim // CHUNKS_PER_MICRO
        nc = num_micro * CHUNKS_PER_MICRO
        rb = seqs * tok
        rows = tp * rb
        qd = heads * hd
        bf16, f32 = jnp.bfloat16, jnp.float32

        cos_tab, sin_tab = rope_tables(tp * tok, hd)
        cos_full = jnp.concatenate([cos_tab, cos_tab], axis=-1)
        sin_full = jnp.concatenate([-sin_tab, sin_tab], axis=-1)

        any_spec = pl.BlockSpec(memory_space=pl.ANY)
        vmem_spec = pl.BlockSpec(memory_space=pltpu.VMEM)
        dma = pltpu.SemaphoreType.DMA
        flops = 2 * num_micro * tp * batch_dim * tok * (3 * qd * d_model + qd * d_model + 2 * ff * d_model)
        out, *_ = pl.pallas_call(
            functools.partial(pipeline_kernel, (nc, LATE, EARLY, tp, pp, heads, hd, tok)),
            out_shape=[pltpu.VMEM((nc, rb, d_model), bf16)] + [jax.ShapeDtypeStruct((d_model, qd), bf16)] * 3 + [
                jax.ShapeDtypeStruct((4, d_model), f32), jax.ShapeDtypeStruct((d_model, ff), bf16),
                jax.ShapeDtypeStruct((qd, d_model), bf16), jax.ShapeDtypeStruct((ff, d_model), bf16)],
            in_specs=[any_spec, vmem_spec, vmem_spec] + [any_spec] * 7,
            out_specs=[vmem_spec] + [any_spec] * 7,
            scratch_shapes=[
                pltpu.VMEM((3, d_model, heads, hd), bf16),
                pltpu.VMEM((d_model, 3 * qd), bf16),
                pltpu.VMEM((4, d_model), f32),
                pltpu.VMEM((d_model, ff), bf16),
                pltpu.VMEM((qd + ff, d_model), bf16),
                pltpu.VMEM((LATE, rb, d_model), bf16),
                pltpu.VMEM((EARLY, tp, rb, d_model), bf16),
                pltpu.VMEM((NX, tp, rb, d_model), bf16),
                pltpu.VMEM((NR, 2, tp - 1, rb, d_model), bf16),
                pltpu.VMEM((NP, tp, rb, d_model), bf16),
                pltpu.VMEM((rows, d_model), bf16),
                pltpu.VMEM((rows, d_model), bf16),
                pltpu.VMEM((3 * heads, rows, hd), bf16),
                pltpu.VMEM((rows, qd + ff), bf16),
                pltpu.VMEM((rows, rows), f32),
                pltpu.VMEM((rows, hd), f32),
                pltpu.VMEM((rows, hd), f32),
                dma((7,)),
                dma((nc + LATE,)),
                dma((NS, 2, tp - 1)),
                dma((NS, 2, tp - 1)),
                dma((NS, 2, tp - 1)),
                dma((NS, 2, tp - 1)),
                dma((nc + LATE,)),
                dma((LATE,)),
                dma((7,)),
                dma((7,)),
                dma((EARLY, 2, tp - 1)),
                dma((EARLY, 2, tp - 1)),
                dma((EARLY, tp)),
                dma((EARLY, tp)),
            ],
            compiler_params=pltpu.CompilerParams(collective_id=0, has_side_effects=True, vmem_limit_bytes=54 * 2 ** 20),
            cost_estimate=pl.CostEstimate(flops=flops, bytes_accessed=50 * 2 ** 20, transcendentals=0),
            name="pipeline",
        )(x_in.reshape(nc, rb, d_model), cos_full, sin_full, w_q.reshape(d_model, heads, hd), w_k[0], w_v[0], ln_params[0], w_up[0], w_o.reshape(qd, d_model), w_down[0])
        return out.reshape(1, num_micro, batch_dim, tok, d_model)

    in_specs = (P(None, "dp", "tp", None), P("pp", None, None), P("pp", None, "tp", None, None), P("pp", None, "tp", None), P("pp", None, "tp", None), P("pp", "tp", None, None, None), P("pp", None, "tp"), P("pp", "tp", None))
    return jax.shard_map(stage_body, mesh=mesh, in_specs=in_specs, out_specs=P("pp", None, "dp", "tp", None), check_vma=False)
```
